256 devices in a mesh: xy: 64 (over z_hi, y, x, core), gz: 4 (over z_lo).
Axes of the slice: x: 4, y: 4, z: 8 (z_hi: 2, z_lo: 4; z = z_hi * 4 + z_lo), core: 2. Of those that a mesh axis runs over, the one named last changes fastest.
Arguments:
- field: float32 [64, 2, 3, 512, 256], P('gz', None, None, 'xy'), may hold values from -6 to 6
- source: float32 [64, 2, 3, 512, 256], P('gz', None, None, 'xy'), may hold values from -6 to 6
- classes: int32 [64, 512, 256], P('gz', 'xy'), may hold values from 0 to 15
- boundary: int32 [64, 512, 256], P('gz', 'xy'), may hold values 0 or 1
- conductance: float32 [16], replicated, may hold values from 0.001 to 1
- angles: float32 [3], replicated, may hold values from -3.140625 to 3.140625
- strengths: float32 [3], replicated, may hold values from 0.5 to 2
Outputs:
- relaxed: float32 [64, 2, 3, 512, 256], P('gz', None, None, 'xy')
The draws below stay inside these ranges and needn't reach their ends.
All inputs are finite; a program needn't handle non-finite values. No bound on the sum of `boundary` on one device may be relied on, other than what follows from the above.
Results may differ from the reference program's by a relative error of at most 0.00029.
Values sent between devices are 32-bit elements; how exact they have to be, the bound alone decides.
A program may use at most 64 MiB of HBM per device.

```python
import math
import jax
import jax.numpy as jnp
from jax import lax

NX = 256
CLASSES = 16
SWEEPS = 2
NZ = 64
NY = 512


def touch_ends(array, stream_key, least, largest):
    extent = array.shape
    place = [jax.random.randint(jax.random.fold_in(stream_key, axis), (), 0, extent[axis]) for axis in range(len(extent))]
    array = array.at[tuple(place)].set(least)
    longest = extent.index(max(extent))
    place[longest] = (place[longest] + 1) % extent[longest]
    return array.at[tuple(place)].set(largest)


def block_levels(rng, dims, pieces, least, largest):
    def one(position, blocks):
        steps = jax.random.uniform(jax.random.fold_in(jax.random.fold_in(rng, 6), position), (blocks,), jnp.float32, least / len(pieces), largest / len(pieces))
        return jnp.repeat(jnp.exp(steps), dims[position] // blocks).reshape((-1,) + (1,) * (len(dims) - position - 1))

    loudness = one(*pieces[0])
    for cut in pieces[1:]:
        loudness = loudness * one(*cut)
    return loudness


def scatter_about(key, extent, width, limit, split=(), kind=jnp.bfloat16):
    gain = block_levels(key, extent, split, -0.22, 0.18) if split else 1.0
    values = jax.random.normal(key, extent, jnp.float32) * width * gain
    return jnp.minimum(jnp.maximum(values, -limit), limit).astype(kind)


def setup_inputs(seed: int = 0) -> dict:
    keys = jax.random.split(jax.random.key(seed), 8)
    return {
        "field": scatter_about(keys[0], (NZ, 2, 3, NY, NX), 1.0, 6.0, ((0, 4), (3, 64)), jnp.float32),
        "source": scatter_about(keys[1], (NZ, 2, 3, NY, NX), 1.0, 6.0, ((0, 4), (3, 64)), jnp.float32),
        "classes": touch_ends(jax.random.randint(keys[2], (NZ, NY, NX), 0, CLASSES), jax.random.fold_in(keys[2], 1), 0, CLASSES - 1).astype(jnp.int32),
        "boundary": touch_ends((jax.random.randint(keys[3], (NZ, NY, NX), 0, 8) < 1).astype(jnp.int32), jax.random.fold_in(keys[3], 1), 0, 1),
        "conductance": jnp.clip(jnp.exp(jax.random.uniform(keys[4], (CLASSES,), jnp.float32, math.log(0.001), math.log(1.0))), 0.001, 1.0),
        "angles": jnp.clip(jax.random.uniform(keys[5], (3,), jnp.float32, -3.140625, 3.140625), -3.140625, 3.140625),
        "strengths": jnp.clip(jnp.exp(jax.random.uniform(keys[6], (3,), jnp.float32, math.log(0.5), math.log(2.0))), 0.5, 2.0),
    }


coupling = 0.1
penalty = 4.0


def about_depth(cosine, sine_val):
    filler = jnp.zeros_like(cosine)
    ones_fill = jnp.ones_like(cosine)
    return jnp.stack([jnp.stack([cosine, -sine_val, filler]), jnp.stack([sine_val, cosine, filler]), jnp.stack([filler, filler, ones_fill])])


def about_north(cosine, sine_val):
    filler = jnp.zeros_like(cosine)
    ones_fill = jnp.ones_like(cosine)
    return jnp.stack([jnp.stack([cosine, filler, sine_val]), jnp.stack([filler, ones_fill, filler]), jnp.stack([-sine_val, filler, cosine])])


def rotation(angles):
    cosines = jnp.cos(angles)
    sines = jnp.sin(angles)
    first = jnp.dot(about_depth(cosines[0], sines[0]), about_north(cosines[1], sines[1]), precision=lax.Precision.HIGHEST)
    return jnp.dot(first, about_depth(cosines[2], sines[2]), precision=lax.Precision.HIGHEST)


def sweep_forward(driven, diag_real, diag_imag, start):
    def advance(previous, slices):
        inverse, earlier = previous
        forcing, diag_re, diag_im = slices
        pivot_re = diag_re[None] - inverse[0]
        pivot_im = diag_im - inverse[1]
        weight_sq = 1.0 / (pivot_re * pivot_re + pivot_im * pivot_im)
        new_inverse = jnp.stack([pivot_re * weight_sq, -pivot_im * weight_sq])
        new_earlier = jnp.stack([forcing[0] + inverse[0] * earlier[0] - inverse[1] * earlier[1],
                                 forcing[1] + inverse[0] * earlier[1] + inverse[1] * earlier[0]])
        return (new_inverse, new_earlier), (new_inverse, new_earlier)

    last_state, history = lax.scan(advance, start, (driven, diag_real, diag_imag))
    return history


def sweep_backward(inverse_all, carried_all, start):
    def advance(following, slices):
        inverse, carried = slices
        summed = carried + following
        result = jnp.stack([inverse[0] * summed[0] - inverse[1] * summed[1],
                            inverse[0] * summed[1] + inverse[1] * summed[0]])
        return result, result

    last_state, history = lax.scan(advance, start, (inverse_all, carried_all), reverse=True)
    return history


def reference(field, source, classes, boundary, conductance, angles, strengths):
    rotation_matrix = rotation(angles)
    diag_real = 2.0 + 4.0 * coupling + penalty * boundary.astype(jnp.float32)
    diag_imag = conductance[classes][:, None] * strengths[None, :, None, None]
    current = field
    for repeat in range(SWEEPS):
        padded = jnp.pad(current, ((0, 0), (0, 0), (0, 0), (1, 1), (1, 1)))
        beside = padded[:, :, :, 2:, 1:-1] + padded[:, :, :, :-2, 1:-1] + padded[:, :, :, 1:-1, 2:] + padded[:, :, :, 1:-1, :-2]
        driven = source + coupling * beside
        turned = jnp.einsum('cj,zpcyx->zpjyx', rotation_matrix, driven, precision=lax.Precision.HIGHEST)
        blank = jnp.zeros(turned.shape[1:], jnp.float32)
        inverse_all, carried_all = sweep_forward(turned, diag_real, diag_imag, (blank, blank))
        solved = sweep_backward(inverse_all, carried_all, blank)
        current = jnp.einsum('cj,zpjyx->zpcyx', rotation_matrix, solved, precision=lax.Precision.HIGHEST)
    return current
```

```python
import functools

import jax
import jax.numpy as jnp
from jax import lax
from jax.experimental import pallas as pl
from jax.experimental.pallas import tpu as pltpu
from jax.sharding import PartitionSpec as P

SWEEPS = 2
PIECES = 2
VMEM_LIMIT = 62 * 2**20

coupling = 0.1
penalty = 4.0


def mul(a, b):
    return (a[0] * b[0] - a[1] * b[1], a[0] * b[1] + a[1] * b[0])


def add(a, b):
    return (a[0] + b[0], a[1] + b[1])


def inv(a):
    weight = 1.0 / (a[0] * a[0] + a[1] * a[1])
    return (a[0] * weight, -a[1] * weight)


def one_minus(a):
    return (1.0 - a[0], -a[1])


def get(ref, *at):
    return (ref[at + (0,)], ref[at + (1,)])


def put(ref, value, *at):
    ref[at + (0,)] = value[0]
    ref[at + (1,)] = value[1]


def loop(low, high, body, carry, by):
    by = by if (high - low) % by == 0 else 1

    def several(k, carry):
        for i in range(by):
            carry = body(low + k * by + i, carry)
        return carry

    return lax.fori_loop(0, (high - low) // by, several, carry)


def rotation(angles, shape):
    cos = [jnp.cos(jnp.full(shape, angles[i], jnp.float32)) for i in range(3)]
    sin = [jnp.sin(jnp.full(shape, angles[i], jnp.float32)) for i in range(3)]
    (ca, cb, cc), (sa, sb, sc) = cos, sin
    left = [[ca * cb, -sa, ca * sb], [sa * cb, ca, sa * sb], [-sb, jnp.zeros_like(cb), cb]]
    return [[row[0] * cc + row[1] * sc, row[1] * cc - row[0] * sc, row[2]] for row in left]


def relax(
    ngz,
    nxy,
    field,
    source,
    classes,
    boundary,
    conductance,
    angles,
    strengths,
    OUT,
    U,
    S,
    C,
    B,
    SG,
    DR,
    PH,
    PHI,
    PSI,
    T,
    QM,
    EPHI,
    EPSI,
    EH,
    ET,
    ends,
    coef,
    near,
    halo_out,
    halo_in,
    value_in,
    info_in,
    info_out,
    lam_in,
    lam_out,
    extra_in,
    extra_out,
    own_in,
    own_out,
    ch_in,
    ch_out,
    XR,
    CX,
    BX,
    FP,
    FPHI,
    FPSI,
    FT,
    FC,
    far_ends,
    mi_in,
    mi_out,
    in_sems,
    halo_send,
    halo_recv,
    info_send,
    info_recv,
    lam_send,
    lam_recv,
    extra_send,
    extra_recv,
    own_send,
    own_recv,
    ch_send,
    ch_recv,
    far_local,
    far_send,
    far_recv,
    mi_send,
    mi_recv,
):
    ix, iz = lax.axis_index("xy"), lax.axis_index("gz")
    depth, _, _, rows, width = U.shape
    kinds = conductance.shape[0]
    plane = (rows, width)
    has = {
        ("xy", 0): ix > 0,
        ("xy", 1): ix < nxy - 1,
    }
    where_is = {
        ("xy", 0): ix - 1,
        ("xy", 1): ix + 1,
    }
    middle = nxy // 2
    far = (ix == middle, ix == middle - 1)
    is_far = jnp.logical_or(far[0], far[1])
    not_far = jnp.logical_not(is_far)
    beside = [jnp.logical_and(has["xy", side], jnp.logical_not(far[side])) for side in range(2)]
    for steps in (1, 2):
        has["gz", -steps] = iz >= steps
        has["gz", steps] = iz < ngz - steps
        where_is["gz", -steps] = iz - steps
        where_is["gz", steps] = iz + steps
    for steps in (-3, 3):
        has["gz", steps] = jnp.logical_and(is_far, (iz + steps >= 0) & (iz + steps < ngz))
        where_is["gz", steps] = iz + steps
    zs = depth // PIECES
    spans = [pl.ds(piece * zs, zs) for piece in range(PIECES)]
    moves = [(field.at[span], U.at[span]) for span in spans]
    moves += [(classes, C), (boundary, B), (source, S)]
    loads = [
        pltpu.make_async_copy(src, dst, in_sems.at[i]) for i, (src, dst) in enumerate(moves)
    ]
    for load in loads[:-1]:
        load.start()

    barrier = pltpu.get_barrier_semaphore()
    for key, there in has.items():

        @pl.when(there)
        def _():
            pl.semaphore_signal(
                barrier,
                inc=1,
                device_id={key[0]: where_is[key]},
                device_id_type=pl.DeviceIdType.MESH,
            )


    def remote(src, dst, send, recv, key):
        return pltpu.make_async_remote_copy(
            src_ref=src,
            dst_ref=dst,
            send_sem=send,
            recv_sem=recv,
            device_id={key[0]: where_is[key]},
            device_id_type=pl.DeviceIdType.MESH,
        )

    def halo_copy(sweep, side, piece):
        span = pl.ds(piece * zs, zs)
        return remote(
            halo_out.at[sweep, side, :, :, span],
            halo_in.at[sweep, side, :, :, span],
            halo_send.at[sweep, side, piece],
            halo_recv.at[sweep, side, piece],
            ("xy", 1 - side),
        )

    def send_halo(sweep, piece, given=None):
        for side in range(2):
            there = has["xy", 1 - side] if sweep else jnp.logical_and(beside[1 - side], given)

            @pl.when(there)
            def _():
                halo_copy(sweep, side, piece).start()

    def pack(first, last, z, values):
        for i in range(6):
            at = (i // 3, i % 3, pl.ds(z, 1), slice(None))
            first[at] = values[i][:1, :]
            last[at] = values[i][rows - 1 :, :]

    for side in range(2):

        for sweep in range(SWEEPS):

            @pl.when(jnp.logical_not(has["xy", side] if sweep else beside[side]))
            def _():
                halo_in[sweep, side] = jnp.zeros(halo_in.shape[2:], jnp.float32)

        @pl.when((iz if side == 0 else ngz - 1 - iz) < 2)
        def _():
            for part in range(3, 9):
                info_in[side, part] = jnp.zeros(info_in.shape[2:], jnp.float32)
            extra_in[side] = jnp.zeros(extra_in.shape[1:], jnp.float32)
            lam_in[side] = jnp.zeros(lam_in.shape[1:], jnp.float32)
            for sweep in range(SWEEPS):
                for j in range(3):
                    ch_in[sweep, side, j] = jnp.zeros(ch_in.shape[3:], jnp.float32)

    count = sum(there.astype(jnp.int32) for there in has.values())

    def pack_first(z, carry):
        values = [U[z, i // 3, i % 3] for i in range(6)]
        pack(halo_out.at[0, 1], halo_out.at[0, 0], z, values)
        return carry

    for piece in range(PIECES):
        loads[piece].wait()
        if piece == PIECES - 1:
            loads[-1].start()
        loop(piece * zs, (piece + 1) * zs, pack_first, 0, 4)
        if piece == 0:

            @pl.when(not_far)
            def _():
                pl.semaphore_wait(barrier, count)

        send_halo(0, piece, not_far)

    loads[PIECES].wait()
    loads[PIECES + 1].wait()

    def diagonal(z, carry):
        ids = C[z]
        sigma = jnp.zeros(plane, jnp.float32)
        for kind in range(kinds):
            sigma = jnp.where(ids == kind, conductance[kind], sigma)
        SG[z] = sigma
        DR[z] = 2.0 + 4.0 * coupling + penalty * B[z].astype(jnp.float32)
        return carry

    loop(0, depth, diagonal, 0, 4)

    def diag(z):
        real = jnp.broadcast_to(DR[z][None], (3,) + plane)
        sigma = SG[z]
        return real, jnp.stack([sigma * strengths[j] for j in range(3)])

    none = (jnp.zeros((3,) + plane, jnp.float32),) * 2

    def pivots(k, carry):
        p, q = carry
        z, back = k, depth - 1 - k
        d, f = diag(z), diag(back)
        p = inv((d[0] - p[0], d[1] - p[1]))
        q = inv((f[0] - q[0], f[1] - q[1]))
        put(PH, p, z)
        put(PHI, q, back)
        return p, q

    loop(0, depth, pivots, (none, none), 2)
    ones = (jnp.ones((3,) + plane, jnp.float32), none[0])

    def columns(k, carry):
        down, up = carry
        z, back = k, depth - 1 - k
        down = mul(get(PHI, z), down)
        up = mul(get(PH, back), up)
        put(PHI, down, z)
        put(PSI, up, back)
        return down, up

    loop(0, depth, columns, (ones, ones), 2)
    LEFT, RIGHT = 0, 1
    tip = (lambda: get(PHI, 0), lambda: get(PSI, depth - 1))
    across = lambda: get(PSI, 0)

    place = (iz, ngz - 1 - iz)
    even = [lax.rem(k, 2) == 0 for k in place]
    odd = [lax.rem(k, 2) == 1 for k in place]
    onward = [ngz - 1 - k for k in place]

    def to(side, steps):
        return {"gz": iz + steps if side == LEFT else iz - steps}

    def chain_copy(src, dst, send, recv, side, steps):
        return pltpu.make_async_remote_copy(
            src_ref=src,
            dst_ref=dst,
            send_sem=send,
            recv_sem=recv,
            device_id=to(side, steps),
            device_id_type=pl.DeviceIdType.MESH,
        )

    def info_copy(side, j):
        return chain_copy(
            info_out.at[side, j],
            info_in.at[side, j],
            info_send.at[side, j],
            info_recv.at[side, j],
            side,
            1,
        )

    def lam_copy(side, steps, j):
        return chain_copy(
            lam_out.at[side, j],
            lam_in.at[side, j],
            lam_send.at[side, steps - 1, j],
            lam_recv.at[side, j],
            side,
            steps,
        )

    def own_copy(sweep, side, j):
        return chain_copy(
            own_out.at[sweep, side, j],
            own_in.at[sweep, side, j],
            own_send.at[sweep, side, j],
            own_recv.at[sweep, side, j],
            side,
            1,
        )

    def x_copy(sweep, side, steps, j):
        return chain_copy(
            ch_out.at[sweep, side, j],
            ch_in.at[sweep, side, j],
            ch_send.at[sweep, side, steps - 1, j],
            ch_recv.at[sweep, side, j],
            side,
            steps,
        )

    both = jnp.logical_and

    def send_info(side):
        parts = (tip[1 - side](), tip[side](), across())
        for part in range(3):
            for j in range(3):
                for p in range(2):
                    info_out[side, part * 3 + j, p] = parts[part][p][j]
            sends = both(even[side], onward[side] >= 1)

            @pl.when(sends if part == 0 else both(sends, place[side] > 0))
            def _():
                for j in range(3):
                    info_copy(side, part * 3 + j).start()

    def pass_lam(side):
        @pl.when(odd[side])
        def _():
            for j in range(3):
                info_copy(side, j).wait_recv()

        @pl.when(both(odd[side], place[side] >= 2))
        def _():
            for j in range(3, 9):
                info_copy(side, j).wait_recv()

        @pl.when(place[side] >= 2)
        def _():
            for j in range(3):
                lam_copy(side, 1, j).wait_recv()

        for j in range(3):
            tips = [(info_in[side, 3 * k + j, 0], info_in[side, 3 * k + j, 1]) for k in range(3)]
            given = (lam_in[side, j, 0], lam_in[side, j, 1])

            @pl.when(odd[side])
            def _():
                skip = mul(tips[2], inv(one_minus(mul(tips[1], given))))
                along = mul(skip, given)
                lam = add(tips[0], mul(tips[2], along))
                for p in range(2):
                    coef[12 + side, p, j] = along[p]
                    coef[8 + side, p, j] = skip[p]
                    coef[10 + side, p, j] = lam[p]

            @pl.when(even[side])
            def _():
                for p in range(2):
                    coef[10 + side, p, j] = given[p]

            of = lambda pair: (pair[0][j], pair[1][j])
            lam = (coef[10 + side, 0, j], coef[10 + side, 1, j])
            kappa = mul(of(across()), inv(one_minus(mul(of(tip[side]()), lam))))
            over = mul(kappa, lam)
            value = add(of(tip[1 - side]()), mul(of(across()), over))
            for p in range(2):
                coef[side, p, j] = kappa[p]
                coef[2 + side, p, j] = over[p]
                lam_out[side, j, p] = value[p]

            @pl.when(both(odd[side], onward[side] >= 2))
            def _():
                lam_copy(side, 2, j).start()

        @pl.when(both(odd[side], onward[side] >= 1))
        def _():
            for j in range(3):
                lam_copy(side, 1, j).start()

    def extra_copy(side, j):
        return chain_copy(
            extra_out.at[side, j],
            extra_in.at[side, j],
            extra_send.at[side, j],
            extra_recv.at[side, j],
            side,
            1,
        )

    def own_base(side, j):
        return add(
            (ends[1 - side, 0, j], ends[1 - side, 1, j]),
            mul(
                (coef[2 + side, 0, j], coef[2 + side, 1, j]),
                (ends[side, 0, j], ends[side, 1, j]),
            ),
        )

    def own_sum(sweep, side):
        for j in range(3):
            if sweep == 0:
                for p in range(2):
                    own_out[sweep, side, j, p] = ends[1 - side, p, j]
                    extra_out[side, j, p] = ends[side, p, j]
            else:
                base = own_base(side, j)
                for p in range(2):
                    own_out[sweep, side, j, p] = base[p]
            sends = both(even[side], onward[side] >= 1)

            @pl.when(sends)
            def _():
                own_copy(sweep, side, j).start()

            if sweep == 0:

                @pl.when(both(sends, place[side] > 0))
                def _():
                    extra_copy(side, j).start()

    def pass_chain(sweep, side):
        for j in range(3):
            base = own_base(side, j)

            @pl.when(odd[side])
            def _():
                own_copy(sweep, side, j).wait_recv()

            if sweep == 0:

                @pl.when(both(odd[side], place[side] >= 2))
                def _():
                    extra_copy(side, j).wait_recv()

            @pl.when(place[side] >= 2)
            def _():
                x_copy(sweep, side, 1, j).wait_recv()

            given = (ch_in[sweep, side, j, 0], ch_in[sweep, side, j, 1])

            @pl.when(odd[side])
            def _():
                own = (own_in[sweep, side, j, 0], own_in[sweep, side, j, 1])
                if sweep == 0:
                    extra = (extra_in[side, j, 0], extra_in[side, j, 1])
                    own = add(own, mul((coef[12 + side, 0, j], coef[12 + side, 1, j]), extra))
                x = add(own, mul((coef[8 + side, 0, j], coef[8 + side, 1, j]), given))
                for p in range(2):
                    value_in[side, j, p] = x[p]

            @pl.when(even[side])
            def _():
                for p in range(2):
                    value_in[side, j, p] = given[p]

            x = (value_in[side, j, 0], value_in[side, j, 1])
            result = add(base, mul((coef[side, 0, j], coef[side, 1, j]), x))
            for p in range(2):
                ch_out[sweep, side, j, p] = result[p]

            @pl.when(both(odd[side], onward[side] >= 2))
            def _():
                x_copy(sweep, side, 2, j).start()

        @pl.when(both(odd[side], onward[side] >= 1))
        def _():
            for j in range(3):
                x_copy(sweep, side, 1, j).start()

    left_first = iz * 2 < ngz - 1

    def near_side(run):
        @pl.when(left_first)
        def _():
            run(LEFT)

        @pl.when(jnp.logical_not(left_first))
        def _():
            run(RIGHT)

    def far_side(run):
        @pl.when(left_first)
        def _():
            run(RIGHT)

        @pl.when(jnp.logical_not(left_first))
        def _():
            run(LEFT)

    def far_moves(side):
        edge = pl.ds(rows - 1 if side else 0, 1)
        to_far = {"xy": ix + 1 if side else ix - 1}
        sources = [C.at[:, edge, :], B.at[:, edge, :]]
        sources += [U.at[:, :, c, edge, :] for c in range(3)]
        kept = [CX.at[:, 0:1, :], BX.at[:, 0:1, :]]
        kept += [XR.at[:, :, 4 + c : 5 + c, :] for c in range(3)]
        sent = [CX.at[:, 4:5, :], BX.at[:, 4:5, :]]
        sent += [XR.at[:, :, c : c + 1, :] for c in range(3)]
        remotes = [
            pltpu.make_async_remote_copy(
                src_ref=sources[i],
                dst_ref=sent[i],
                send_sem=far_send.at[i],
                recv_sem=far_recv.at[i],
                device_id=to_far,
                device_id_type=pl.DeviceIdType.MESH,
            )
            for i in range(5)
        ]
        locals_ = [pltpu.make_async_copy(sources[i], kept[i], far_local.at[i]) for i in range(5)]
        return remotes, locals_

    @pl.when(is_far)
    def _():
        pl.semaphore_wait(barrier, count)

    for side in range(2):

        @pl.when(far[side])
        def _():
            remotes, locals_ = far_moves(side)
            for copy in remotes + locals_:
                copy.start()

    for piece in range(PIECES):
        send_halo(0, piece, is_far)

    near_side(send_info)
    far_side(send_info)

    angle_matrix = rotation(angles, (rows, 128))
    for c in range(3):
        for j in range(3):
            QM[c, j] = angle_matrix[c][j]

    def matrix():
        return [
            [jnp.concatenate([QM[c, j]] * (width // 128), axis=1) for j in range(3)]
            for c in range(3)
        ]

    def pack_columns(z, carry):
        for src, dst in ((PHI, EPHI), (PSI, EPSI)):
            pack(dst.at[0], dst.at[1], z, [src[z, i // 3, i % 3] for i in range(6)])
        return carry

    loop(0, depth, pack_columns, 0, 4)

    row = lax.broadcasted_iota(jnp.int32, plane, 0)
    lane = lax.broadcasted_iota(jnp.int32, plane, 1)
    zero = jnp.zeros(plane, jnp.float32)

    def turn(q, driven):
        return [
            jnp.stack(
                [
                    q[0][j] * driven[p][0] + q[1][j] * driven[p][1] + q[2][j] * driven[p][2]
                    for j in range(3)
                ]
            )
            for p in range(2)
        ]

    def inner(z, carry):
        first, last = carry
        q = matrix()
        driven = []
        for p in range(2):
            of = []
            for c in range(3):
                u = U[z, p, c]
                around = jnp.where(lane == 0, zero, pltpu.roll(u, 1, 1))
                around += jnp.where(lane == width - 1, zero, pltpu.roll(u, width - 1, 1))
                around += jnp.where(row == 0, zero, pltpu.roll(u, 1, 0))
                around += jnp.where(row == rows - 1, zero, pltpu.roll(u, rows - 1, 0))
                of.append(S[z, p, c] + coupling * around)
            driven.append(of)
        turned = turn(q, driven)
        put(T, turned, z)
        return add(first, mul(get(PHI, z), turned)), add(last, mul(get(PSI, z), turned))

    tiles = [pl.ds(z, rows) for z in range(0, depth, rows)]

    def outer(sweep, side, tile, carry):
        first, last = carry
        q = matrix()
        turned = turn(
            q,
            [[coupling * halo_in[sweep, side, p, c, tile] for c in range(3)] for p in range(2)],
        )
        for p in range(2):
            EH[side, p, :, tile] = turned[p]
        phi = [EPHI[side, p, :, tile] for p in range(2)]
        psi = [EPSI[side, p, :, tile] for p in range(2)]
        return add(first, mul(phi, turned)), add(last, mul(psi, turned))

    third = lax.rem(row, 4)
    part = lambda k: third == k
    used = third < 3

    def mi_copy(steps, stage):
        slot = steps + 3 if steps < 0 else steps + 2
        parts = pl.ds(0, 6) if stage == 0 else pl.ds(6, 4)
        return pltpu.make_async_remote_copy(
            src_ref=mi_out.at[parts],
            dst_ref=mi_in.at[5 - slot, parts],
            send_sem=mi_send.at[slot, stage],
            recv_sem=mi_recv.at[5 - slot, stage],
            device_id={"gz": iz + steps},
            device_id_type=pl.DeviceIdType.MESH,
        )

    all_steps = (-3, -2, -1, 1, 2, 3)

    def to_all(stage, act):
        for steps in all_steps:

            @pl.when((iz + steps >= 0) & (iz + steps < ngz))
            def _():
                act(mi_copy(steps, stage))

    def from_all(stage):
        for steps in all_steps:
            slot = steps + 3 if steps < 0 else steps + 2

            @pl.when((iz + steps >= 0) & (iz + steps < ngz))
            def _():
                pltpu.make_async_remote_copy(
                    src_ref=mi_out.at[pl.ds(0, 6) if stage == 0 else pl.ds(6, 4)],
                    dst_ref=mi_in.at[slot, pl.ds(0, 6) if stage == 0 else pl.ds(6, 4)],
                    send_sem=mi_send.at[slot, stage],
                    recv_sem=mi_recv.at[slot, stage],
                    device_id={"gz": iz + steps},
                    device_id_type=pl.DeviceIdType.MESH,
                ).wait_recv()

    def shifts(of):
        planes = []
        for d in (-2, -1, 0, 1, 2):
            plane_ = zero
            for j in range(3):
                if 0 <= j + d <= 2:
                    plane_ = jnp.where(part(j), of(j, j + d), plane_)
            planes.append((d, plane_))
        return planes

    def mix(planes, x):
        total = None
        for d, plane_ in planes:
            term = plane_ * (x if d == 0 else pltpu.roll(x, (rows - d) % rows, 0))
            total = term if total is None else total + term
        return total

    def far_setup():
        for slot, steps in enumerate(all_steps):

            @pl.when(jnp.logical_not((iz + steps >= 0) & (iz + steps < ngz)))
            def _():
                mi_in[slot] = jnp.zeros(mi_in.shape[1:], jnp.float32)

        q = matrix()
        for i, (_, plane_) in enumerate(shifts(lambda j, k: q[k][j])):
            FC[i] = plane_
        for i, (_, plane_) in enumerate(shifts(lambda j, k: q[j][k])):
            FC[5 + i] = plane_
        strength = jnp.full(plane, strengths[0], jnp.float32)
        for j in (1, 2):
            strength = jnp.where(part(j), strengths[j], strength)
        FC[10] = strength

    def far_first():
        for side in range(2):

            @pl.when(far[side])
            def _():
                remotes, locals_ = far_moves(side)
                for i in range(2):
                    locals_[i].wait()
                    remotes[i].wait_recv()

        own = row < 4

        def far_diagonal(z, carry):
            ids_tile, bound = CX[z], BX[z]
            ids = jnp.where(
                own,
                jnp.broadcast_to(ids_tile[0:1, :], plane),
                jnp.broadcast_to(ids_tile[4:5, :], plane),
            )
            edge = jnp.where(
                own, jnp.broadcast_to(bound[0:1, :], plane), jnp.broadcast_to(bound[4:5, :], plane)
            )
            sigma = jnp.zeros(plane, jnp.float32)
            for kind in range(kinds):
                sigma = jnp.where(ids == kind, conductance[kind], sigma)
            FT[z, 0] = 2.0 + 4.0 * coupling + penalty * edge.astype(jnp.float32)
            FT[z, 1] = sigma * FC[10]
            return carry

        loop(0, depth, far_diagonal, 0, 4)

        def far_pivots(k, carry):
            p, q = carry
            d, f = get(FT, k), get(FT, depth - 1 - k)
            p = inv((d[0] - p[0], d[1] - p[1]))
            q = inv((f[0] - q[0], f[1] - q[1]))
            put(FP, p, k)
            put(FPHI, q, depth - 1 - k)
            return p, q

        loop(0, depth, far_pivots, ((zero, zero), (zero, zero)), 2)
        one = jnp.ones(plane, jnp.float32)

        def far_columns(k, carry):
            down, up = carry
            back = depth - 1 - k
            down = mul(get(FPHI, k), down)
            up = mul(get(FP, back), up)
            put(FPHI, down, k)
            put(FPSI, up, back)
            return down, up

        loop(0, depth, far_columns, ((one, zero), (one, zero)), 2)
        for i, value in enumerate((get(FPHI, 0), get(FPSI, depth - 1), get(FPSI, 0))):
            mi_out[2 * i] = value[0]
            mi_out[2 * i + 1] = value[1]
        to_all(0, lambda copy: copy.start())

    def far_second():
        for side in range(2):

            @pl.when(far[side])
            def _():
                remotes, locals_ = far_moves(side)
                for i in range(2, 5):
                    remotes[i].wait_recv()

        turned_by = [(d, FC[i]) for i, d in enumerate((-2, -1, 0, 1, 2))]

        def far_sums(z, carry):
            first, last = carry
            t = tuple(
                mix(turned_by, jnp.where(used, coupling * XR[z, p], zero)) for p in range(2)
            )
            put(FT, t, z)
            return add(first, mul(get(FPHI, z), t)), add(last, mul(get(FPSI, z), t))

        first, last = loop(0, depth, far_sums, ((zero, zero), (zero, zero)), 4)
        for i, value in enumerate((first, last)):
            mi_out[6 + 2 * i] = value[0]
            mi_out[7 + 2 * i] = value[1]
        to_all(1, lambda copy: copy.start())

        def far_forward(z, m):
            m = mul(get(FP, z), add(get(FT, z), m))
            put(FT, m, z)
            return m

        def far_backward(k, w):
            z = depth - 1 - k
            w = add(get(FT, z), mul(get(FP, z), w))
            put(FT, w, z)
            return w

        loop(0, depth, far_forward, (zero, zero), 4)
        loop(0, depth, far_backward, (zero, zero), 4)

    def far_third():
        from_all(0)
        from_all(1)
        block = lambda slot: [(mi_in[slot, 2 * i], mi_in[slot, 2 * i + 1]) for i in range(5)]
        x = lam = y = mu = (zero, zero)
        for slot in range(3):
            top, bottom, cross, first, last = block(slot)
            det = inv(one_minus(mul(top, lam)))
            x, lam = (
                add(last, mul(cross, mul(det, add(x, mul(lam, first))))),
                add(bottom, mul(mul(cross, cross), mul(det, lam))),
            )
        for slot in (5, 4, 3):
            top, bottom, cross, first, last = block(slot)
            det = inv(one_minus(mul(bottom, mu)))
            y, mu = (
                add(first, mul(cross, mul(det, add(y, mul(mu, last))))),
                add(top, mul(mul(cross, cross), mul(det, mu))),
            )
        top, bottom, cross, first, last = [(mi_out[2 * i], mi_out[2 * i + 1]) for i in range(5)]
        g, h = add(x, mul(lam, first)), add(y, mul(mu, last))
        alpha, beta = one_minus(mul(lam, top)), one_minus(mul(mu, bottom))
        lc, mc = mul(lam, cross), mul(mu, cross)
        both_ = mul(lc, mc)
        whole = mul(alpha, beta)
        det = inv((whole[0] - both_[0], whole[1] - both_[1]))
        put(far_ends, mul(det, add(mul(g, beta), mul(lc, h))), 0)
        put(far_ends, mul(det, add(mul(h, alpha), mul(mc, g))), 1)
        back_by = [(d, FC[5 + i]) for i, d in enumerate((-2, -1, 0, 1, 2))]
        here = row == jnp.where(far[1], rows - 1, 0)

        def far_join(z, carry):
            before, after = get(far_ends, 0), get(far_ends, 1)
            w = add(add(get(FT, z), mul(get(FPHI, z), before)), mul(get(FPSI, z), after))
            for p in range(2):
                u = mix(back_by, w[p])
                FT[z, p] = u
                for c in range(3):
                    U[z, p, c] += jnp.where(here, jnp.broadcast_to(u[c : c + 1, :], plane), zero)
            return carry

        loop(0, depth, far_join, 0, 4)

    def add_far_row(side, piece):
        def one_row(z, carry):
            for p in range(2):
                for c in range(3):
                    halo_in[1, side, p, c, pl.ds(z, 1), :] += FT[z, p, 4 + c : 5 + c, :]
            return carry

        loop(piece * zs, (piece + 1) * zs, one_row, 0, 4)

    loads[PIECES + 2].wait()
    for sweep in range(SWEEPS):
        sums = loop(0, depth, inner, (none, none), 4)
        if sweep == 0:
            near_side(pass_lam)
        halves = [(none, none), (none, none)]
        for piece in range(PIECES):
            for side in range(2):

                @pl.when(has["xy", side] if sweep else beside[side])
                def _():
                    halo_copy(sweep, side, piece).wait_recv()

                if sweep:

                    @pl.when(far[side])
                    def _():
                        add_far_row(side, piece)

                for tile in tiles[piece * len(tiles) // PIECES : (piece + 1) * len(tiles) // PIECES]:
                    halves[side] = outer(sweep, side, tile, halves[side])
        for side in range(2):
            here = row == (0 if side == 0 else rows - 1)
            sums = tuple(
                add(
                    sums[end],
                    tuple(
                        jnp.where(here[None], jnp.sum(part, axis=1, keepdims=True), 0.0)
                        for part in halves[side][end]
                    ),
                )
                for end in range(2)
            )
        put(ends, sums[0], 0)
        put(ends, sums[1], 1)

        near_side(functools.partial(own_sum, sweep))
        far_side(functools.partial(own_sum, sweep))
        near_side(functools.partial(pass_chain, sweep))

        def forward(z, m):
            given = []
            for p in range(2):
                edges = []
                for j in range(3):
                    above = jnp.broadcast_to(EH[0, p, j, pl.ds(z, 1), :], plane)
                    below = jnp.broadcast_to(EH[1, p, j, pl.ds(z, 1), :], plane)
                    edges.append(
                        jnp.where(row == 0, above, zero) + jnp.where(row == rows - 1, below, zero)
                    )
                given.append(T[z, p] + jnp.stack(edges))
            m = mul(get(PH, z), add(given, m))
            put(T, m, z)
            return m

        def backward(k, w):
            z = depth - 1 - k
            w = add(get(T, z), mul(get(PH, z), w))
            put(T, w, z)
            if sweep < SWEEPS - 1:
                pack(ET.at[0], ET.at[1], z, [w[i // 3][i % 3] for i in range(6)])
            return w

        loop(0, depth, forward, none, 4)
        loop(0, depth, backward, none, 4)
        if sweep == 0:
            far_side(pass_lam)
            for side in range(2):
                lam = get(coef, 10 + side)
                away = tuple(
                    jnp.stack([lam_out[1 - side, j, p] for j in range(3)]) for p in range(2)
                )
                det = inv(one_minus(mul(lam, away)))
                put(coef, det, 6 + side)
                put(coef, mul(det, lam), 4 + side)
        far_side(functools.partial(pass_chain, sweep))

        for side in range(2):
            for j in range(3):
                arrived = (value_in[side, j, 0], value_in[side, j, 1])
                other = (ch_out[sweep, 1 - side, j, 0], ch_out[sweep, 1 - side, j, 1])
                value = add(
                    mul((coef[6 + side, 0, j], coef[6 + side, 1, j]), arrived),
                    mul((coef[4 + side, 0, j], coef[4 + side, 1, j]), other),
                )
                near[side, 0, j] = value[0]
                near[side, 1, j] = value[1]

        final = sweep == SWEEPS - 1

        def join_edge(side, tile):
            q = matrix()
            r = 0 if side == 0 else rows - 1
            w = [ET[side, p, :, tile] for p in range(2)]
            for end, column in ((0, EPHI), (1, EPSI)):
                entry = [
                    jnp.broadcast_to(near[end, p, :, r : r + 1, :], (3,) + plane)
                    for p in range(2)
                ]
                w = add(w, mul([column[side, p, :, tile] for p in range(2)], entry))
            for p in range(2):
                for c in range(3):
                    halo_out[sweep + 1, 1 - side, p, c, tile] = (
                        q[c][0] * w[p][0] + q[c][1] * w[p][1] + q[c][2] * w[p][2]
                    )

        if not final:
            for piece in range(PIECES):
                for tile in tiles[piece * len(tiles) // PIECES : (piece + 1) * len(tiles) // PIECES]:
                    for side in range(2):
                        join_edge(side, tile)
                send_halo(sweep + 1, piece)


        def join(z, carry):
            q = matrix()
            before, after = get(near, 0), get(near, 1)
            w = add(add(get(T, z), mul(get(PHI, z), before)), mul(get(PSI, z), after))
            values = []
            for p in range(2):
                for c in range(3):
                    values.append(q[c][0] * w[p][0] + q[c][1] * w[p][1] + q[c][2] * w[p][2])
            target = OUT if final else U
            for i in range(6):
                target[z, i // 3, i % 3] = values[i]
            return carry

        if not final:
            for side in range(2):

                @pl.when(far[side])
                def _():
                    remotes, locals_ = far_moves(side)
                    for copy in remotes:
                        copy.wait_send()
                    for copy in locals_[2:]:
                        copy.wait()

        loop(0, depth, join, 0, 4)

        if not final:

            @pl.when(is_far)
            def _():
                far_setup()
                far_first()
                far_second()
                far_third()

    @pl.when(is_far)
    def _():
        for stage in range(2):
            to_all(stage, lambda copy: copy.wait_send())

    for side in range(2):
        for sweep in range(SWEEPS):

            @pl.when(has["xy", 1 - side] if sweep else beside[1 - side])
            def _():
                for piece in range(PIECES):
                    halo_copy(sweep, side, piece).wait_send()

        sends = both(even[side], onward[side] >= 1)

        @pl.when(sends)
        def _():
            for j in range(3):
                info_copy(side, j).wait_send()
                for sweep in range(SWEEPS):
                    own_copy(sweep, side, j).wait_send()

        @pl.when(both(sends, place[side] > 0))
        def _():
            for j in range(3, 9):
                info_copy(side, j).wait_send()
            for j in range(3):
                extra_copy(side, j).wait_send()

        for steps in (2, 1):

            @pl.when(both(odd[side], onward[side] >= steps))
            def _():
                for j in range(3):
                    lam_copy(side, steps, j).wait_send()
                    for sweep in range(SWEEPS):
                        x_copy(sweep, side, steps, j).wait_send()


def local(ngz, nxy, field, source, classes, boundary, conductance, angles, strengths):
    depth, _, _, rows, width = field.shape
    f32 = jnp.float32
    block = pltpu.VMEM(field.shape, f32)
    flat = (depth, rows, width)
    line = (2, 3, rows, width)
    pair = (2, rows, width)
    edge = (2, 2, 3, depth, width)
    narrow = pltpu.VMEM((depth, 2, rows, width), f32)
    dma = pltpu.SemaphoreType.DMA
    hbm = pl.BlockSpec(memory_space=pl.ANY)
    smem = pl.BlockSpec(memory_space=pltpu.SMEM)
    return pl.pallas_call(
        functools.partial(relax, ngz, nxy),
        out_shape=pltpu.VMEM(field.shape, f32),
        in_specs=[hbm] * 4 + [smem] * 3,
        out_specs=pl.BlockSpec(memory_space=pltpu.VMEM),
        scratch_shapes=[
            block,
            block,
            pltpu.VMEM(flat, jnp.int32),
            pltpu.VMEM(flat, jnp.int32),
            pltpu.VMEM(flat, f32),
            pltpu.VMEM(flat, f32),
            block,
            block,
            block,
            block,
            pltpu.VMEM((3, 3, rows, 128), f32),
            pltpu.VMEM(edge, f32),
            pltpu.VMEM(edge, f32),
            pltpu.VMEM(edge, f32),
            pltpu.VMEM(edge, f32),
            pltpu.VMEM((2,) + line, f32),
            pltpu.VMEM((14,) + line, f32),
            pltpu.VMEM((2,) + line, f32),
            pltpu.VMEM((SWEEPS,) + edge, f32),
            pltpu.VMEM((SWEEPS,) + edge, f32),
            pltpu.VMEM((2, 3) + pair, f32),
            pltpu.VMEM((2, 9) + pair, f32),
            pltpu.VMEM((2, 9) + pair, f32),
            pltpu.VMEM((2, 3) + pair, f32),
            pltpu.VMEM((2, 3) + pair, f32),
            pltpu.VMEM((2, 3) + pair, f32),
            pltpu.VMEM((2, 3) + pair, f32),
            pltpu.VMEM((SWEEPS, 2, 3) + pair, f32),
            pltpu.VMEM((SWEEPS, 2, 3) + pair, f32),
            pltpu.VMEM((SWEEPS, 2, 3) + pair, f32),
            pltpu.VMEM((SWEEPS, 2, 3) + pair, f32),
            narrow,
            pltpu.VMEM(flat, jnp.int32),
            pltpu.VMEM(flat, jnp.int32),
            narrow,
            narrow,
            narrow,
            narrow,
            pltpu.VMEM((11, rows, width), f32),
            pltpu.VMEM((2,) + pair, f32),
            pltpu.VMEM((6, 10, rows, width), f32),
            pltpu.VMEM((10, rows, width), f32),
            dma((PIECES + 3,)),
            dma((SWEEPS, 2, PIECES)),
            dma((SWEEPS, 2, PIECES)),
            dma((2, 9)),
            dma((2, 9)),
            dma((2, 2, 3)),
            dma((2, 3)),
            dma((2, 3)),
            dma((2, 3)),
            dma((SWEEPS, 2, 3)),
            dma((SWEEPS, 2, 3)),
            dma((SWEEPS, 2, 2, 3)),
            dma((SWEEPS, 2, 3)),
            dma((5,)),
            dma((5,)),
            dma((5,)),
            dma((6, 2)),
            dma((6, 2)),
        ],
        compiler_params=pltpu.CompilerParams(collective_id=0, has_side_effects=True, vmem_limit_bytes=VMEM_LIMIT),
    )(field, source, classes, boundary, conductance, angles, strengths)


def solution(mesh):
    in_specs = (
        P("gz", None, None, "xy", None),
        P("gz", None, None, "xy", None),
        P("gz", "xy", None),
        P("gz", "xy", None),
        P(),
        P(),
        P(),
    )
    out_specs = P("gz", None, None, "xy", None)
    body = functools.partial(local, mesh.shape["gz"], mesh.shape["xy"])
    return jax.shard_map(body, mesh=mesh, in_specs=in_specs, out_specs=out_specs, check_vma=False)
```

```python
import functools

import jax
import jax.numpy as jnp
from jax import lax
from jax.experimental import pallas as pl
from jax.experimental.pallas import tpu as pltpu
from jax.sharding import PartitionSpec as P

SWEEPS = 2
PIECES = 2
VMEM_LIMIT = 62 * 2**20

coupling = 0.1
penalty = 4.0


def mul(a, b):
    return (a[0] * b[0] - a[1] * b[1], a[0] * b[1] + a[1] * b[0])


def add(a, b):
    return (a[0] + b[0], a[1] + b[1])


def inv(a):
    weight = 1.0 / (a[0] * a[0] + a[1] * a[1])
    return (a[0] * weight, -a[1] * weight)


def one_minus(a):
    return (1.0 - a[0], -a[1])


def get(ref, *at):
    return (ref[at + (0,)], ref[at + (1,)])


def put(ref, value, *at):
    ref[at + (0,)] = value[0]
    ref[at + (1,)] = value[1]


def loop(low, high, body, carry, by):
    by = by if (high - low) % by == 0 else 1

    def several(k, carry):
        for i in range(by):
            carry = body(low + k * by + i, carry)
        return carry

    return lax.fori_loop(0, (high - low) // by, several, carry)


def rotation(angles, shape):
    cos = [jnp.cos(jnp.full(shape, angles[i], jnp.float32)) for i in range(3)]
    sin = [jnp.sin(jnp.full(shape, angles[i], jnp.float32)) for i in range(3)]
    (ca, cb, cc), (sa, sb, sc) = cos, sin
    left = [[ca * cb, -sa, ca * sb], [sa * cb, ca, sa * sb], [-sb, jnp.zeros_like(cb), cb]]
    return [[row[0] * cc + row[1] * sc, row[1] * cc - row[0] * sc, row[2]] for row in left]


def relax(
    ngz,
    nxy,
    field,
    source,
    classes,
    boundary,
    conductance,
    angles,
    strengths,
    OUT,
    U,
    S,
    C,
    B,
    SG,
    DR,
    PH,
    PHI,
    PSI,
    T,
    QM,
    EPHI,
    EPSI,
    EH,
    ET,
    ends,
    coef,
    near,
    halo_out,
    halo_in,
    value_in,
    info_in,
    info_out,
    lam_in,
    lam_out,
    own_in,
    own_out,
    ch_in,
    ch_out,
    XR,
    CX,
    BX,
    FP,
    FPHI,
    FPSI,
    FT,
    FC,
    far_ends,
    mi_in,
    mi_out,
    in_sems,
    halo_send,
    halo_recv,
    tip_send,
    tip_recv,
    info_send,
    info_recv,
    lam_send,
    lam_recv,
    own_send,
    own_recv,
    ch_send,
    ch_recv,
    far_local,
    far_send,
    far_recv,
    near_ready,
    row_send,
    row_recv,
    mi_send,
    mi_recv,
):
    ix, iz = lax.axis_index("xy"), lax.axis_index("gz")
    depth, _, _, rows, width = U.shape
    kinds = conductance.shape[0]
    plane = (rows, width)
    has = {
        ("xy", 0): ix > 0,
        ("xy", 1): ix < nxy - 1,
    }
    where_is = {
        ("xy", 0): ix - 1,
        ("xy", 1): ix + 1,
    }
    middle = nxy // 2
    far = (ix == middle, ix == middle - 1)
    is_far = jnp.logical_or(far[0], far[1])
    not_far = jnp.logical_not(is_far)
    helps = (ix == middle + 1, ix == middle - 2)
    helper = jnp.logical_or(helps[0], helps[1])
    pair = jnp.where(far[0], ix + 1, ix - 1)
    beside = [jnp.logical_and(has["xy", side], jnp.logical_not(far[side])) for side in range(2)]
    for steps in (1, 2):
        has["gz", -steps] = iz >= steps
        has["gz", steps] = iz < ngz - steps
        where_is["gz", -steps] = iz - steps
        where_is["gz", steps] = iz + steps
    signals = {}
    for key, there in has.items():
        signals[key] = jnp.logical_and(there, not_far)
        if key[0] == "xy":
            signals[key] = jnp.logical_and(signals[key], jnp.logical_not(helps[key[1]]))
    count = sum(there.astype(jnp.int32) for there in signals.values())
    count += ngz * helper.astype(jnp.int32)
    zs = depth // PIECES
    spans = [pl.ds(piece * zs, zs) for piece in range(PIECES)]
    moves = [(field.at[span], U.at[span]) for span in spans]
    moves += [(classes, C), (boundary, B), (source, S)]
    loads = [
        pltpu.make_async_copy(src, dst, in_sems.at[i]) for i, (src, dst) in enumerate(moves)
    ]
    for load in loads[PIECES : PIECES + 2] + loads[:PIECES] + loads[PIECES + 2 :]:
        load.start()

    barrier = pltpu.get_barrier_semaphore()
    for key, there in signals.items():

        @pl.when(there)
        def _():
            pl.semaphore_signal(
                barrier,
                inc=1,
                device_id={key[0]: where_is[key]},
                device_id_type=pl.DeviceIdType.MESH,
            )


    @pl.when(is_far)
    def _():
        for g in range(ngz):
            pl.semaphore_signal(
                barrier,
                inc=1,
                device_id={"xy": pair, "gz": g},
                device_id_type=pl.DeviceIdType.MESH,
            )
        pl.semaphore_signal(
            barrier,
            inc=1,
            device_id={"xy": jnp.where(far[0], ix - 1, ix + 1)},
            device_id_type=pl.DeviceIdType.MESH,
        )

    def remote(src, dst, send, recv, key):
        return pltpu.make_async_remote_copy(
            src_ref=src,
            dst_ref=dst,
            send_sem=send,
            recv_sem=recv,
            device_id={key[0]: where_is[key]},
            device_id_type=pl.DeviceIdType.MESH,
        )

    def halo_copy(sweep, side, piece):
        span = pl.ds(piece * zs, zs)
        return remote(
            halo_out.at[sweep, side, :, :, span],
            halo_in.at[sweep, side, :, :, span],
            halo_send.at[side, piece],
            halo_recv.at[side, piece],
            ("xy", 1 - side),
        )

    def send_halo(sweep, piece):
        for side in range(2):

            @pl.when(has["xy", 1 - side])
            def _():
                halo_copy(sweep, side, piece).start()

    def row_copy(side, p, c):
        return remote(
            U.at[:, p, c, 0 if side else rows - 1, :],
            halo_in.at[0, side, p, c],
            row_send.at[side],
            row_recv.at[side],
            ("xy", 1 - side),
        )

    row_copies = lambda side: [row_copy(side, p, c) for p in range(2) for c in range(3)]
    rows_moved = lambda side: remote(
        halo_in.at[0, side],
        halo_in.at[0, side],
        row_send.at[side],
        row_recv.at[side],
        ("xy", 1 - side),
    )

    def pack(first, last, z, values):
        for i in range(6):
            at = (i // 3, i % 3, pl.ds(z, 1), slice(None))
            first[at] = values[i][:1, :]
            last[at] = values[i][rows - 1 :, :]

    for side in range(2):

        for sweep in range(SWEEPS):

            @pl.when(jnp.logical_not(has["xy", side] if sweep else beside[side]))
            def _():
                halo_in[sweep, side] = jnp.zeros(halo_in.shape[2:], jnp.float32)

        @pl.when((iz if side == 0 else ngz - 1 - iz) < 2)
        def _():
            for part in range(3, 9):
                info_in[side, part] = jnp.zeros(info_in.shape[2:], jnp.float32)
            lam_in[side] = jnp.zeros(lam_in.shape[1:], jnp.float32)
            for sweep in range(SWEEPS):
                ch_in[sweep, side] = jnp.zeros(ch_in.shape[2:], jnp.float32)

    loads[PIECES].wait()
    loads[PIECES + 1].wait()

    def diagonal(z, carry):
        ids = C[z]
        sigma = jnp.zeros(plane, jnp.float32)
        for kind in range(kinds):
            sigma = jnp.where(ids == kind, conductance[kind], sigma)
        SG[z] = sigma
        DR[z] = 2.0 + 4.0 * coupling + penalty * B[z].astype(jnp.float32)
        return carry

    loop(0, depth, diagonal, 0, 4)

    def diag(z):
        real = jnp.broadcast_to(DR[z][None], (3,) + plane)
        sigma = SG[z]
        return real, jnp.stack([sigma * strengths[j] for j in range(3)])

    none = (jnp.zeros((3,) + plane, jnp.float32),) * 2

    def pivots(k, carry):
        p, q = carry
        z, back = k, depth - 1 - k
        d, f = diag(z), diag(back)
        p = inv((d[0] - p[0], d[1] - p[1]))
        q = inv((f[0] - q[0], f[1] - q[1]))
        put(PH, p, z)
        put(PHI, q, back)
        return p, q

    loop(0, depth, pivots, (none, none), 2)
    ones = (jnp.ones((3,) + plane, jnp.float32), none[0])

    def columns(k, carry):
        down, up = carry
        z, back = k, depth - 1 - k
        down = mul(get(PHI, z), down)
        up = mul(get(PH, back), up)
        put(PHI, down, z)
        put(PSI, up, back)
        return down, up

    loop(0, depth, columns, (ones, ones), 2)
    for piece in range(PIECES):
        loads[piece].wait()

    @pl.when(not_far)
    def _():
        pl.semaphore_wait(barrier, count)

    @pl.when(helper)
    def _():
        pl.semaphore_signal(
            near_ready,
            inc=1,
            device_id={"xy": jnp.where(helps[0], ix - 1, ix + 1)},
            device_id_type=pl.DeviceIdType.MESH,
        )

    @pl.when(is_far)
    def _():
        pl.semaphore_wait(near_ready, 1)

    for side in range(2):

        @pl.when(beside[1 - side])
        def _():
            for copy in row_copies(side):
                copy.start()

    LEFT, RIGHT = 0, 1
    tip = (lambda: get(PHI, 0), lambda: get(PSI, depth - 1))
    across = lambda: get(PSI, 0)

    place = (iz, ngz - 1 - iz)
    even = [lax.rem(k, 2) == 0 for k in place]
    odd = [lax.rem(k, 2) == 1 for k in place]
    onward = [ngz - 1 - k for k in place]

    def to(side, steps):
        return {"gz": iz + steps if side == LEFT else iz - steps}

    def chain_copy(src, dst, send, recv, side, steps):
        return pltpu.make_async_remote_copy(
            src_ref=src,
            dst_ref=dst,
            send_sem=send,
            recv_sem=recv,
            device_id=to(side, steps),
            device_id_type=pl.DeviceIdType.MESH,
        )

    def tip_copy(side, j):
        return chain_copy(
            info_out.at[side, j],
            info_in.at[side, j],
            tip_send.at[side],
            tip_recv.at[side, j],
            side,
            1,
        )

    def info_copy(side):
        return chain_copy(
            info_out.at[side, 3:9],
            info_in.at[side, 3:9],
            info_send.at[side],
            info_recv.at[side],
            side,
            1,
        )

    def lam_copy(side, steps, j):
        return chain_copy(
            lam_out.at[side, j],
            lam_in.at[side, j],
            lam_send.at[side, steps - 1],
            lam_recv.at[side, j],
            side,
            steps,
        )

    def own_copy(sweep, side, j):
        return chain_copy(
            own_out.at[sweep, side, j],
            own_in.at[sweep, side, j],
            own_send.at[sweep, side],
            own_recv.at[sweep, side, j],
            side,
            1,
        )

    def x_copy(sweep, side, steps, j):
        return chain_copy(
            ch_out.at[sweep, side, j],
            ch_in.at[sweep, side, j],
            ch_send.at[sweep, side, steps - 1],
            ch_recv.at[sweep, side, j],
            side,
            steps,
        )

    whole = slice(None)

    both = jnp.logical_and

    def send_info(side):
        sends = both(even[side], onward[side] >= 1)
        parts = (tip[1 - side](), tip[side](), across())
        for part in range(3):
            for j in range(3):
                for p in range(2):
                    info_out[side, part * 3 + j, p] = parts[part][p][j]
            if part == 0:

                @pl.when(sends)
                def _():
                    for j in range(3):
                        tip_copy(side, j).start()

        @pl.when(both(sends, place[side] > 0))
        def _():
            info_copy(side).start()

    def pass_lam(side):
        @pl.when(both(odd[side], place[side] >= 2))
        def _():
            info_copy(side).wait_recv()

        for j in range(3):

            @pl.when(odd[side])
            def _():
                tip_copy(side, j).wait_recv()

            @pl.when(place[side] >= 2)
            def _():
                lam_copy(side, 1, j).wait_recv()

            tips = [(info_in[side, 3 * k + j, 0], info_in[side, 3 * k + j, 1]) for k in range(3)]
            given = (lam_in[side, j, 0], lam_in[side, j, 1])

            @pl.when(odd[side])
            def _():
                skip = mul(tips[2], inv(one_minus(mul(tips[1], given))))
                lam = add(tips[0], mul(tips[2], mul(skip, given)))
                for p in range(2):
                    coef[8 + side, p, j] = skip[p]
                    coef[10 + side, p, j] = lam[p]

            @pl.when(even[side])
            def _():
                for p in range(2):
                    coef[10 + side, p, j] = given[p]

            of = lambda pair: (pair[0][j], pair[1][j])
            lam = (coef[10 + side, 0, j], coef[10 + side, 1, j])
            kappa = mul(of(across()), inv(one_minus(mul(of(tip[side]()), lam))))
            over = mul(kappa, lam)
            value = add(of(tip[1 - side]()), mul(of(across()), over))
            for p in range(2):
                coef[side, p, j] = kappa[p]
                coef[2 + side, p, j] = over[p]
                lam_out[side, j, p] = value[p]

            @pl.when(both(odd[side], onward[side] >= 1))
            def _():
                lam_copy(side, 1, j).start()

        @pl.when(both(odd[side], onward[side] >= 2))
        def _():
            for j in range(3):
                lam_copy(side, 2, j).start()

    def own_base(side, j):
        return add(
            (ends[1 - side, 0, j], ends[1 - side, 1, j]),
            mul(
                (coef[2 + side, 0, j], coef[2 + side, 1, j]),
                (ends[side, 0, j], ends[side, 1, j]),
            ),
        )

    def own_sum(sweep, side):
        for j in range(3):
            base = own_base(side, j)
            for p in range(2):
                own_out[sweep, side, j, p] = base[p]

            @pl.when(both(even[side], onward[side] >= 1))
            def _():
                own_copy(sweep, side, j).start()

    def pass_chain(sweep, side):
        for j in range(3):
            base = own_base(side, j)

            @pl.when(odd[side])
            def _():
                own_copy(sweep, side, j).wait_recv()

            @pl.when(place[side] >= 2)
            def _():
                x_copy(sweep, side, 1, j).wait_recv()

            given = (ch_in[sweep, side, j, 0], ch_in[sweep, side, j, 1])

            @pl.when(odd[side])
            def _():
                own = (own_in[sweep, side, j, 0], own_in[sweep, side, j, 1])
                x = add(own, mul((coef[8 + side, 0, j], coef[8 + side, 1, j]), given))
                for p in range(2):
                    value_in[side, j, p] = x[p]

            @pl.when(even[side])
            def _():
                for p in range(2):
                    value_in[side, j, p] = given[p]

            x = (value_in[side, j, 0], value_in[side, j, 1])
            result = add(base, mul((coef[side, 0, j], coef[side, 1, j]), x))
            for p in range(2):
                ch_out[sweep, side, j, p] = result[p]

            @pl.when(both(odd[side], onward[side] >= 2))
            def _():
                x_copy(sweep, side, 2, j).start()

        @pl.when(both(odd[side], onward[side] >= 1))
        def _():
            for j in range(3):
                x_copy(sweep, side, 1, j).start()

    left_first = iz * 2 < ngz - 1

    def near_side(run):
        @pl.when(left_first)
        def _():
            run(LEFT)

        @pl.when(jnp.logical_not(left_first))
        def _():
            run(RIGHT)

    def far_side(run):
        @pl.when(left_first)
        def _():
            run(RIGHT)

        @pl.when(jnp.logical_not(left_first))
        def _():
            run(LEFT)

    def far_source(side, i):
        edge = pl.ds(rows - 1 if side else 0, 1)
        return (C.at[:, edge, :], B.at[:, edge, :])[i] if i < 2 else U.at[:, :, i - 2, edge, :]

    def far_target(i, first):
        at = pl.ds(first if i < 2 else first + i - 2, 1)
        return (CX.at[:, at, :], BX.at[:, at, :])[i] if i < 2 else XR.at[:, :, at, :]

    def far_copy(side, i):
        return pltpu.make_async_remote_copy(
            src_ref=far_source(side, i),
            dst_ref=far_target(i, 4 if i < 2 else 0),
            send_sem=far_send.at[i],
            recv_sem=far_recv.at[i],
            device_id={"xy": ix + 1 if side else ix - 1},
            device_id_type=pl.DeviceIdType.MESH,
        )

    def kept_copy(side, i):
        return pltpu.make_async_copy(
            far_source(side, i), far_target(i, 0 if i < 2 else 4), far_local.at[i]
        )

    def far_begin():
        pl.semaphore_wait(barrier, 1)
        for side in range(2):

            @pl.when(far[side])
            def _():
                for i in range(5):
                    far_copy(side, i).start()
                for i in range(5):
                    kept_copy(side, i).start()

    def near_lam(side):
        pl.when(place[side] < 2)(functools.partial(pass_lam, side))

    def far_lam(side):
        pl.when(place[side] == 2)(functools.partial(pass_lam, side))

    def last_lam(side):
        pl.when(place[side] >= 3)(functools.partial(pass_lam, side))

    near_side(send_info)
    far_side(send_info)

    angle_matrix = rotation(angles, (rows, 128))
    for c in range(3):
        for j in range(3):
            QM[c, j] = angle_matrix[c][j]

    def matrix():
        return [
            [jnp.concatenate([QM[c, j]] * (width // 128), axis=1) for j in range(3)]
            for c in range(3)
        ]

    def pack_columns(z, carry):
        for src, dst in ((PHI, EPHI), (PSI, EPSI)):
            pack(dst.at[0], dst.at[1], z, [src[z, i // 3, i % 3] for i in range(6)])
        return carry

    loop(0, depth, pack_columns, 0, 4)

    row = lax.broadcasted_iota(jnp.int32, plane, 0)
    lane = lax.broadcasted_iota(jnp.int32, plane, 1)
    zero = jnp.zeros(plane, jnp.float32)

    def turn(q, driven):
        return [
            jnp.stack(
                [
                    q[0][j] * driven[p][0] + q[1][j] * driven[p][1] + q[2][j] * driven[p][2]
                    for j in range(3)
                ]
            )
            for p in range(2)
        ]

    def inner(z, carry):
        first, last = carry
        q = matrix()
        driven = []
        for p in range(2):
            of = []
            for c in range(3):
                u = U[z, p, c]
                around = jnp.where(lane == 0, zero, pltpu.roll(u, 1, 1))
                around += jnp.where(lane == width - 1, zero, pltpu.roll(u, width - 1, 1))
                around += jnp.where(row == 0, zero, pltpu.roll(u, 1, 0))
                around += jnp.where(row == rows - 1, zero, pltpu.roll(u, rows - 1, 0))
                of.append(S[z, p, c] + coupling * around)
            driven.append(of)
        turned = turn(q, driven)
        put(T, turned, z)
        return add(first, mul(get(PHI, z), turned)), add(last, mul(get(PSI, z), turned))

    tiles = [pl.ds(z, rows) for z in range(0, depth, rows)]

    def outer(sweep, side, tile, carry):
        first, last = carry
        q = matrix()
        turned = turn(
            q,
            [[coupling * halo_in[sweep, side, p, c, tile] for c in range(3)] for p in range(2)],
        )
        for p in range(2):
            EH[side, p, :, tile] = turned[p]
        phi = [EPHI[side, p, :, tile] for p in range(2)]
        psi = [EPSI[side, p, :, tile] for p in range(2)]
        return add(first, mul(phi, turned)), add(last, mul(psi, turned))

    third = lax.rem(row, 4)
    part = lambda k: third == k
    used = third < 3

    def mi_copy(steps, stage):
        slot = steps + 3 if steps < 0 else steps + 2
        parts = pl.ds(0, 6) if stage == 0 else pl.ds(6, 4)
        return pltpu.make_async_remote_copy(
            src_ref=mi_out.at[parts],
            dst_ref=mi_in.at[5 - slot, parts],
            send_sem=mi_send.at[slot, stage],
            recv_sem=mi_recv.at[5 - slot, stage],
            device_id={"gz": iz + steps},
            device_id_type=pl.DeviceIdType.MESH,
        )

    all_steps = (-3, -2, -1, 1, 2, 3)

    def to_all(stage, act):
        for steps in all_steps:

            @pl.when((iz + steps >= 0) & (iz + steps < ngz))
            def _():
                act(mi_copy(steps, stage))

    def from_all(stage):
        for steps in all_steps:
            slot = steps + 3 if steps < 0 else steps + 2

            @pl.when((iz + steps >= 0) & (iz + steps < ngz))
            def _():
                pltpu.make_async_remote_copy(
                    src_ref=mi_out.at[pl.ds(0, 6) if stage == 0 else pl.ds(6, 4)],
                    dst_ref=mi_in.at[slot, pl.ds(0, 6) if stage == 0 else pl.ds(6, 4)],
                    send_sem=mi_send.at[slot, stage],
                    recv_sem=mi_recv.at[slot, stage],
                    device_id={"gz": iz + steps},
                    device_id_type=pl.DeviceIdType.MESH,
                ).wait_recv()

    def shifts(of):
        planes = []
        for d in (-2, -1, 0, 1, 2):
            plane_ = zero
            for j in range(3):
                if 0 <= j + d <= 2:
                    plane_ = jnp.where(part(j), of(j, j + d), plane_)
            planes.append((d, plane_))
        return planes

    def mix(planes, x):
        total = None
        for d, plane_ in planes:
            term = plane_ * (x if d == 0 else pltpu.roll(x, (rows - d) % rows, 0))
            total = term if total is None else total + term
        return total

    def far_setup():
        for slot, steps in enumerate(all_steps):

            @pl.when(jnp.logical_not((iz + steps >= 0) & (iz + steps < ngz)))
            def _():
                mi_in[slot] = jnp.zeros(mi_in.shape[1:], jnp.float32)

        q = matrix()
        for i, (_, plane_) in enumerate(shifts(lambda j, k: q[k][j])):
            FC[i] = plane_
        for i, (_, plane_) in enumerate(shifts(lambda j, k: q[j][k])):
            FC[5 + i] = plane_
        strength = jnp.full(plane, strengths[0], jnp.float32)
        for j in (1, 2):
            strength = jnp.where(part(j), strengths[j], strength)
        FC[10] = strength

    def far_first():
        for side in range(2):

            @pl.when(far[side])
            def _():
                for i in range(2):
                    kept_copy(side, i).wait()
                    far_copy(side, i).wait_recv()

        own = row < 4

        def far_diagonal(z, carry):
            ids_tile, bound = CX[z], BX[z]
            ids = jnp.where(
                own,
                jnp.broadcast_to(ids_tile[0:1, :], plane),
                jnp.broadcast_to(ids_tile[4:5, :], plane),
            )
            edge = jnp.where(
                own, jnp.broadcast_to(bound[0:1, :], plane), jnp.broadcast_to(bound[4:5, :], plane)
            )
            sigma = jnp.zeros(plane, jnp.float32)
            for kind in range(kinds):
                sigma = jnp.where(ids == kind, conductance[kind], sigma)
            FT[z, 0] = 2.0 + 4.0 * coupling + penalty * edge.astype(jnp.float32)
            FT[z, 1] = sigma * FC[10]
            return carry

        loop(0, depth, far_diagonal, 0, 4)

        def far_pivots(k, carry):
            p, q = carry
            d, f = get(FT, k), get(FT, depth - 1 - k)
            p = inv((d[0] - p[0], d[1] - p[1]))
            q = inv((f[0] - q[0], f[1] - q[1]))
            put(FP, p, k)
            put(FPHI, q, depth - 1 - k)
            return p, q

        loop(0, depth, far_pivots, ((zero, zero), (zero, zero)), 2)
        one = jnp.ones(plane, jnp.float32)

        def far_columns(k, carry):
            down, up = carry
            back = depth - 1 - k
            down = mul(get(FPHI, k), down)
            up = mul(get(FP, back), up)
            put(FPHI, down, k)
            put(FPSI, up, back)
            return down, up

        loop(0, depth, far_columns, ((one, zero), (one, zero)), 2)
        for i, value in enumerate((get(FPHI, 0), get(FPSI, depth - 1), get(FPSI, 0))):
            mi_out[2 * i] = value[0]
            mi_out[2 * i + 1] = value[1]
        to_all(0, lambda copy: copy.start())

    def far_second():
        for side in range(2):

            @pl.when(far[side])
            def _():
                for i in range(2, 5):
                    far_copy(side, i).wait_recv()

        turned_by = [(d, FC[i]) for i, d in enumerate((-2, -1, 0, 1, 2))]

        def far_sums(z, carry):
            first, last = carry
            t = tuple(
                mix(turned_by, jnp.where(used, coupling * XR[z, p], zero)) for p in range(2)
            )
            put(FT, t, z)
            return add(first, mul(get(FPHI, z), t)), add(last, mul(get(FPSI, z), t))

        first, last = loop(0, depth, far_sums, ((zero, zero), (zero, zero)), 4)
        for i, value in enumerate((first, last)):
            mi_out[6 + 2 * i] = value[0]
            mi_out[7 + 2 * i] = value[1]
        to_all(1, lambda copy: copy.start())

        def far_forward(z, m):
            m = mul(get(FP, z), add(get(FT, z), m))
            put(FT, m, z)
            return m

        def far_backward(k, w):
            z = depth - 1 - k
            w = add(get(FT, z), mul(get(FP, z), w))
            put(FT, w, z)
            return w

        loop(0, depth, far_forward, (zero, zero), 4)
        loop(0, depth, far_backward, (zero, zero), 4)

    def far_third():
        from_all(0)
        from_all(1)
        block = lambda slot: [(mi_in[slot, 2 * i], mi_in[slot, 2 * i + 1]) for i in range(5)]
        x = lam = y = mu = (zero, zero)
        for slot in range(3):
            top, bottom, cross, first, last = block(slot)
            det = inv(one_minus(mul(top, lam)))
            x, lam = (
                add(last, mul(cross, mul(det, add(x, mul(lam, first))))),
                add(bottom, mul(mul(cross, cross), mul(det, lam))),
            )
        for slot in (5, 4, 3):
            top, bottom, cross, first, last = block(slot)
            det = inv(one_minus(mul(bottom, mu)))
            y, mu = (
                add(first, mul(cross, mul(det, add(y, mul(mu, last))))),
                add(top, mul(mul(cross, cross), mul(det, mu))),
            )
        top, bottom, cross, first, last = [(mi_out[2 * i], mi_out[2 * i + 1]) for i in range(5)]
        g, h = add(x, mul(lam, first)), add(y, mul(mu, last))
        alpha, beta = one_minus(mul(lam, top)), one_minus(mul(mu, bottom))
        lc, mc = mul(lam, cross), mul(mu, cross)
        both_ = mul(lc, mc)
        whole = mul(alpha, beta)
        det = inv((whole[0] - both_[0], whole[1] - both_[1]))
        put(far_ends, mul(det, add(mul(g, beta), mul(lc, h))), 0)
        put(far_ends, mul(det, add(mul(h, alpha), mul(mc, g))), 1)
        back_by = [(d, FC[5 + i]) for i, d in enumerate((-2, -1, 0, 1, 2))]
        here = row == jnp.where(far[1], rows - 1, 0)

        def far_join(z, carry):
            before, after = get(far_ends, 0), get(far_ends, 1)
            w = add(add(get(FT, z), mul(get(FPHI, z), before)), mul(get(FPSI, z), after))
            for p in range(2):
                u = mix(back_by, w[p])
                FT[z, p] = u
                for c in range(3):
                    U[z, p, c] += jnp.where(here, jnp.broadcast_to(u[c : c + 1, :], plane), zero)
            return carry

        loop(0, depth, far_join, 0, 4)

    def add_far_row(side, piece):
        def one_row(z, carry):
            for p in range(2):
                for c in range(3):
                    halo_in[1, side, p, c, pl.ds(z, 1), :] += FT[z, p, 4 + c : 5 + c, :]
            return carry

        loop(piece * zs, (piece + 1) * zs, one_row, 0, 4)

    loads[PIECES + 2].wait()
    for sweep in range(SWEEPS):
        sums = loop(0, depth, inner, (none, none), 4)
        if sweep == 0:
            near_side(near_lam)
        halves = [(none, none), (none, none)]
        for piece in range(PIECES):
            for side in range(2):

                if sweep == 0 and piece == 0:

                    @pl.when(beside[side])
                    def _():
                        rows_moved(side).wait_recv()

                if sweep:

                    @pl.when(has["xy", side])
                    def _():
                        halo_copy(sweep, side, piece).wait_recv()

                    @pl.when(far[side])
                    def _():
                        add_far_row(side, piece)

                for tile in tiles[piece * len(tiles) // PIECES : (piece + 1) * len(tiles) // PIECES]:
                    halves[side] = outer(sweep, side, tile, halves[side])
        for side in range(2):
            here = row == (0 if side == 0 else rows - 1)
            sums = tuple(
                add(
                    sums[end],
                    tuple(
                        jnp.where(here[None], jnp.sum(part, axis=1, keepdims=True), 0.0)
                        for part in halves[side][end]
                    ),
                )
                for end in range(2)
            )
        put(ends, sums[0], 0)
        put(ends, sums[1], 1)

        near_side(functools.partial(own_sum, sweep))
        if sweep == 0:
            pl.when(is_far)(far_begin)
            far_side(far_lam)
        far_side(functools.partial(own_sum, sweep))
        near_side(functools.partial(pass_chain, sweep))

        def forward(z, m):
            given = []
            for p in range(2):
                edges = []
                for j in range(3):
                    above = jnp.broadcast_to(EH[0, p, j, pl.ds(z, 1), :], plane)
                    below = jnp.broadcast_to(EH[1, p, j, pl.ds(z, 1), :], plane)
                    edges.append(
                        jnp.where(row == 0, above, zero) + jnp.where(row == rows - 1, below, zero)
                    )
                given.append(T[z, p] + jnp.stack(edges))
            m = mul(get(PH, z), add(given, m))
            put(T, m, z)
            return m

        def backward(k, w):
            z = depth - 1 - k
            w = add(get(T, z), mul(get(PH, z), w))
            put(T, w, z)
            if sweep < SWEEPS - 1:
                pack(ET.at[0], ET.at[1], z, [w[i // 3][i % 3] for i in range(6)])
            return w

        loop(0, depth, forward, none, 4)
        loop(0, depth, backward, none, 4)
        if sweep == 0:
            far_side(last_lam)
            for side in range(2):
                lam = get(coef, 10 + side)
                away = tuple(
                    jnp.stack([lam_out[1 - side, j, p] for j in range(3)]) for p in range(2)
                )
                det = inv(one_minus(mul(lam, away)))
                put(coef, det, 6 + side)
                put(coef, mul(det, lam), 4 + side)
        far_side(functools.partial(pass_chain, sweep))

        for side in range(2):
            for j in range(3):
                arrived = (value_in[side, j, 0], value_in[side, j, 1])
                other = (ch_out[sweep, 1 - side, j, 0], ch_out[sweep, 1 - side, j, 1])
                value = add(
                    mul((coef[6 + side, 0, j], coef[6 + side, 1, j]), arrived),
                    mul((coef[4 + side, 0, j], coef[4 + side, 1, j]), other),
                )
                near[side, 0, j] = value[0]
                near[side, 1, j] = value[1]

        final = sweep == SWEEPS - 1

        def join_edge(side, tile):
            q = matrix()
            r = 0 if side == 0 else rows - 1
            w = [ET[side, p, :, tile] for p in range(2)]
            for end, column in ((0, EPHI), (1, EPSI)):
                entry = [
                    jnp.broadcast_to(near[end, p, :, r : r + 1, :], (3,) + plane)
                    for p in range(2)
                ]
                w = add(w, mul([column[side, p, :, tile] for p in range(2)], entry))
            for p in range(2):
                for c in range(3):
                    halo_out[sweep + 1, 1 - side, p, c, tile] = (
                        q[c][0] * w[p][0] + q[c][1] * w[p][1] + q[c][2] * w[p][2]
                    )

        if not final:
            for piece in range(PIECES):
                for tile in tiles[piece * len(tiles) // PIECES : (piece + 1) * len(tiles) // PIECES]:
                    for side in range(2):
                        join_edge(side, tile)
                send_halo(sweep + 1, piece)


        def join(z, carry):
            q = matrix()
            before, after = get(near, 0), get(near, 1)
            w = add(add(get(T, z), mul(get(PHI, z), before)), mul(get(PSI, z), after))
            values = []
            for p in range(2):
                for c in range(3):
                    values.append(q[c][0] * w[p][0] + q[c][1] * w[p][1] + q[c][2] * w[p][2])
            target = OUT if final else U
            for i in range(6):
                target[z, i // 3, i % 3] = values[i]
            return carry

        if not final:
            for side in range(2):

                @pl.when(far[side])
                def _():
                    for i in range(5):
                        far_copy(side, i).wait_send()
                    for i in range(2, 5):
                        kept_copy(side, i).wait()

                @pl.when(beside[1 - side])
                def _():
                    rows_moved(side).wait_send()

        loop(0, depth, join, 0, 4)

        if not final:

            @pl.when(is_far)
            def _():
                far_setup()
                far_first()
                far_second()
                far_third()

    @pl.when(is_far)
    def _():
        for stage in range(2):
            to_all(stage, lambda copy: copy.wait_send())

    for side in range(2):

        @pl.when(has["xy", 1 - side])
        def _():
            for sweep in range(1, SWEEPS):
                for piece in range(PIECES):
                    halo_copy(sweep, side, piece).wait_send()

        sends = both(even[side], onward[side] >= 1)

        @pl.when(sends)
        def _():
            chain_copy(
                info_out.at[side, 0:3],
                info_in.at[side, 0:3],
                tip_send.at[side],
                info_recv.at[side],
                side,
                1,
            ).wait_send()
            for sweep in range(SWEEPS):
                own_copy(sweep, side, whole).wait_send()

        @pl.when(both(sends, place[side] > 0))
        def _():
            info_copy(side).wait_send()

        for steps in (2, 1):

            @pl.when(both(odd[side], onward[side] >= steps))
            def _():
                lam_copy(side, steps, whole).wait_send()
                for sweep in range(SWEEPS):
                    x_copy(sweep, side, steps, whole).wait_send()


def local(ngz, nxy, field, source, classes, boundary, conductance, angles, strengths):
    depth, _, _, rows, width = field.shape
    f32 = jnp.float32
    block = pltpu.VMEM(field.shape, f32)
    flat = (depth, rows, width)
    line = (2, 3, rows, width)
    pair = (2, rows, width)
    edge = (2, 2, 3, depth, width)
    narrow = pltpu.VMEM((depth, 2, rows, width), f32)
    dma = pltpu.SemaphoreType.DMA
    hbm = pl.BlockSpec(memory_space=pl.ANY)
    smem = pl.BlockSpec(memory_space=pltpu.SMEM)
    return pl.pallas_call(
        functools.partial(relax, ngz, nxy),
        out_shape=pltpu.VMEM(field.shape, f32),
        in_specs=[hbm] * 4 + [smem] * 3,
        out_specs=pl.BlockSpec(memory_space=pltpu.VMEM),
        scratch_shapes=[
            block,
            block,
            pltpu.VMEM(flat, jnp.int32),
            pltpu.VMEM(flat, jnp.int32),
            pltpu.VMEM(flat, f32),
            pltpu.VMEM(flat, f32),
            block,
            block,
            block,
            block,
            pltpu.VMEM((3, 3, rows, 128), f32),
            pltpu.VMEM(edge, f32),
            pltpu.VMEM(edge, f32),
            pltpu.VMEM(edge, f32),
            pltpu.VMEM(edge, f32),
            pltpu.VMEM((2,) + line, f32),
            pltpu.VMEM((14,) + line, f32),
            pltpu.VMEM((2,) + line, f32),
            pltpu.VMEM((SWEEPS,) + edge, f32),
            pltpu.VMEM((SWEEPS,) + edge, f32),
            pltpu.VMEM((2, 3) + pair, f32),
            pltpu.VMEM((2, 9) + pair, f32),
            pltpu.VMEM((2, 9) + pair, f32),
            pltpu.VMEM((2, 3) + pair, f32),
            pltpu.VMEM((2, 3) + pair, f32),
            pltpu.VMEM((SWEEPS, 2, 3) + pair, f32),
            pltpu.VMEM((SWEEPS, 2, 3) + pair, f32),
            pltpu.VMEM((SWEEPS, 2, 3) + pair, f32),
            pltpu.VMEM((SWEEPS, 2, 3) + pair, f32),
            narrow,
            pltpu.VMEM(flat, jnp.int32),
            pltpu.VMEM(flat, jnp.int32),
            narrow,
            narrow,
            narrow,
            narrow,
            pltpu.VMEM((11, rows, width), f32),
            pltpu.VMEM((2,) + pair, f32),
            pltpu.VMEM((6, 10, rows, width), f32),
            pltpu.VMEM((10, rows, width), f32),
            dma((PIECES + 3,)),
            dma((2, PIECES)),
            dma((2, PIECES)),
            dma((2,)),
            dma((2, 3)),
            dma((2,)),
            dma((2,)),
            dma((2, 2)),
            dma((2, 3)),
            dma((SWEEPS, 2)),
            dma((SWEEPS, 2, 3)),
            dma((SWEEPS, 2, 2)),
            dma((SWEEPS, 2, 3)),
            dma((5,)),
            dma((5,)),
            dma((5,)),
            pltpu.SemaphoreType.REGULAR,
            dma((2,)),
            dma((2,)),
            dma((6, 2)),
            dma((6, 2)),
        ],
        compiler_params=pltpu.CompilerParams(collective_id=0, has_side_effects=True, vmem_limit_bytes=VMEM_LIMIT),
    )(field, source, classes, boundary, conductance, angles, strengths)


def solution(mesh):
    in_specs = (
        P("gz", None, None, "xy", None),
        P("gz", None, None, "xy", None),
        P("gz", "xy", None),
        P("gz", "xy", None),
        P(),
        P(),
        P(),
    )
    out_specs = P("gz", None, None, "xy", None)
    body = functools.partial(local, mesh.shape["gz"], mesh.shape["xy"])
    return jax.shard_map(body, mesh=mesh, in_specs=in_specs, out_specs=out_specs, check_vma=False)
```

```python
import functools

import jax
import jax.numpy as jnp
from jax import lax
from jax.experimental import pallas as pl
from jax.experimental.pallas import tpu as pltpu
from jax.sharding import PartitionSpec as P

SWEEPS = 2
PIECES = 2
VMEM_LIMIT = 62 * 2**20

coupling = 0.1
penalty = 4.0


def mul(a, b):
    return (a[0] * b[0] - a[1] * b[1], a[0] * b[1] + a[1] * b[0])


def add(a, b):
    return (a[0] + b[0], a[1] + b[1])


def inv(a):
    weight = 1.0 / (a[0] * a[0] + a[1] * a[1])
    return (a[0] * weight, -a[1] * weight)


def one_minus(a):
    return (1.0 - a[0], -a[1])


def get(ref, *at):
    return (ref[at + (0,)], ref[at + (1,)])


def put(ref, value, *at):
    ref[at + (0,)] = value[0]
    ref[at + (1,)] = value[1]


def loop(low, high, body, carry, by):
    by = by if (high - low) % by == 0 else 1

    def several(k, carry):
        for i in range(by):
            carry = body(low + k * by + i, carry)
        return carry

    return lax.fori_loop(0, (high - low) // by, several, carry)


def rotation(angles, shape):
    cos = [jnp.cos(jnp.full(shape, angles[i], jnp.float32)) for i in range(3)]
    sin = [jnp.sin(jnp.full(shape, angles[i], jnp.float32)) for i in range(3)]
    (ca, cb, cc), (sa, sb, sc) = cos, sin
    left = [[ca * cb, -sa, ca * sb], [sa * cb, ca, sa * sb], [-sb, jnp.zeros_like(cb), cb]]
    return [[row[0] * cc + row[1] * sc, row[1] * cc - row[0] * sc, row[2]] for row in left]


def relax(
    ngz,
    nxy,
    field,
    source,
    classes,
    boundary,
    conductance,
    angles,
    strengths,
    OUT,
    U,
    S,
    C,
    B,
    SG,
    DR,
    PH,
    PHI,
    PSI,
    T,
    QM,
    EPHI,
    EPSI,
    EH,
    ET,
    ends,
    coef,
    near,
    halo_out,
    halo_in,
    value_in,
    info_in,
    info_out,
    lam_in,
    lam_out,
    own_in,
    own_out,
    ch_in,
    ch_out,
    XR,
    FA,
    CX,
    BX,
    FP,
    FPHI,
    FPSI,
    FT,
    FC,
    far_ends,
    mi_in,
    mi_out,
    in_sems,
    halo_send,
    halo_recv,
    tip_send,
    tip_recv,
    info_send,
    info_recv,
    lam_send,
    lam_recv,
    own_send,
    own_recv,
    ch_send,
    ch_recv,
    far_local,
    far_send,
    far_recv,
    near_ready,
    row_send,
    row_recv,
    early_send,
    early_recv,
    mi_send,
    mi_recv,
):
    ix, iz = lax.axis_index("xy"), lax.axis_index("gz")
    depth, _, _, rows, width = U.shape
    kinds = conductance.shape[0]
    plane = (rows, width)
    has = {
        ("xy", 0): ix > 0,
        ("xy", 1): ix < nxy - 1,
    }
    where_is = {
        ("xy", 0): ix - 1,
        ("xy", 1): ix + 1,
    }
    middle = nxy // 2
    far = (ix == middle, ix == middle - 1)
    is_far = jnp.logical_or(far[0], far[1])
    not_far = jnp.logical_not(is_far)
    helps = (ix == middle + 1, ix == middle - 2)
    helper = jnp.logical_or(helps[0], helps[1])
    pair = jnp.where(far[0], ix + 1, ix - 1)
    beside = [jnp.logical_and(has["xy", side], jnp.logical_not(far[side])) for side in range(2)]
    for steps in (1, 2):
        has["gz", -steps] = iz >= steps
        has["gz", steps] = iz < ngz - steps
        where_is["gz", -steps] = iz - steps
        where_is["gz", steps] = iz + steps
    signals = {}
    for key, there in has.items():
        signals[key] = jnp.logical_and(there, not_far)
        if key[0] == "xy":
            signals[key] = jnp.logical_and(signals[key], jnp.logical_not(helps[key[1]]))
    count = sum(there.astype(jnp.int32) for there in signals.values())
    count += ngz * helper.astype(jnp.int32)
    zs = depth // PIECES
    spans = [pl.ds(piece * zs, zs) for piece in range(PIECES)]
    moves = [(field.at[span], U.at[span]) for span in spans]
    moves += [(classes, C), (boundary, B), (source, S)]
    loads = [
        pltpu.make_async_copy(src, dst, in_sems.at[i]) for i, (src, dst) in enumerate(moves)
    ]
    for load in loads[PIECES : PIECES + 2] + loads[:PIECES] + loads[PIECES + 2 :]:
        load.start()

    barrier = pltpu.get_barrier_semaphore()
    for key, there in signals.items():

        @pl.when(there)
        def _():
            pl.semaphore_signal(
                barrier,
                inc=1,
                device_id={key[0]: where_is[key]},
                device_id_type=pl.DeviceIdType.MESH,
            )


    @pl.when(is_far)
    def _():
        for g in range(ngz):
            pl.semaphore_signal(
                barrier,
                inc=1,
                device_id={"xy": pair, "gz": g},
                device_id_type=pl.DeviceIdType.MESH,
            )
        pl.semaphore_signal(
            barrier,
            inc=1,
            device_id={"xy": jnp.where(far[0], ix - 1, ix + 1)},
            device_id_type=pl.DeviceIdType.MESH,
        )

    def remote(src, dst, send, recv, key):
        return pltpu.make_async_remote_copy(
            src_ref=src,
            dst_ref=dst,
            send_sem=send,
            recv_sem=recv,
            device_id={key[0]: where_is[key]},
            device_id_type=pl.DeviceIdType.MESH,
        )

    def halo_copy(sweep, side, piece):
        span = pl.ds(piece * zs, zs)
        return remote(
            halo_out.at[sweep, side, :, :, span],
            halo_in.at[sweep, side, :, :, span],
            halo_send.at[side, piece],
            halo_recv.at[side, piece],
            ("xy", 1 - side),
        )

    def send_halo(sweep, piece):
        for side in range(2):

            @pl.when(beside[1 - side])
            def _():
                halo_copy(sweep, side, piece).start()

    def early_copy(side, p, c):
        return remote(
            halo_out.at[1, 1 - side, p, c],
            FA.at[:, p, c, :],
            early_send,
            early_recv,
            ("xy", side),
        )

    def early_moved(side):
        return remote(
            halo_out.at[1, 1 - side],
            halo_out.at[1, 1 - side],
            early_send,
            early_recv,
            ("xy", side),
        )

    def row_copy(side, p, c):
        return remote(
            U.at[:, p, c, 0 if side else rows - 1, :],
            halo_in.at[0, side, p, c],
            row_send.at[side],
            row_recv.at[side],
            ("xy", 1 - side),
        )

    row_copies = lambda side: [row_copy(side, p, c) for p in range(2) for c in range(3)]
    rows_moved = lambda side: remote(
        halo_in.at[0, side],
        halo_in.at[0, side],
        row_send.at[side],
        row_recv.at[side],
        ("xy", 1 - side),
    )

    def pack(first, last, z, values):
        for i in range(6):
            at = (i // 3, i % 3, pl.ds(z, 1), slice(None))
            first[at] = values[i][:1, :]
            last[at] = values[i][rows - 1 :, :]

    for side in range(2):

        for sweep in range(SWEEPS):

            @pl.when(jnp.logical_not(beside[side]))
            def _():
                halo_in[sweep, side] = jnp.zeros(halo_in.shape[2:], jnp.float32)

        @pl.when((iz if side == 0 else ngz - 1 - iz) < 2)
        def _():
            for part in range(3, 9):
                info_in[side, part] = jnp.zeros(info_in.shape[2:], jnp.float32)
            lam_in[side] = jnp.zeros(lam_in.shape[1:], jnp.float32)
            for sweep in range(SWEEPS):
                ch_in[sweep, side] = jnp.zeros(ch_in.shape[2:], jnp.float32)

    loads[PIECES].wait()
    loads[PIECES + 1].wait()

    def diagonal(z, carry):
        ids = C[z]
        sigma = jnp.zeros(plane, jnp.float32)
        for kind in range(kinds):
            sigma = jnp.where(ids == kind, conductance[kind], sigma)
        SG[z] = sigma
        DR[z] = 2.0 + 4.0 * coupling + penalty * B[z].astype(jnp.float32)
        return carry

    loop(0, depth, diagonal, 0, 4)

    def diag(z):
        real = jnp.broadcast_to(DR[z][None], (3,) + plane)
        sigma = SG[z]
        return real, jnp.stack([sigma * strengths[j] for j in range(3)])

    none = (jnp.zeros((3,) + plane, jnp.float32),) * 2

    def pivots(k, carry):
        p, q = carry
        z, back = k, depth - 1 - k
        d, f = diag(z), diag(back)
        p = inv((d[0] - p[0], d[1] - p[1]))
        q = inv((f[0] - q[0], f[1] - q[1]))
        put(PH, p, z)
        put(PHI, q, back)
        return p, q

    loop(0, depth, pivots, (none, none), 2)
    ones = (jnp.ones((3,) + plane, jnp.float32), none[0])

    def columns(k, carry):
        down, up = carry
        z, back = k, depth - 1 - k
        down = mul(get(PHI, z), down)
        up = mul(get(PH, back), up)
        put(PHI, down, z)
        put(PSI, up, back)
        return down, up

    loop(0, depth, columns, (ones, ones), 2)
    for piece in range(PIECES):
        loads[piece].wait()

    @pl.when(not_far)
    def _():
        pl.semaphore_wait(barrier, count)

    @pl.when(helper)
    def _():
        pl.semaphore_signal(
            near_ready,
            inc=1,
            device_id={"xy": jnp.where(helps[0], ix - 1, ix + 1)},
            device_id_type=pl.DeviceIdType.MESH,
        )

    @pl.when(is_far)
    def _():
        pl.semaphore_wait(near_ready, 1)

    for side in range(2):

        @pl.when(beside[1 - side])
        def _():
            for copy in row_copies(side):
                copy.start()

    LEFT, RIGHT = 0, 1
    tip = (lambda: get(PHI, 0), lambda: get(PSI, depth - 1))
    across = lambda: get(PSI, 0)

    place = (iz, ngz - 1 - iz)
    even = [lax.rem(k, 2) == 0 for k in place]
    odd = [lax.rem(k, 2) == 1 for k in place]
    onward = [ngz - 1 - k for k in place]

    def to(side, steps):
        return {"gz": iz + steps if side == LEFT else iz - steps}

    def chain_copy(src, dst, send, recv, side, steps):
        return pltpu.make_async_remote_copy(
            src_ref=src,
            dst_ref=dst,
            send_sem=send,
            recv_sem=recv,
            device_id=to(side, steps),
            device_id_type=pl.DeviceIdType.MESH,
        )

    def tip_copy(side, j):
        return chain_copy(
            info_out.at[side, j],
            info_in.at[side, j],
            tip_send.at[side],
            tip_recv.at[side, j],
            side,
            1,
        )

    def info_copy(side):
        return chain_copy(
            info_out.at[side, 3:9],
            info_in.at[side, 3:9],
            info_send.at[side],
            info_recv.at[side],
            side,
            1,
        )

    def lam_copy(side, steps, j):
        return chain_copy(
            lam_out.at[side, j],
            lam_in.at[side, j],
            lam_send.at[side, steps - 1],
            lam_recv.at[side, j],
            side,
            steps,
        )

    def own_copy(sweep, side, j):
        return chain_copy(
            own_out.at[sweep, side, j],
            own_in.at[sweep, side, j],
            own_send.at[sweep, side],
            own_recv.at[sweep, side, j],
            side,
            1,
        )

    def x_copy(sweep, side, steps, j):
        return chain_copy(
            ch_out.at[sweep, side, j],
            ch_in.at[sweep, side, j],
            ch_send.at[sweep, side, steps - 1],
            ch_recv.at[sweep, side, j],
            side,
            steps,
        )

    whole = slice(None)

    both = jnp.logical_and

    def send_info(side):
        sends = both(even[side], onward[side] >= 1)
        parts = (tip[1 - side](), tip[side](), across())
        for part in range(3):
            for j in range(3):
                for p in range(2):
                    info_out[side, part * 3 + j, p] = parts[part][p][j]
            if part == 0:

                @pl.when(sends)
                def _():
                    for j in range(3):
                        tip_copy(side, j).start()

        @pl.when(both(sends, place[side] > 0))
        def _():
            info_copy(side).start()

    def pass_lam(side):
        @pl.when(both(odd[side], place[side] >= 2))
        def _():
            info_copy(side).wait_recv()

        for j in range(3):

            @pl.when(odd[side])
            def _():
                tip_copy(side, j).wait_recv()

            @pl.when(place[side] >= 2)
            def _():
                lam_copy(side, 1, j).wait_recv()

            tips = [(info_in[side, 3 * k + j, 0], info_in[side, 3 * k + j, 1]) for k in range(3)]
            given = (lam_in[side, j, 0], lam_in[side, j, 1])

            @pl.when(odd[side])
            def _():
                skip = mul(tips[2], inv(one_minus(mul(tips[1], given))))
                lam = add(tips[0], mul(tips[2], mul(skip, given)))
                for p in range(2):
                    coef[8 + side, p, j] = skip[p]
                    coef[10 + side, p, j] = lam[p]

            @pl.when(even[side])
            def _():
                for p in range(2):
                    coef[10 + side, p, j] = given[p]

            of = lambda pair: (pair[0][j], pair[1][j])
            lam = (coef[10 + side, 0, j], coef[10 + side, 1, j])
            kappa = mul(of(across()), inv(one_minus(mul(of(tip[side]()), lam))))
            over = mul(kappa, lam)
            value = add(of(tip[1 - side]()), mul(of(across()), over))
            for p in range(2):
                coef[side, p, j] = kappa[p]
                coef[2 + side, p, j] = over[p]
                lam_out[side, j, p] = value[p]

            @pl.when(both(odd[side], onward[side] >= 1))
            def _():
                lam_copy(side, 1, j).start()

        @pl.when(both(odd[side], onward[side] >= 2))
        def _():
            for j in range(3):
                lam_copy(side, 2, j).start()

    def own_base(side, j):
        return add(
            (ends[1 - side, 0, j], ends[1 - side, 1, j]),
            mul(
                (coef[2 + side, 0, j], coef[2 + side, 1, j]),
                (ends[side, 0, j], ends[side, 1, j]),
            ),
        )

    def own_sum(sweep, side):
        for j in range(3):
            base = own_base(side, j)
            for p in range(2):
                own_out[sweep, side, j, p] = base[p]

            @pl.when(both(even[side], onward[side] >= 1))
            def _():
                own_copy(sweep, side, j).start()

    def pass_chain(sweep, side):
        for j in range(3):
            base = own_base(side, j)

            @pl.when(odd[side])
            def _():
                own_copy(sweep, side, j).wait_recv()

            @pl.when(place[side] >= 2)
            def _():
                x_copy(sweep, side, 1, j).wait_recv()

            given = (ch_in[sweep, side, j, 0], ch_in[sweep, side, j, 1])

            @pl.when(odd[side])
            def _():
                own = (own_in[sweep, side, j, 0], own_in[sweep, side, j, 1])
                x = add(own, mul((coef[8 + side, 0, j], coef[8 + side, 1, j]), given))
                for p in range(2):
                    value_in[side, j, p] = x[p]

            @pl.when(even[side])
            def _():
                for p in range(2):
                    value_in[side, j, p] = given[p]

            x = (value_in[side, j, 0], value_in[side, j, 1])
            result = add(base, mul((coef[side, 0, j], coef[side, 1, j]), x))
            for p in range(2):
                ch_out[sweep, side, j, p] = result[p]

            @pl.when(both(odd[side], onward[side] >= 2))
            def _():
                x_copy(sweep, side, 2, j).start()

        @pl.when(both(odd[side], onward[side] >= 1))
        def _():
            for j in range(3):
                x_copy(sweep, side, 1, j).start()

    left_first = iz * 2 < ngz - 1

    def near_side(run):
        @pl.when(left_first)
        def _():
            run(LEFT)

        @pl.when(jnp.logical_not(left_first))
        def _():
            run(RIGHT)

    def far_side(run):
        @pl.when(left_first)
        def _():
            run(RIGHT)

        @pl.when(jnp.logical_not(left_first))
        def _():
            run(LEFT)

    def far_source(side, i):
        edge = pl.ds(rows - 1 if side else 0, 1)
        return (C.at[:, edge, :], B.at[:, edge, :])[i] if i < 2 else U.at[:, :, i - 2, edge, :]

    def far_target(i, first):
        at = pl.ds(first if i < 2 else first + i - 2, 1)
        return (CX.at[0, :, at, :], BX.at[0, :, at, :])[i] if i < 2 else XR.at[:, :, at, :]

    def far_copy(side, i):
        return pltpu.make_async_remote_copy(
            src_ref=far_source(side, i),
            dst_ref=far_target(i, 4 if i < 2 else 0),
            send_sem=far_send.at[i],
            recv_sem=far_recv.at[i],
            device_id={"xy": ix + 1 if side else ix - 1},
            device_id_type=pl.DeviceIdType.MESH,
        )

    def kept_copy(side, i):
        return pltpu.make_async_copy(
            far_source(side, i), far_target(i, 0 if i < 2 else 4), far_local.at[i]
        )

    def line_copy(side, i):
        first = rows - 1 if side else 0
        edge = pl.ds(first if i < 2 else (first - 1 if side else first + 1), 1)
        at = pl.ds(0 if i < 2 else 4, 1)
        return pltpu.make_async_copy(
            (C, B)[i % 2].at[:, edge, :], (CX, BX)[i % 2].at[1, :, at, :], far_local.at[5 + i]
        )

    def far_begin():
        pl.semaphore_wait(barrier, 1)
        for side in range(2):

            @pl.when(far[side])
            def _():
                for i in range(5):
                    far_copy(side, i).start()
                for i in range(5):
                    kept_copy(side, i).start()
                for i in range(4):
                    line_copy(side, i).start()

    def near_lam(side):
        pl.when(place[side] < 2)(functools.partial(pass_lam, side))

    def far_lam(side):
        pl.when(place[side] == 2)(functools.partial(pass_lam, side))

    def last_lam(side):
        pl.when(place[side] >= 3)(functools.partial(pass_lam, side))

    near_side(send_info)
    far_side(send_info)

    angle_matrix = rotation(angles, (rows, 128))
    for c in range(3):
        for j in range(3):
            QM[c, j] = angle_matrix[c][j]

    def matrix():
        return [
            [jnp.concatenate([QM[c, j]] * (width // 128), axis=1) for j in range(3)]
            for c in range(3)
        ]

    def pack_columns(z, carry):
        for src, dst in ((PHI, EPHI), (PSI, EPSI)):
            pack(dst.at[0], dst.at[1], z, [src[z, i // 3, i % 3] for i in range(6)])
        return carry

    loop(0, depth, pack_columns, 0, 4)

    row = lax.broadcasted_iota(jnp.int32, plane, 0)
    lane = lax.broadcasted_iota(jnp.int32, plane, 1)
    zero = jnp.zeros(plane, jnp.float32)

    def turn(q, driven):
        return [
            jnp.stack(
                [
                    q[0][j] * driven[p][0] + q[1][j] * driven[p][1] + q[2][j] * driven[p][2]
                    for j in range(3)
                ]
            )
            for p in range(2)
        ]

    def inner(z, carry):
        first, last = carry
        q = matrix()
        driven = []
        for p in range(2):
            of = []
            for c in range(3):
                u = U[z, p, c]
                around = jnp.where(lane == 0, zero, pltpu.roll(u, 1, 1))
                around += jnp.where(lane == width - 1, zero, pltpu.roll(u, width - 1, 1))
                around += jnp.where(row == 0, zero, pltpu.roll(u, 1, 0))
                around += jnp.where(row == rows - 1, zero, pltpu.roll(u, rows - 1, 0))
                of.append(S[z, p, c] + coupling * around)
            driven.append(of)
        turned = turn(q, driven)
        put(T, turned, z)
        return add(first, mul(get(PHI, z), turned)), add(last, mul(get(PSI, z), turned))

    tiles = [pl.ds(z, rows) for z in range(0, depth, rows)]

    def outer(sweep, side, tile, carry):
        first, last = carry
        q = matrix()
        turned = turn(
            q,
            [[coupling * halo_in[sweep, side, p, c, tile] for c in range(3)] for p in range(2)],
        )
        for p in range(2):
            EH[side, p, :, tile] = turned[p]
        phi = [EPHI[side, p, :, tile] for p in range(2)]
        psi = [EPSI[side, p, :, tile] for p in range(2)]
        return add(first, mul(phi, turned)), add(last, mul(psi, turned))

    third = lax.rem(row, 4)
    part = lambda k: third == k
    used = third < 3

    def mi_copy(k, steps, parts=slice(None)):
        slot = steps + 3 if steps < 0 else steps + 2
        return pltpu.make_async_remote_copy(
            src_ref=mi_out.at[k, parts],
            dst_ref=mi_in.at[k, 5 - slot, parts],
            send_sem=mi_send.at[k, slot],
            recv_sem=mi_recv.at[k, 5 - slot],
            device_id={"gz": iz + steps},
            device_id_type=pl.DeviceIdType.MESH,
        )

    all_steps = (-3, -2, -1, 1, 2, 3)

    def for_all(act):
        for steps in all_steps:

            @pl.when((iz + steps >= 0) & (iz + steps < ngz))
            def _():
                act(steps)

    def to_all(k, parts):
        for_all(lambda steps: mi_copy(k, steps, parts).start())

    def from_all(k):
        for_all(lambda steps: mi_copy(k, -steps).wait_recv())

    def shifts(of):
        planes = []
        for d in (-2, -1, 0, 1, 2):
            plane_ = zero
            for j in range(3):
                if 0 <= j + d <= 2:
                    plane_ = jnp.where(part(j), of(j, j + d), plane_)
            planes.append((d, plane_))
        return planes

    def mix(planes, x):
        total = None
        for d, plane_ in planes:
            term = plane_ * (x if d == 0 else pltpu.roll(x, (rows - d) % rows, 0))
            total = term if total is None else total + term
        return total

    def far_setup():
        for slot, steps in enumerate(all_steps):

            @pl.when(jnp.logical_not((iz + steps >= 0) & (iz + steps < ngz)))
            def _():
                for k in range(2):
                    mi_in[k, slot] = jnp.zeros(mi_in.shape[2:], jnp.float32)

        q = matrix()
        for i, (_, plane_) in enumerate(shifts(lambda j, k: q[k][j])):
            FC[i] = plane_
        for i, (_, plane_) in enumerate(shifts(lambda j, k: q[j][k])):
            FC[5 + i] = plane_
        strength = jnp.full(plane, strengths[0], jnp.float32)
        for j in (1, 2):
            strength = jnp.where(part(j), strengths[j], strength)
        FC[10] = strength

    own = row < 4

    def far_first(k):
        for side in range(2):

            @pl.when(far[side])
            def _():
                if k == 0:
                    for i in range(2):
                        kept_copy(side, i).wait()
                        far_copy(side, i).wait_recv()
                else:
                    for i in range(4):
                        line_copy(side, i).wait()

        def far_diagonal(z, carry):
            ids_tile, bound = CX[k, z], BX[k, z]
            ids = jnp.where(
                own,
                jnp.broadcast_to(ids_tile[0:1, :], plane),
                jnp.broadcast_to(ids_tile[4:5, :], plane),
            )
            edge = jnp.where(
                own, jnp.broadcast_to(bound[0:1, :], plane), jnp.broadcast_to(bound[4:5, :], plane)
            )
            sigma = jnp.zeros(plane, jnp.float32)
            for kind in range(kinds):
                sigma = jnp.where(ids == kind, conductance[kind], sigma)
            FT[k, z, 0] = 2.0 + 4.0 * coupling + penalty * edge.astype(jnp.float32)
            FT[k, z, 1] = sigma * FC[10]
            return carry

        loop(0, depth, far_diagonal, 0, 4)

        def far_pivots(z, carry):
            p, q = carry
            d, f = get(FT, k, z), get(FT, k, depth - 1 - z)
            p = inv((d[0] - p[0], d[1] - p[1]))
            q = inv((f[0] - q[0], f[1] - q[1]))
            put(FP, p, k, z)
            put(FPHI, q, k, depth - 1 - z)
            return p, q

        loop(0, depth, far_pivots, ((zero, zero), (zero, zero)), 2)
        one = jnp.ones(plane, jnp.float32)

        def far_columns(z, carry):
            down, up = carry
            back = depth - 1 - z
            down = mul(get(FPHI, k, z), down)
            up = mul(get(FP, k, back), up)
            put(FPHI, down, k, z)
            put(FPSI, up, k, back)
            return down, up

        loop(0, depth, far_columns, ((one, zero), (one, zero)), 2)
        ends_ = (get(FPHI, k, 0), get(FPSI, k, depth - 1), get(FPSI, k, 0))
        for i, value in enumerate(ends_):
            mi_out[k, 2 * i] = value[0]
            mi_out[k, 2 * i + 1] = value[1]
        to_all(k, pl.ds(0, 6))

    def far_solve(k, rhs):
        turned_by = [(d, FC[i]) for i, d in enumerate((-2, -1, 0, 1, 2))]

        def far_sums(z, carry):
            first, last = carry
            t = tuple(
                mix(turned_by, jnp.where(used, coupling * rhs(z, p), zero)) for p in range(2)
            )
            put(FT, t, k, z)
            return add(first, mul(get(FPHI, k, z), t)), add(last, mul(get(FPSI, k, z), t))

        first, last = loop(0, depth, far_sums, ((zero, zero), (zero, zero)), 4)
        for i, value in enumerate((first, last)):
            mi_out[k, 6 + 2 * i] = value[0]
            mi_out[k, 7 + 2 * i] = value[1]
        to_all(k, pl.ds(6, 4))

        def far_forward(z, m):
            m = mul(get(FP, k, z), add(get(FT, k, z), m))
            put(FT, m, k, z)
            return m

        def far_backward(i, w):
            z = depth - 1 - i
            w = add(get(FT, k, z), mul(get(FP, k, z), w))
            put(FT, w, k, z)
            return w

        loop(0, depth, far_forward, (zero, zero), 4)
        loop(0, depth, far_backward, (zero, zero), 4)

    def far_second():
        for side in range(2):

            @pl.when(far[side])
            def _():
                for i in range(2, 5):
                    far_copy(side, i).wait_recv()

        far_solve(0, lambda z, p: XR[z, p])

    def far_meet(k, take):
        from_all(k)
        block = lambda slot: [(mi_in[k, slot, 2 * i], mi_in[k, slot, 2 * i + 1]) for i in range(5)]
        x = lam = y = mu = (zero, zero)
        for slot in range(3):
            top, bottom, cross, first, last = block(slot)
            det = inv(one_minus(mul(top, lam)))
            x, lam = (
                add(last, mul(cross, mul(det, add(x, mul(lam, first))))),
                add(bottom, mul(mul(cross, cross), mul(det, lam))),
            )
        for slot in (5, 4, 3):
            top, bottom, cross, first, last = block(slot)
            det = inv(one_minus(mul(bottom, mu)))
            y, mu = (
                add(first, mul(cross, mul(det, add(y, mul(mu, last))))),
                add(top, mul(mul(cross, cross), mul(det, mu))),
            )
        top, bottom, cross, first, last = [(mi_out[k, 2 * i], mi_out[k, 2 * i + 1]) for i in range(5)]
        g, h = add(x, mul(lam, first)), add(y, mul(mu, last))
        alpha, beta = one_minus(mul(lam, top)), one_minus(mul(mu, bottom))
        lc, mc = mul(lam, cross), mul(mu, cross)
        both_ = mul(lc, mc)
        all_ = mul(alpha, beta)
        det = inv((all_[0] - both_[0], all_[1] - both_[1]))
        put(far_ends, mul(det, add(mul(g, beta), mul(lc, h))), 0)
        put(far_ends, mul(det, add(mul(h, alpha), mul(mc, g))), 1)
        back_by = [(d, FC[5 + i]) for i, d in enumerate((-2, -1, 0, 1, 2))]

        def far_join(z, carry):
            before, after = get(far_ends, 0), get(far_ends, 1)
            w = add(
                add(get(FT, k, z), mul(get(FPHI, k, z), before)), mul(get(FPSI, k, z), after)
            )
            for p in range(2):
                take(z, p, mix(back_by, w[p]))
            return carry

        loop(0, depth, far_join, 0, 4)

    def far_third():
        def keep(z, p, u):
            FT[0, z, p] = u

        far_meet(0, keep)
        for side in range(2):

            @pl.when(far[side])
            def _():
                early_moved(side).wait_recv()

        def rhs(z, p):
            u = FT[0, z, p]
            beside_ = jnp.where(lane == 0, zero, pltpu.roll(u, 1, 1))
            beside_ += jnp.where(lane == width - 1, zero, pltpu.roll(u, width - 1, 1))
            early = jnp.where(row < 3, FA[z, p], zero)
            return pltpu.roll(u, 4, 0) + jnp.where(own, beside_ + early, zero)

        far_solve(1, rhs)

    def far_last():
        here = row == jnp.where(far[1], rows - 1, 0)
        next_ = row == jnp.where(far[1], rows - 2, 1)

        def give(z, p, u):
            for c in range(3):
                OUT[z, p, c] += jnp.where(
                    here,
                    jnp.broadcast_to(u[c : c + 1, :], plane),
                    jnp.where(next_, jnp.broadcast_to(u[4 + c : 5 + c, :], plane), zero),
                )

        far_meet(1, give)

    loads[PIECES + 2].wait()
    for sweep in range(SWEEPS):
        sums = loop(0, depth, inner, (none, none), 4)
        if sweep == 0:
            near_side(near_lam)
        halves = [(none, none), (none, none)]
        for piece in range(PIECES):
            for side in range(2):

                if sweep == 0 and piece == 0:

                    @pl.when(beside[side])
                    def _():
                        rows_moved(side).wait_recv()

                if sweep:

                    @pl.when(beside[side])
                    def _():
                        halo_copy(sweep, side, piece).wait_recv()

                for tile in tiles[piece * len(tiles) // PIECES : (piece + 1) * len(tiles) // PIECES]:
                    halves[side] = outer(sweep, side, tile, halves[side])
        for side in range(2):
            here = row == (0 if side == 0 else rows - 1)
            sums = tuple(
                add(
                    sums[end],
                    tuple(
                        jnp.where(here[None], jnp.sum(part, axis=1, keepdims=True), 0.0)
                        for part in halves[side][end]
                    ),
                )
                for end in range(2)
            )
        put(ends, sums[0], 0)
        put(ends, sums[1], 1)

        near_side(functools.partial(own_sum, sweep))
        if sweep == 0:
            pl.when(is_far)(far_begin)
            far_side(far_lam)
        far_side(functools.partial(own_sum, sweep))
        near_side(functools.partial(pass_chain, sweep))

        def forward(z, m):
            given = []
            for p in range(2):
                edges = []
                for j in range(3):
                    above = jnp.broadcast_to(EH[0, p, j, pl.ds(z, 1), :], plane)
                    below = jnp.broadcast_to(EH[1, p, j, pl.ds(z, 1), :], plane)
                    edges.append(
                        jnp.where(row == 0, above, zero) + jnp.where(row == rows - 1, below, zero)
                    )
                given.append(T[z, p] + jnp.stack(edges))
            m = mul(get(PH, z), add(given, m))
            put(T, m, z)
            return m

        def backward(k, w):
            z = depth - 1 - k
            w = add(get(T, z), mul(get(PH, z), w))
            put(T, w, z)
            if sweep < SWEEPS - 1:
                pack(ET.at[0], ET.at[1], z, [w[i // 3][i % 3] for i in range(6)])
            return w

        loop(0, depth, forward, none, 4)
        loop(0, depth, backward, none, 4)
        if sweep:
            pl.when(is_far)(far_third)
        if sweep == 0:
            far_side(last_lam)
            for side in range(2):
                lam = get(coef, 10 + side)
                away = tuple(
                    jnp.stack([lam_out[1 - side, j, p] for j in range(3)]) for p in range(2)
                )
                det = inv(one_minus(mul(lam, away)))
                put(coef, det, 6 + side)
                put(coef, mul(det, lam), 4 + side)
        far_side(functools.partial(pass_chain, sweep))

        for side in range(2):
            for j in range(3):
                arrived = (value_in[side, j, 0], value_in[side, j, 1])
                other = (ch_out[sweep, 1 - side, j, 0], ch_out[sweep, 1 - side, j, 1])
                value = add(
                    mul((coef[6 + side, 0, j], coef[6 + side, 1, j]), arrived),
                    mul((coef[4 + side, 0, j], coef[4 + side, 1, j]), other),
                )
                near[side, 0, j] = value[0]
                near[side, 1, j] = value[1]

        final = sweep == SWEEPS - 1

        def join_edge(side, tile):
            q = matrix()
            r = 0 if side == 0 else rows - 1
            w = [ET[side, p, :, tile] for p in range(2)]
            for end, column in ((0, EPHI), (1, EPSI)):
                entry = [
                    jnp.broadcast_to(near[end, p, :, r : r + 1, :], (3,) + plane)
                    for p in range(2)
                ]
                w = add(w, mul([column[side, p, :, tile] for p in range(2)], entry))
            for p in range(2):
                for c in range(3):
                    halo_out[sweep + 1, 1 - side, p, c, tile] = (
                        q[c][0] * w[p][0] + q[c][1] * w[p][1] + q[c][2] * w[p][2]
                    )

        if not final:
            for piece in range(PIECES):
                for tile in tiles[piece * len(tiles) // PIECES : (piece + 1) * len(tiles) // PIECES]:
                    for side in range(2):
                        join_edge(side, tile)
                send_halo(sweep + 1, piece)
            for side in range(2):

                @pl.when(far[side])
                def _():
                    for p in range(2):
                        for c in range(3):
                            early_copy(side, p, c).start()


        def join(z, carry):
            q = matrix()
            before, after = get(near, 0), get(near, 1)
            w = add(add(get(T, z), mul(get(PHI, z), before)), mul(get(PSI, z), after))
            values = []
            for p in range(2):
                for c in range(3):
                    values.append(q[c][0] * w[p][0] + q[c][1] * w[p][1] + q[c][2] * w[p][2])
            target = OUT if final else U
            for i in range(6):
                target[z, i // 3, i % 3] = values[i]
            return carry

        if not final:
            for side in range(2):

                @pl.when(far[side])
                def _():
                    for i in range(5):
                        far_copy(side, i).wait_send()
                    for i in range(2, 5):
                        kept_copy(side, i).wait()

                @pl.when(beside[1 - side])
                def _():
                    rows_moved(side).wait_send()

        loop(0, depth, join, 0, 4)

        if not final:

            @pl.when(is_far)
            def _():
                far_setup()
                far_first(0)
                far_second()
                far_first(1)

        else:
            pl.when(is_far)(far_last)

    @pl.when(is_far)
    def _():
        for k in range(2):
            for_all(lambda steps: mi_copy(k, steps).wait_send())

    for side in range(2):

        @pl.when(beside[1 - side])
        def _():
            for sweep in range(1, SWEEPS):
                for piece in range(PIECES):
                    halo_copy(sweep, side, piece).wait_send()

        @pl.when(far[side])
        def _():
            early_moved(side).wait_send()

        sends = both(even[side], onward[side] >= 1)

        @pl.when(sends)
        def _():
            chain_copy(
                info_out.at[side, 0:3],
                info_in.at[side, 0:3],
                tip_send.at[side],
                info_recv.at[side],
                side,
                1,
            ).wait_send()
            for sweep in range(SWEEPS):
                own_copy(sweep, side, whole).wait_send()

        @pl.when(both(sends, place[side] > 0))
        def _():
            info_copy(side).wait_send()

        for steps in (2, 1):

            @pl.when(both(odd[side], onward[side] >= steps))
            def _():
                lam_copy(side, steps, whole).wait_send()
                for sweep in range(SWEEPS):
                    x_copy(sweep, side, steps, whole).wait_send()


def local(ngz, nxy, field, source, classes, boundary, conductance, angles, strengths):
    depth, _, _, rows, width = field.shape
    f32 = jnp.float32
    block = pltpu.VMEM(field.shape, f32)
    flat = (depth, rows, width)
    line = (2, 3, rows, width)
    pair = (2, rows, width)
    edge = (2, 2, 3, depth, width)
    narrow = pltpu.VMEM((depth, 2, rows, width), f32)
    lines = pltpu.VMEM((2, depth, 2, rows, width), f32)
    dma = pltpu.SemaphoreType.DMA
    hbm = pl.BlockSpec(memory_space=pl.ANY)
    smem = pl.BlockSpec(memory_space=pltpu.SMEM)
    return pl.pallas_call(
        functools.partial(relax, ngz, nxy),
        out_shape=pltpu.VMEM(field.shape, f32),
        in_specs=[hbm] * 4 + [smem] * 3,
        out_specs=pl.BlockSpec(memory_space=pltpu.VMEM),
        scratch_shapes=[
            block,
            block,
            pltpu.VMEM(flat, jnp.int32),
            pltpu.VMEM(flat, jnp.int32),
            pltpu.VMEM(flat, f32),
            pltpu.VMEM(flat, f32),
            block,
            block,
            block,
            block,
            pltpu.VMEM((3, 3, rows, 128), f32),
            pltpu.VMEM(edge, f32),
            pltpu.VMEM(edge, f32),
            pltpu.VMEM(edge, f32),
            pltpu.VMEM(edge, f32),
            pltpu.VMEM((2,) + line, f32),
            pltpu.VMEM((14,) + line, f32),
            pltpu.VMEM((2,) + line, f32),
            pltpu.VMEM((SWEEPS,) + edge, f32),
            pltpu.VMEM((SWEEPS,) + edge, f32),
            pltpu.VMEM((2, 3) + pair, f32),
            pltpu.VMEM((2, 9) + pair, f32),
            pltpu.VMEM((2, 9) + pair, f32),
            pltpu.VMEM((2, 3) + pair, f32),
            pltpu.VMEM((2, 3) + pair, f32),
            pltpu.VMEM((SWEEPS, 2, 3) + pair, f32),
            pltpu.VMEM((SWEEPS, 2, 3) + pair, f32),
            pltpu.VMEM((SWEEPS, 2, 3) + pair, f32),
            pltpu.VMEM((SWEEPS, 2, 3) + pair, f32),
            narrow,
            narrow,
            pltpu.VMEM((2,) + flat, jnp.int32),
            pltpu.VMEM((2,) + flat, jnp.int32),
            lines,
            lines,
            lines,
            lines,
            pltpu.VMEM((11, rows, width), f32),
            pltpu.VMEM((2,) + pair, f32),
            pltpu.VMEM((2, 6, 10, rows, width), f32),
            pltpu.VMEM((2, 10, rows, width), f32),
            dma((PIECES + 3,)),
            dma((2, PIECES)),
            dma((2, PIECES)),
            dma((2,)),
            dma((2, 3)),
            dma((2,)),
            dma((2,)),
            dma((2, 2)),
            dma((2, 3)),
            dma((SWEEPS, 2)),
            dma((SWEEPS, 2, 3)),
            dma((SWEEPS, 2, 2)),
            dma((SWEEPS, 2, 3)),
            dma((9,)),
            dma((5,)),
            dma((5,)),
            pltpu.SemaphoreType.REGULAR,
            dma((2,)),
            dma((2,)),
            dma(()),
            dma(()),
            dma((2, 6)),
            dma((2, 6)),
        ],
        compiler_params=pltpu.CompilerParams(collective_id=0, has_side_effects=True, vmem_limit_bytes=VMEM_LIMIT),
    )(field, source, classes, boundary, conductance, angles, strengths)


def solution(mesh):
    in_specs = (
        P("gz", None, None, "xy", None),
        P("gz", None, None, "xy", None),
        P("gz", "xy", None),
        P("gz", "xy", None),
        P(),
        P(),
        P(),
    )
    out_specs = P("gz", None, None, "xy", None)
    body = functools.partial(local, mesh.shape["gz"], mesh.shape["xy"])
    return jax.shard_map(body, mesh=mesh, in_specs=in_specs, out_specs=out_specs, check_vma=False)
```

```python
import functools

import jax
import jax.numpy as jnp
from jax import lax
from jax.experimental import pallas as pl
from jax.experimental.pallas import tpu as pltpu
from jax.sharding import PartitionSpec as P

SWEEPS = 2
PIECES = 2
VMEM_LIMIT = 62 * 2**20

coupling = 0.1
penalty = 4.0


def mul(a, b):
    return (a[0] * b[0] - a[1] * b[1], a[0] * b[1] + a[1] * b[0])


def add(a, b):
    return (a[0] + b[0], a[1] + b[1])


def inv(a):
    weight = 1.0 / (a[0] * a[0] + a[1] * a[1])
    return (a[0] * weight, -a[1] * weight)


def one_minus(a):
    return (1.0 - a[0], -a[1])


def get(ref, *at):
    return (ref[at + (0,)], ref[at + (1,)])


def put(ref, value, *at):
    ref[at + (0,)] = value[0]
    ref[at + (1,)] = value[1]


def loop(low, high, body, carry, by):
    by = by if (high - low) % by == 0 else 1

    def several(k, carry):
        for i in range(by):
            carry = body(low + k * by + i, carry)
        return carry

    return lax.fori_loop(0, (high - low) // by, several, carry)


def rotation(angles, shape):
    cos = [jnp.cos(jnp.full(shape, angles[i], jnp.float32)) for i in range(3)]
    sin = [jnp.sin(jnp.full(shape, angles[i], jnp.float32)) for i in range(3)]
    (ca, cb, cc), (sa, sb, sc) = cos, sin
    left = [[ca * cb, -sa, ca * sb], [sa * cb, ca, sa * sb], [-sb, jnp.zeros_like(cb), cb]]
    return [[row[0] * cc + row[1] * sc, row[1] * cc - row[0] * sc, row[2]] for row in left]


def relax(
    ngz,
    nxy,
    field,
    source,
    classes,
    boundary,
    conductance,
    angles,
    strengths,
    OUT,
    U,
    S,
    C,
    B,
    SG,
    DR,
    PH,
    PHI,
    PSI,
    T,
    QM,
    EPHI,
    EPSI,
    EH,
    ET,
    ends,
    coef,
    near,
    halo_out,
    halo_in,
    value_in,
    info_in,
    info_out,
    lam_in,
    lam_out,
    own_in,
    own_out,
    ch_in,
    ch_out,
    XR,
    FA,
    CX,
    BX,
    FP,
    FPHI,
    FPSI,
    FT,
    FC,
    far_ends,
    mi_in,
    mi_out,
    in_sems,
    halo_send,
    halo_recv,
    tip_send,
    tip_recv,
    info_send,
    info_recv,
    lam_send,
    lam_recv,
    own_send,
    own_recv,
    ch_send,
    ch_recv,
    far_local,
    far_send,
    far_recv,
    near_ready,
    row_send,
    row_recv,
    early_send,
    early_recv,
    mi_send,
    mi_recv,
):
    ix, iz = lax.axis_index("xy"), lax.axis_index("gz")
    depth, _, _, rows, width = U.shape
    kinds = conductance.shape[0]
    plane = (rows, width)
    has = {
        ("xy", 0): ix > 0,
        ("xy", 1): ix < nxy - 1,
    }
    where_is = {
        ("xy", 0): ix - 1,
        ("xy", 1): ix + 1,
    }
    middle = nxy // 2
    far = (ix == middle, ix == middle - 1)
    is_far = jnp.logical_or(far[0], far[1])
    not_far = jnp.logical_not(is_far)
    helps = (ix == middle + 1, ix == middle - 2)
    helper = jnp.logical_or(helps[0], helps[1])
    pair = jnp.where(far[0], ix + 1, ix - 1)
    beside = [jnp.logical_and(has["xy", side], jnp.logical_not(far[side])) for side in range(2)]
    for steps in (1, 2):
        has["gz", -steps] = iz >= steps
        has["gz", steps] = iz < ngz - steps
        where_is["gz", -steps] = iz - steps
        where_is["gz", steps] = iz + steps
    signals = {}
    for key, there in has.items():
        signals[key] = jnp.logical_and(there, not_far)
        if key[0] == "xy":
            signals[key] = jnp.logical_and(signals[key], jnp.logical_not(helps[key[1]]))
    count = sum(there.astype(jnp.int32) for there in signals.values())
    count += ngz * helper.astype(jnp.int32)
    zs = depth // PIECES
    spans = [pl.ds(piece * zs, zs) for piece in range(PIECES)]
    moves = [(field.at[span], U.at[span]) for span in spans]
    moves += [(classes, C), (boundary, B), (source, S)]
    loads = [
        pltpu.make_async_copy(src, dst, in_sems.at[i]) for i, (src, dst) in enumerate(moves)
    ]
    for load in loads[PIECES : PIECES + 2] + loads[:PIECES] + loads[PIECES + 2 :]:
        load.start()

    barrier = pltpu.get_barrier_semaphore()
    for key, there in signals.items():

        @pl.when(there)
        def _():
            pl.semaphore_signal(
                barrier,
                inc=1,
                device_id={key[0]: where_is[key]},
                device_id_type=pl.DeviceIdType.MESH,
            )


    @pl.when(is_far)
    def _():
        for g in range(ngz):
            pl.semaphore_signal(
                barrier,
                inc=1,
                device_id={"xy": pair, "gz": g},
                device_id_type=pl.DeviceIdType.MESH,
            )
        pl.semaphore_signal(
            barrier,
            inc=1,
            device_id={"xy": jnp.where(far[0], ix - 1, ix + 1)},
            device_id_type=pl.DeviceIdType.MESH,
        )

    def remote(src, dst, send, recv, key):
        return pltpu.make_async_remote_copy(
            src_ref=src,
            dst_ref=dst,
            send_sem=send,
            recv_sem=recv,
            device_id={key[0]: where_is[key]},
            device_id_type=pl.DeviceIdType.MESH,
        )

    def halo_copy(sweep, side, piece):
        span = pl.ds(piece * zs, zs)
        return remote(
            halo_out.at[sweep, side, :, :, span],
            halo_in.at[sweep, side, :, :, span],
            halo_send.at[side, piece],
            halo_recv.at[side, piece],
            ("xy", 1 - side),
        )

    def send_halo(sweep, piece):
        for side in range(2):

            @pl.when(beside[1 - side])
            def _():
                halo_copy(sweep, side, piece).start()

    def early_copy(side, p, c):
        return remote(
            halo_out.at[1, 1 - side, p, c],
            FA.at[:, p, c, :],
            early_send,
            early_recv,
            ("xy", side),
        )

    def early_moved(side):
        return remote(
            halo_out.at[1, 1 - side],
            halo_out.at[1, 1 - side],
            early_send,
            early_recv,
            ("xy", side),
        )

    def row_copy(side, p, c):
        return remote(
            U.at[:, p, c, 0 if side else rows - 1, :],
            halo_in.at[0, side, p, c],
            row_send.at[side],
            row_recv.at[side],
            ("xy", 1 - side),
        )

    row_copies = lambda side: [row_copy(side, p, c) for p in range(2) for c in range(3)]
    rows_moved = lambda side: remote(
        halo_in.at[0, side],
        halo_in.at[0, side],
        row_send.at[side],
        row_recv.at[side],
        ("xy", 1 - side),
    )

    def pack(first, last, z, values):
        for i in range(6):
            at = (i // 3, i % 3, pl.ds(z, 1), slice(None))
            first[at] = values[i][:1, :]
            last[at] = values[i][rows - 1 :, :]

    for side in range(2):

        for sweep in range(SWEEPS):

            @pl.when(jnp.logical_not(beside[side]))
            def _():
                halo_in[sweep, side] = jnp.zeros(halo_in.shape[2:], jnp.float32)

        @pl.when((iz if side == 0 else ngz - 1 - iz) < 2)
        def _():
            for part in range(3, 9):
                info_in[side, part] = jnp.zeros(info_in.shape[2:], jnp.float32)
            lam_in[side] = jnp.zeros(lam_in.shape[1:], jnp.float32)
            for sweep in range(SWEEPS):
                ch_in[sweep, side] = jnp.zeros(ch_in.shape[2:], jnp.float32)

    loads[PIECES].wait()
    loads[PIECES + 1].wait()

    def diagonal(z, carry):
        ids = C[z]
        sigma = jnp.zeros(plane, jnp.float32)
        for kind in range(kinds):
            sigma = jnp.where(ids == kind, conductance[kind], sigma)
        SG[z] = sigma
        DR[z] = 2.0 + 4.0 * coupling + penalty * B[z].astype(jnp.float32)
        return carry

    loop(0, depth, diagonal, 0, 4)

    def diag(z):
        real = jnp.broadcast_to(DR[z][None], (3,) + plane)
        sigma = SG[z]
        return real, jnp.stack([sigma * strengths[j] for j in range(3)])

    none = (jnp.zeros((3,) + plane, jnp.float32),) * 2

    def pivots(k, carry):
        p, q = carry
        z, back = k, depth - 1 - k
        d, f = diag(z), diag(back)
        p = inv((d[0] - p[0], d[1] - p[1]))
        q = inv((f[0] - q[0], f[1] - q[1]))
        put(PH, p, z)
        put(PHI, q, back)
        return p, q

    loop(0, depth, pivots, (none, none), 2)
    ones = (jnp.ones((3,) + plane, jnp.float32), none[0])

    def columns(k, carry):
        down, up = carry
        z, back = k, depth - 1 - k
        down = mul(get(PHI, z), down)
        up = mul(get(PH, back), up)
        put(PHI, down, z)
        put(PSI, up, back)
        return down, up

    loop(0, depth, columns, (ones, ones), 2)
    for piece in range(PIECES):
        loads[piece].wait()

    @pl.when(not_far)
    def _():
        pl.semaphore_wait(barrier, count)

    @pl.when(helper)
    def _():
        pl.semaphore_signal(
            near_ready,
            inc=1,
            device_id={"xy": jnp.where(helps[0], ix - 1, ix + 1)},
            device_id_type=pl.DeviceIdType.MESH,
        )

    @pl.when(is_far)
    def _():
        pl.semaphore_wait(near_ready, 1)

    for side in range(2):

        @pl.when(beside[1 - side])
        def _():
            for copy in row_copies(side):
                copy.start()

    LEFT, RIGHT = 0, 1
    tip = (lambda: get(PHI, 0), lambda: get(PSI, depth - 1))
    across = lambda: get(PSI, 0)

    place = (iz, ngz - 1 - iz)
    even = [lax.rem(k, 2) == 0 for k in place]
    odd = [lax.rem(k, 2) == 1 for k in place]
    onward = [ngz - 1 - k for k in place]

    def to(side, steps):
        return {"gz": iz + steps if side == LEFT else iz - steps}

    def chain_copy(src, dst, send, recv, side, steps):
        return pltpu.make_async_remote_copy(
            src_ref=src,
            dst_ref=dst,
            send_sem=send,
            recv_sem=recv,
            device_id=to(side, steps),
            device_id_type=pl.DeviceIdType.MESH,
        )

    whole = slice(None)
    way = (lambda side: 0) if ngz == 4 else (lambda side: side)

    def tip_copy(side, j):
        return chain_copy(
            info_out.at[side, j],
            info_in.at[side, j],
            tip_send.at[way(side)],
            tip_recv.at[way(side), j],
            side,
            1,
        )

    def info_copy(side):
        return chain_copy(
            info_out.at[side, 3:9],
            info_in.at[side, 3:9],
            info_send.at[way(side)],
            info_recv.at[way(side)],
            side,
            1,
        )

    def lam_copy(side, steps, j):
        return chain_copy(
            lam_out.at[side, j],
            lam_in.at[side, j],
            lam_send.at[way(side), steps - 1],
            lam_recv.at[way(side), j],
            side,
            steps,
        )

    def own_copy(sweep, side, j):
        return chain_copy(
            own_out.at[sweep, side, j],
            own_in.at[sweep, side, j],
            own_send.at[sweep, way(side)],
            own_recv.at[sweep, way(side), j],
            side,
            1,
        )

    def x_copy(sweep, side, steps, j):
        return chain_copy(
            ch_out.at[sweep, side, j],
            ch_in.at[sweep, side, j],
            ch_send.at[sweep, way(side), steps - 1],
            ch_recv.at[sweep, way(side), j],
            side,
            steps,
        )


    both = jnp.logical_and

    def send_info(side):
        sends = both(even[side], onward[side] >= 1)
        parts = (tip[1 - side](), tip[side](), across())
        for part in range(3):
            for j in range(3):
                for p in range(2):
                    info_out[side, part * 3 + j, p] = parts[part][p][j]
            if part == 0:

                @pl.when(sends)
                def _():
                    for j in range(3):
                        tip_copy(side, j).start()

        @pl.when(both(sends, place[side] > 0))
        def _():
            info_copy(side).start()

    def pass_lam(side):
        @pl.when(both(odd[side], place[side] >= 2))
        def _():
            info_copy(side).wait_recv()

        for j in range(3):

            @pl.when(odd[side])
            def _():
                tip_copy(side, j).wait_recv()

            @pl.when(place[side] >= 2)
            def _():
                lam_copy(side, 1, j).wait_recv()

            tips = [(info_in[side, 3 * k + j, 0], info_in[side, 3 * k + j, 1]) for k in range(3)]
            given = (lam_in[side, j, 0], lam_in[side, j, 1])

            @pl.when(odd[side])
            def _():
                skip = mul(tips[2], inv(one_minus(mul(tips[1], given))))
                lam = add(tips[0], mul(tips[2], mul(skip, given)))
                for p in range(2):
                    coef[8 + side, p, j] = skip[p]
                    coef[10 + side, p, j] = lam[p]

            @pl.when(even[side])
            def _():
                for p in range(2):
                    coef[10 + side, p, j] = given[p]

            of = lambda pair: (pair[0][j], pair[1][j])
            lam = (coef[10 + side, 0, j], coef[10 + side, 1, j])
            kappa = mul(of(across()), inv(one_minus(mul(of(tip[side]()), lam))))
            over = mul(kappa, lam)
            value = add(of(tip[1 - side]()), mul(of(across()), over))
            for p in range(2):
                coef[side, p, j] = kappa[p]
                coef[2 + side, p, j] = over[p]
                lam_out[side, j, p] = value[p]

            @pl.when(both(odd[side], onward[side] >= 1))
            def _():
                lam_copy(side, 1, j).start()

        @pl.when(both(odd[side], onward[side] >= 2))
        def _():
            for j in range(3):
                lam_copy(side, 2, j).start()

    def own_base(side, j):
        return add(
            (ends[1 - side, 0, j], ends[1 - side, 1, j]),
            mul(
                (coef[2 + side, 0, j], coef[2 + side, 1, j]),
                (ends[side, 0, j], ends[side, 1, j]),
            ),
        )

    def own_sum(sweep, side):
        for j in range(3):
            base = own_base(side, j)
            for p in range(2):
                own_out[sweep, side, j, p] = base[p]

            @pl.when(both(even[side], onward[side] >= 1))
            def _():
                own_copy(sweep, side, j).start()

    def pass_chain(sweep, side):
        for j in range(3):
            base = own_base(side, j)

            @pl.when(odd[side])
            def _():
                own_copy(sweep, side, j).wait_recv()

            @pl.when(place[side] >= 2)
            def _():
                x_copy(sweep, side, 1, j).wait_recv()

            given = (ch_in[sweep, side, j, 0], ch_in[sweep, side, j, 1])

            @pl.when(odd[side])
            def _():
                own = (own_in[sweep, side, j, 0], own_in[sweep, side, j, 1])
                x = add(own, mul((coef[8 + side, 0, j], coef[8 + side, 1, j]), given))
                for p in range(2):
                    value_in[side, j, p] = x[p]

            @pl.when(even[side])
            def _():
                for p in range(2):
                    value_in[side, j, p] = given[p]

            x = (value_in[side, j, 0], value_in[side, j, 1])
            result = add(base, mul((coef[side, 0, j], coef[side, 1, j]), x))
            for p in range(2):
                ch_out[sweep, side, j, p] = result[p]

            @pl.when(both(odd[side], onward[side] >= 2))
            def _():
                x_copy(sweep, side, 2, j).start()

        @pl.when(both(odd[side], onward[side] >= 1))
        def _():
            for j in range(3):
                x_copy(sweep, side, 1, j).start()

    left_first = iz * 2 < ngz - 1

    def near_side(run):
        @pl.when(left_first)
        def _():
            run(LEFT)

        @pl.when(jnp.logical_not(left_first))
        def _():
            run(RIGHT)

    def far_side(run):
        @pl.when(left_first)
        def _():
            run(RIGHT)

        @pl.when(jnp.logical_not(left_first))
        def _():
            run(LEFT)

    def far_source(side, i):
        edge = pl.ds(rows - 1 if side else 0, 1)
        return (C.at[:, edge, :], B.at[:, edge, :])[i] if i < 2 else U.at[:, :, i - 2, edge, :]

    def far_target(i, first):
        at = pl.ds(first if i < 2 else first + i - 2, 1)
        return (CX.at[0, :, at, :], BX.at[0, :, at, :])[i] if i < 2 else XR.at[:, :, at, :]

    def far_copy(side, i):
        return pltpu.make_async_remote_copy(
            src_ref=far_source(side, i),
            dst_ref=far_target(i, 4 if i < 2 else 0),
            send_sem=far_send.at[min(i, 2)],
            recv_sem=far_recv.at[min(i, 2)],
            device_id={"xy": ix + 1 if side else ix - 1},
            device_id_type=pl.DeviceIdType.MESH,
        )

    def kept_copy(side, i):
        return pltpu.make_async_copy(
            far_source(side, i), far_target(i, 0 if i < 2 else 4), far_local.at[min(i, 2)]
        )

    def field_moved(side):
        return pltpu.make_async_remote_copy(
            src_ref=XR.at[:, :, 0:3, :],
            dst_ref=XR.at[:, :, 0:3, :],
            send_sem=far_send.at[2],
            recv_sem=far_recv.at[2],
            device_id={"xy": ix + 1 if side else ix - 1},
            device_id_type=pl.DeviceIdType.MESH,
        )

    def field_kept():
        return pltpu.make_async_copy(XR.at[:, :, 4:7, :], XR.at[:, :, 4:7, :], far_local.at[2])

    def lines_kept(i):
        ref = (CX, BX)[i].at[1, :, 0:2, :]
        return pltpu.make_async_copy(ref, ref, far_local.at[3 + i])

    def line_copy(side, i):
        first = rows - 1 if side else 0
        edge = pl.ds(first if i < 2 else (first - 1 if side else first + 1), 1)
        at = pl.ds(0 if i < 2 else 4, 1)
        return pltpu.make_async_copy(
            (C, B)[i % 2].at[:, edge, :], (CX, BX)[i % 2].at[1, :, at, :], far_local.at[3 + i % 2]
        )

    def far_begin():
        pl.semaphore_wait(barrier, 1)
        for side in range(2):

            @pl.when(far[side])
            def _():
                for i in range(5):
                    far_copy(side, i).start()
                for i in range(5):
                    kept_copy(side, i).start()
                for i in range(4):
                    line_copy(side, i).start()

    def near_lam(side):
        pl.when(place[side] < 2)(functools.partial(pass_lam, side))

    def far_lam(side):
        pl.when(place[side] == 2)(functools.partial(pass_lam, side))

    def last_lam(side):
        pl.when(place[side] >= 3)(functools.partial(pass_lam, side))

    near_side(send_info)
    far_side(send_info)

    angle_matrix = rotation(angles, (rows, 128))
    for c in range(3):
        for j in range(3):
            QM[c, j] = angle_matrix[c][j]

    def matrix():
        return [
            [jnp.concatenate([QM[c, j]] * (width // 128), axis=1) for j in range(3)]
            for c in range(3)
        ]

    def pack_columns(z, carry):
        for src, dst in ((PHI, EPHI), (PSI, EPSI)):
            pack(dst.at[0], dst.at[1], z, [src[z, i // 3, i % 3] for i in range(6)])
        return carry

    loop(0, depth, pack_columns, 0, 4)

    row = lax.broadcasted_iota(jnp.int32, plane, 0)
    lane = lax.broadcasted_iota(jnp.int32, plane, 1)
    zero = jnp.zeros(plane, jnp.float32)

    def turn(q, driven):
        return [
            jnp.stack(
                [
                    q[0][j] * driven[p][0] + q[1][j] * driven[p][1] + q[2][j] * driven[p][2]
                    for j in range(3)
                ]
            )
            for p in range(2)
        ]

    def inner(z, carry):
        first, last = carry
        q = matrix()
        driven = []
        for p in range(2):
            of = []
            for c in range(3):
                u = U[z, p, c]
                around = jnp.where(lane == 0, zero, pltpu.roll(u, 1, 1))
                around += jnp.where(lane == width - 1, zero, pltpu.roll(u, width - 1, 1))
                around += jnp.where(row == 0, zero, pltpu.roll(u, 1, 0))
                around += jnp.where(row == rows - 1, zero, pltpu.roll(u, rows - 1, 0))
                of.append(S[z, p, c] + coupling * around)
            driven.append(of)
        turned = turn(q, driven)
        put(T, turned, z)
        return add(first, mul(get(PHI, z), turned)), add(last, mul(get(PSI, z), turned))

    tiles = [pl.ds(z, rows) for z in range(0, depth, rows)]

    def outer(sweep, side, tile, carry):
        first, last = carry
        q = matrix()
        turned = turn(
            q,
            [[coupling * halo_in[sweep, side, p, c, tile] for c in range(3)] for p in range(2)],
        )
        for p in range(2):
            EH[side, p, :, tile] = turned[p]
        phi = [EPHI[side, p, :, tile] for p in range(2)]
        psi = [EPSI[side, p, :, tile] for p in range(2)]
        return add(first, mul(phi, turned)), add(last, mul(psi, turned))

    third = lax.rem(row, 4)
    part = lambda k: third == k
    used = third < 3

    def mi_copy(k, steps, parts):
        slot = steps + 3 if steps < 0 else steps + 2
        return pltpu.make_async_remote_copy(
            src_ref=mi_out.at[k, parts],
            dst_ref=mi_in.at[k, 5 - slot, parts],
            send_sem=mi_send.at[slot],
            recv_sem=mi_recv.at[0 if k == whole else k, 5 - slot],
            device_id={"gz": iz + steps},
            device_id_type=pl.DeviceIdType.MESH,
        )

    all_steps = (-3, -2, -1, 1, 2, 3)
    at_end = lambda k: jnp.logical_or(k == 0, k == ngz - 1)

    def for_all(of, act):
        for steps in all_steps:
            there = (iz + steps >= 0) & (iz + steps < ngz)
            edge_ = at_end(iz + steps * of)

            @pl.when(jnp.logical_and(there, edge_))
            def _():
                act(steps, True)

            @pl.when(jnp.logical_and(there, jnp.logical_not(edge_)))
            def _():
                act(steps, False)

    def to_all(k, first):
        def act(steps, ends_only):
            if not ends_only:
                parts = pl.ds(first, 4 if first else 6)
            else:
                parts = pl.ds(first + (2 if steps > 0 else 0), 2)
            mi_copy(k, steps, parts).start()

        for_all(0, act)

    def moved(ends_only):
        return pl.ds(0, 4 if ends_only else 10)

    def from_all(k):
        for_all(1, lambda steps, e: mi_copy(k, -steps, moved(e)).wait_recv())

    def shifts(of):
        planes = []
        for d in (-2, -1, 0, 1, 2):
            plane_ = zero
            for j in range(3):
                if 0 <= j + d <= 2:
                    plane_ = jnp.where(part(j), of(j, j + d), plane_)
            planes.append((d, plane_))
        return planes

    def mix(planes, x):
        total = None
        for d, plane_ in planes:
            term = plane_ * (x if d == 0 else pltpu.roll(x, (rows - d) % rows, 0))
            total = term if total is None else total + term
        return total

    def far_clear():
        none_ = jnp.zeros((2,) + plane, jnp.float32)
        for slot, steps in enumerate(all_steps):
            there = (iz + steps >= 0) & (iz + steps < ngz)

            @pl.when(jnp.logical_not(there))
            def _():
                for k in range(2):
                    for part_ in range(5):
                        mi_in[k, slot, 2 * part_ : 2 * part_ + 2] = none_

            @pl.when(jnp.logical_and(there, at_end(iz + steps)))
            def _():
                for k in range(2):
                    for part_ in (0, 2, 3) if steps < 0 else (1, 2, 4):
                        mi_in[k, slot, 2 * part_ : 2 * part_ + 2] = none_

    def far_setup():
        q = matrix()
        for i, (_, plane_) in enumerate(shifts(lambda j, k: q[k][j])):
            FC[i] = plane_
        for i, (_, plane_) in enumerate(shifts(lambda j, k: q[j][k])):
            FC[5 + i] = plane_
        strength = jnp.full(plane, strengths[0], jnp.float32)
        for j in (1, 2):
            strength = jnp.where(part(j), strengths[j], strength)
        FC[10] = strength

    own = row < 4

    def far_first(k):
        for side in range(2):

            @pl.when(far[side])
            def _():
                if k == 0:
                    for i in range(2):
                        kept_copy(side, i).wait()
                        far_copy(side, i).wait_recv()
                else:
                    for i in range(2):
                        lines_kept(i).wait()

        def far_diagonal(z, carry):
            ids_tile, bound = CX[k, z], BX[k, z]
            ids = jnp.where(
                own,
                jnp.broadcast_to(ids_tile[0:1, :], plane),
                jnp.broadcast_to(ids_tile[4:5, :], plane),
            )
            edge = jnp.where(
                own, jnp.broadcast_to(bound[0:1, :], plane), jnp.broadcast_to(bound[4:5, :], plane)
            )
            sigma = jnp.zeros(plane, jnp.float32)
            for kind in range(kinds):
                sigma = jnp.where(ids == kind, conductance[kind], sigma)
            FT[k, z, 0] = 2.0 + 4.0 * coupling + penalty * edge.astype(jnp.float32)
            FT[k, z, 1] = sigma * FC[10]
            return carry

        loop(0, depth, far_diagonal, 0, 4)

        def far_pivots(z, carry):
            p, q = carry
            d, f = get(FT, k, z), get(FT, k, depth - 1 - z)
            p = inv((d[0] - p[0], d[1] - p[1]))
            q = inv((f[0] - q[0], f[1] - q[1]))
            put(FP, p, k, z)
            put(FPHI, q, k, depth - 1 - z)
            return p, q

        loop(0, depth, far_pivots, ((zero, zero), (zero, zero)), 2)
        one = jnp.ones(plane, jnp.float32)

        def far_columns(z, carry):
            down, up = carry
            back = depth - 1 - z
            down = mul(get(FPHI, k, z), down)
            up = mul(get(FP, k, back), up)
            put(FPHI, down, k, z)
            put(FPSI, up, k, back)
            return down, up

        loop(0, depth, far_columns, ((one, zero), (one, zero)), 2)
        ends_ = (get(FPHI, k, 0), get(FPSI, k, depth - 1), get(FPSI, k, 0))
        for i, value in enumerate(ends_):
            mi_out[k, 2 * i] = value[0]
            mi_out[k, 2 * i + 1] = value[1]

    def send_columns(k):
        to_all(k, 0)

    def far_solve(k, rhs):
        turned_by = [(d, FC[i]) for i, d in enumerate((-2, -1, 0, 1, 2))]

        def far_sums(z, carry):
            first, last = carry
            t = tuple(
                mix(turned_by, jnp.where(used, coupling * rhs(z, p), zero)) for p in range(2)
            )
            put(FT, t, k, z)
            return add(first, mul(get(FPHI, k, z), t)), add(last, mul(get(FPSI, k, z), t))

        first, last = loop(0, depth, far_sums, ((zero, zero), (zero, zero)), 4)
        for i, value in enumerate((first, last)):
            mi_out[k, 6 + 2 * i] = value[0]
            mi_out[k, 7 + 2 * i] = value[1]
        to_all(k, 6)

        def far_forward(z, m):
            m = mul(get(FP, k, z), add(get(FT, k, z), m))
            put(FT, m, k, z)
            return m

        def far_backward(i, w):
            z = depth - 1 - i
            w = add(get(FT, k, z), mul(get(FP, k, z), w))
            put(FT, w, k, z)
            return w

        loop(0, depth, far_forward, (zero, zero), 4)
        loop(0, depth, far_backward, (zero, zero), 4)

    def far_second():
        for side in range(2):

            @pl.when(far[side])
            def _():
                field_moved(side).wait_recv()

        far_solve(0, lambda z, p: XR[z, p])

    def far_meet(k, take):
        from_all(k)
        block = lambda slot: [(mi_in[k, slot, 2 * i], mi_in[k, slot, 2 * i + 1]) for i in range(5)]
        x = lam = y = mu = (zero, zero)
        for slot in range(3):
            top, bottom, cross, first, last = block(slot)
            det = inv(one_minus(mul(top, lam)))
            x, lam = (
                add(last, mul(cross, mul(det, add(x, mul(lam, first))))),
                add(bottom, mul(mul(cross, cross), mul(det, lam))),
            )
        for slot in (5, 4, 3):
            top, bottom, cross, first, last = block(slot)
            det = inv(one_minus(mul(bottom, mu)))
            y, mu = (
                add(first, mul(cross, mul(det, add(y, mul(mu, last))))),
                add(top, mul(mul(cross, cross), mul(det, mu))),
            )
        top, bottom, cross, first, last = [(mi_out[k, 2 * i], mi_out[k, 2 * i + 1]) for i in range(5)]
        g, h = add(x, mul(lam, first)), add(y, mul(mu, last))
        alpha, beta = one_minus(mul(lam, top)), one_minus(mul(mu, bottom))
        lc, mc = mul(lam, cross), mul(mu, cross)
        both_ = mul(lc, mc)
        all_ = mul(alpha, beta)
        det = inv((all_[0] - both_[0], all_[1] - both_[1]))
        put(far_ends, mul(det, add(mul(g, beta), mul(lc, h))), 0)
        put(far_ends, mul(det, add(mul(h, alpha), mul(mc, g))), 1)
        back_by = [(d, FC[5 + i]) for i, d in enumerate((-2, -1, 0, 1, 2))]

        def far_join(z, carry):
            before, after = get(far_ends, 0), get(far_ends, 1)
            w = add(
                add(get(FT, k, z), mul(get(FPHI, k, z), before)), mul(get(FPSI, k, z), after)
            )
            for p in range(2):
                take(z, p, mix(back_by, w[p]))
            return carry

        loop(0, depth, far_join, 0, 4)

    def far_third():
        def keep(z, p, u):
            FT[0, z, p] = u

        far_meet(0, keep)
        for side in range(2):

            @pl.when(far[side])
            def _():
                early_moved(side).wait_recv()

        def rhs(z, p):
            u = FT[0, z, p]
            beside_ = jnp.where(lane == 0, zero, pltpu.roll(u, 1, 1))
            beside_ += jnp.where(lane == width - 1, zero, pltpu.roll(u, width - 1, 1))
            early = jnp.where(row < 3, FA[z, p], zero)
            return pltpu.roll(u, 4, 0) + jnp.where(own, beside_ + early, zero)

        far_solve(1, rhs)

    def far_last():
        here = row == jnp.where(far[1], rows - 1, 0)
        next_ = row == jnp.where(far[1], rows - 2, 1)

        def give(z, p, u):
            for c in range(3):
                OUT[z, p, c] += jnp.where(
                    here,
                    jnp.broadcast_to(u[c : c + 1, :], plane),
                    jnp.where(next_, jnp.broadcast_to(u[4 + c : 5 + c, :], plane), zero),
                )

        far_meet(1, give)

    loads[PIECES + 2].wait()
    for sweep in range(SWEEPS):
        sums = loop(0, depth, inner, (none, none), 4)
        if sweep == 0:
            near_side(near_lam)
        halves = [(none, none), (none, none)]
        for piece in range(PIECES):
            for side in range(2):

                if sweep == 0 and piece == 0:

                    @pl.when(beside[side])
                    def _():
                        rows_moved(side).wait_recv()

                if sweep:

                    @pl.when(beside[side])
                    def _():
                        halo_copy(sweep, side, piece).wait_recv()

                for tile in tiles[piece * len(tiles) // PIECES : (piece + 1) * len(tiles) // PIECES]:
                    halves[side] = outer(sweep, side, tile, halves[side])
        for side in range(2):
            here = row == (0 if side == 0 else rows - 1)
            sums = tuple(
                add(
                    sums[end],
                    tuple(
                        jnp.where(here[None], jnp.sum(part, axis=1, keepdims=True), 0.0)
                        for part in halves[side][end]
                    ),
                )
                for end in range(2)
            )
        put(ends, sums[0], 0)
        put(ends, sums[1], 1)

        near_side(functools.partial(own_sum, sweep))
        if sweep == 0:
            pl.when(is_far)(far_begin)
            far_side(far_lam)
        far_side(functools.partial(own_sum, sweep))
        if sweep:

            @pl.when(is_far)
            def _():
                far_second()
                send_columns(1)

        near_side(functools.partial(pass_chain, sweep))

        def forward(z, m):
            given = []
            for p in range(2):
                edges = []
                for j in range(3):
                    above = jnp.broadcast_to(EH[0, p, j, pl.ds(z, 1), :], plane)
                    below = jnp.broadcast_to(EH[1, p, j, pl.ds(z, 1), :], plane)
                    edges.append(
                        jnp.where(row == 0, above, zero) + jnp.where(row == rows - 1, below, zero)
                    )
                given.append(T[z, p] + jnp.stack(edges))
            m = mul(get(PH, z), add(given, m))
            put(T, m, z)
            return m

        def backward(k, w):
            z = depth - 1 - k
            w = add(get(T, z), mul(get(PH, z), w))
            put(T, w, z)
            if sweep < SWEEPS - 1:
                pack(ET.at[0], ET.at[1], z, [w[i // 3][i % 3] for i in range(6)])
            return w

        loop(0, depth, forward, none, 4)
        loop(0, depth, backward, none, 4)
        if sweep:
            pl.when(is_far)(far_third)
        else:

            @pl.when(is_far)
            def _():
                far_clear()
                far_setup()
                far_first(1)

        if sweep == 0:
            far_side(last_lam)
            for side in range(2):
                lam = get(coef, 10 + side)
                away = tuple(
                    jnp.stack([lam_out[1 - side, j, p] for j in range(3)]) for p in range(2)
                )
                det = inv(one_minus(mul(lam, away)))
                put(coef, det, 6 + side)
                put(coef, mul(det, lam), 4 + side)
        far_side(functools.partial(pass_chain, sweep))

        for side in range(2):
            for j in range(3):
                arrived = (value_in[side, j, 0], value_in[side, j, 1])
                other = (ch_out[sweep, 1 - side, j, 0], ch_out[sweep, 1 - side, j, 1])
                value = add(
                    mul((coef[6 + side, 0, j], coef[6 + side, 1, j]), arrived),
                    mul((coef[4 + side, 0, j], coef[4 + side, 1, j]), other),
                )
                near[side, 0, j] = value[0]
                near[side, 1, j] = value[1]

        final = sweep == SWEEPS - 1

        def join_edge(side, tile):
            q = matrix()
            r = 0 if side == 0 else rows - 1
            w = [ET[side, p, :, tile] for p in range(2)]
            for end, column in ((0, EPHI), (1, EPSI)):
                entry = [
                    jnp.broadcast_to(near[end, p, :, r : r + 1, :], (3,) + plane)
                    for p in range(2)
                ]
                w = add(w, mul([column[side, p, :, tile] for p in range(2)], entry))
            for p in range(2):
                for c in range(3):
                    halo_out[sweep + 1, 1 - side, p, c, tile] = (
                        q[c][0] * w[p][0] + q[c][1] * w[p][1] + q[c][2] * w[p][2]
                    )

        if not final:
            for piece in range(PIECES):
                for tile in tiles[piece * len(tiles) // PIECES : (piece + 1) * len(tiles) // PIECES]:
                    for side in range(2):
                        join_edge(side, tile)
                send_halo(sweep + 1, piece)
            for side in range(2):

                @pl.when(far[side])
                def _():
                    for p in range(2):
                        for c in range(3):
                            early_copy(side, p, c).start()


        def join(z, carry):
            q = matrix()
            before, after = get(near, 0), get(near, 1)
            w = add(add(get(T, z), mul(get(PHI, z), before)), mul(get(PSI, z), after))
            values = []
            for p in range(2):
                for c in range(3):
                    values.append(q[c][0] * w[p][0] + q[c][1] * w[p][1] + q[c][2] * w[p][2])
            target = OUT if final else U
            for i in range(6):
                target[z, i // 3, i % 3] = values[i]
            return carry

        if not final:
            for side in range(2):

                @pl.when(far[side])
                def _():
                    for i in range(2):
                        far_copy(side, i).wait_send()
                    field_moved(side).wait_send()
                    field_kept().wait()

                @pl.when(beside[1 - side])
                def _():
                    rows_moved(side).wait_send()

        loop(0, depth, join, 0, 4)

        if not final:


            @pl.when(is_far)
            def _():
                far_first(0)
                send_columns(0)

        else:
            pl.when(is_far)(far_last)

    @pl.when(is_far)
    def _():
        for_all(0, lambda steps, e: mi_copy(whole, steps, moved(e)).wait_send())

    for side in range(2):

        @pl.when(beside[1 - side])
        def _():
            for sweep in range(1, SWEEPS):
                for piece in range(PIECES):
                    halo_copy(sweep, side, piece).wait_send()

        @pl.when(far[side])
        def _():
            early_moved(side).wait_send()

        sends = both(even[side], onward[side] >= 1)

        @pl.when(sends)
        def _():
            chain_copy(
                info_out.at[side, 0:3],
                info_in.at[side, 0:3],
                tip_send.at[way(side)],
                info_recv.at[way(side)],
                side,
                1,
            ).wait_send()
            for sweep in range(SWEEPS):
                own_copy(sweep, side, whole).wait_send()

        @pl.when(both(sends, place[side] > 0))
        def _():
            info_copy(side).wait_send()

        for steps in (2, 1):

            @pl.when(both(odd[side], onward[side] >= steps))
            def _():
                lam_copy(side, steps, whole).wait_send()
                for sweep in range(SWEEPS):
                    x_copy(sweep, side, steps, whole).wait_send()


def local(ngz, nxy, field, source, classes, boundary, conductance, angles, strengths):
    depth, _, _, rows, width = field.shape
    f32 = jnp.float32
    block = pltpu.VMEM(field.shape, f32)
    flat = (depth, rows, width)
    line = (2, 3, rows, width)
    pair = (2, rows, width)
    edge = (2, 2, 3, depth, width)
    narrow = pltpu.VMEM((depth, 2, rows, width), f32)
    lines = pltpu.VMEM((2, depth, 2, rows, width), f32)
    dma = pltpu.SemaphoreType.DMA
    ways = 1 if ngz == 4 else 2
    hbm = pl.BlockSpec(memory_space=pl.ANY)
    smem = pl.BlockSpec(memory_space=pltpu.SMEM)
    return pl.pallas_call(
        functools.partial(relax, ngz, nxy),
        out_shape=pltpu.VMEM(field.shape, f32),
        in_specs=[hbm] * 4 + [smem] * 3,
        out_specs=pl.BlockSpec(memory_space=pltpu.VMEM),
        scratch_shapes=[
            block,
            block,
            pltpu.VMEM(flat, jnp.int32),
            pltpu.VMEM(flat, jnp.int32),
            pltpu.VMEM(flat, f32),
            pltpu.VMEM(flat, f32),
            block,
            block,
            block,
            block,
            pltpu.VMEM((3, 3, rows, 128), f32),
            pltpu.VMEM(edge, f32),
            pltpu.VMEM(edge, f32),
            pltpu.VMEM(edge, f32),
            pltpu.VMEM(edge, f32),
            pltpu.VMEM((2,) + line, f32),
            pltpu.VMEM((14,) + line, f32),
            pltpu.VMEM((2,) + line, f32),
            pltpu.VMEM((SWEEPS,) + edge, f32),
            pltpu.VMEM((SWEEPS,) + edge, f32),
            pltpu.VMEM((2, 3) + pair, f32),
            pltpu.VMEM((2, 9) + pair, f32),
            pltpu.VMEM((2, 9) + pair, f32),
            pltpu.VMEM((2, 3) + pair, f32),
            pltpu.VMEM((2, 3) + pair, f32),
            pltpu.VMEM((SWEEPS, 2, 3) + pair, f32),
            pltpu.VMEM((SWEEPS, 2, 3) + pair, f32),
            pltpu.VMEM((SWEEPS, 2, 3) + pair, f32),
            pltpu.VMEM((SWEEPS, 2, 3) + pair, f32),
            narrow,
            narrow,
            pltpu.VMEM((2,) + flat, jnp.int32),
            pltpu.VMEM((2,) + flat, jnp.int32),
            lines,
            lines,
            lines,
            lines,
            pltpu.VMEM((11, rows, width), f32),
            pltpu.VMEM((2,) + pair, f32),
            pltpu.VMEM((2, 6, 10, rows, width), f32),
            pltpu.VMEM((2, 10, rows, width), f32),
            dma((PIECES + 3,)),
            dma((2, PIECES)),
            dma((2, PIECES)),
            dma((ways,)),
            dma((ways, 3)),
            dma((ways,)),
            dma((ways,)),
            dma((ways, 2)),
            dma((ways, 3)),
            dma((SWEEPS, ways)),
            dma((SWEEPS, ways, 3)),
            dma((SWEEPS, ways, 2)),
            dma((SWEEPS, ways, 3)),
            dma((5,)),
            dma((3,)),
            dma((3,)),
            pltpu.SemaphoreType.REGULAR,
            dma((2,)),
            dma((2,)),
            dma(()),
            dma(()),
            dma((6,)),
            dma((2, 6)),
        ],
        compiler_params=pltpu.CompilerParams(collective_id=0, has_side_effects=True, vmem_limit_bytes=VMEM_LIMIT),
    )(field, source, classes, boundary, conductance, angles, strengths)


def solution(mesh):
    in_specs = (
        P("gz", None, None, "xy", None),
        P("gz", None, None, "xy", None),
        P("gz", "xy", None),
        P("gz", "xy", None),
        P(),
        P(),
        P(),
    )
    out_specs = P("gz", None, None, "xy", None)
    body = functools.partial(local, mesh.shape["gz"], mesh.shape["xy"])
    return jax.shard_map(body, mesh=mesh, in_specs=in_specs, out_specs=out_specs, check_vma=False)
```

```python
import functools

import jax
import jax.numpy as jnp
from jax import lax
from jax.experimental import pallas as pl
from jax.experimental.pallas import tpu as pltpu
from jax.sharding import PartitionSpec as P

SWEEPS = 2
PIECES = 2
VMEM_LIMIT = 62 * 2**20

coupling = 0.1
penalty = 4.0


def mul(a, b):
    return (a[0] * b[0] - a[1] * b[1], a[0] * b[1] + a[1] * b[0])


def add(a, b):
    return (a[0] + b[0], a[1] + b[1])


def inv(a):
    weight = 1.0 / (a[0] * a[0] + a[1] * a[1])
    return (a[0] * weight, -a[1] * weight)


def one_minus(a):
    return (1.0 - a[0], -a[1])


def get(ref, *at):
    return (ref[at + (0,)], ref[at + (1,)])


def put(ref, value, *at):
    ref[at + (0,)] = value[0]
    ref[at + (1,)] = value[1]


def loop(low, high, body, carry, by):
    by = by if (high - low) % by == 0 else 1

    def several(k, carry):
        for i in range(by):
            carry = body(low + k * by + i, carry)
        return carry

    return lax.fori_loop(0, (high - low) // by, several, carry)


def rotation(angles, shape):
    cos = [jnp.cos(jnp.full(shape, angles[i], jnp.float32)) for i in range(3)]
    sin = [jnp.sin(jnp.full(shape, angles[i], jnp.float32)) for i in range(3)]
    (ca, cb, cc), (sa, sb, sc) = cos, sin
    left = [[ca * cb, -sa, ca * sb], [sa * cb, ca, sa * sb], [-sb, jnp.zeros_like(cb), cb]]
    return [[row[0] * cc + row[1] * sc, row[1] * cc - row[0] * sc, row[2]] for row in left]


def relax(
    ngz,
    nxy,
    field,
    source,
    classes,
    boundary,
    conductance,
    angles,
    strengths,
    OUT,
    U,
    S,
    C,
    B,
    SG,
    DR,
    PH,
    PHI,
    PSI,
    T,
    QM,
    EPHI,
    EPSI,
    EH,
    ET,
    ends,
    coef,
    near,
    halo_out,
    halo_in,
    value_in,
    info_in,
    info_out,
    lam_in,
    lam_out,
    own_in,
    own_out,
    ch_in,
    ch_out,
    XR,
    FA,
    CX,
    BX,
    FP,
    FPHI,
    FPSI,
    FT,
    FC,
    far_ends,
    mi_in,
    mi_out,
    in_sems,
    halo_send,
    halo_recv,
    tip_send,
    tip_recv,
    info_send,
    info_recv,
    lam_send,
    lam_recv,
    own_send,
    own_recv,
    ch_send,
    ch_recv,
    far_local,
    far_send,
    far_recv,
    near_ready,
    row_send,
    row_recv,
    early_send,
    early_recv,
    mi_send,
    mi_recv,
):
    ix, iz = lax.axis_index("xy"), lax.axis_index("gz")
    depth, _, _, rows, width = U.shape
    kinds = conductance.shape[0]
    plane = (rows, width)
    has = {
        ("xy", 0): ix > 0,
        ("xy", 1): ix < nxy - 1,
    }
    where_is = {
        ("xy", 0): ix - 1,
        ("xy", 1): ix + 1,
    }
    middle = nxy // 2
    far = (ix == middle, ix == middle - 1)
    is_far = jnp.logical_or(far[0], far[1])
    not_far = jnp.logical_not(is_far)
    helps = (ix == middle + 1, ix == middle - 2)
    helper = jnp.logical_or(helps[0], helps[1])
    pair = jnp.where(far[0], ix + 1, ix - 1)
    beside = [jnp.logical_and(has["xy", side], jnp.logical_not(far[side])) for side in range(2)]
    for steps in (1, 2):
        has["gz", -steps] = iz >= steps
        has["gz", steps] = iz < ngz - steps
        where_is["gz", -steps] = iz - steps
        where_is["gz", steps] = iz + steps
    signals = {}
    for key, there in has.items():
        signals[key] = jnp.logical_and(there, not_far)
        if key[0] == "xy":
            signals[key] = jnp.logical_and(signals[key], jnp.logical_not(helps[key[1]]))
    count = sum(there.astype(jnp.int32) for there in signals.values())
    count += ngz * helper.astype(jnp.int32)
    zs = depth // PIECES
    spans = [pl.ds(piece * zs, zs) for piece in range(PIECES)]
    moves = [(field.at[span], U.at[span]) for span in spans]
    moves += [(classes, C), (boundary, B), (source, S)]
    loads = [
        pltpu.make_async_copy(src, dst, in_sems.at[i]) for i, (src, dst) in enumerate(moves)
    ]
    for load in loads[PIECES : PIECES + 2] + loads[:PIECES] + loads[PIECES + 2 :]:
        load.start()

    barrier = pltpu.get_barrier_semaphore()
    for key, there in signals.items():

        @pl.when(there)
        def _():
            pl.semaphore_signal(
                barrier,
                inc=1,
                device_id={key[0]: where_is[key]},
                device_id_type=pl.DeviceIdType.MESH,
            )


    @pl.when(is_far)
    def _():
        for g in range(ngz):
            pl.semaphore_signal(
                barrier,
                inc=1,
                device_id={"xy": pair, "gz": g},
                device_id_type=pl.DeviceIdType.MESH,
            )
        pl.semaphore_signal(
            barrier,
            inc=1,
            device_id={"xy": jnp.where(far[0], ix - 1, ix + 1)},
            device_id_type=pl.DeviceIdType.MESH,
        )

    def remote(src, dst, send, recv, key):
        return pltpu.make_async_remote_copy(
            src_ref=src,
            dst_ref=dst,
            send_sem=send,
            recv_sem=recv,
            device_id={key[0]: where_is[key]},
            device_id_type=pl.DeviceIdType.MESH,
        )

    def halo_copy(sweep, side, piece):
        span = pl.ds(piece * zs, zs)
        return remote(
            halo_out.at[sweep, side, :, :, span],
            halo_in.at[sweep, side, :, :, span],
            halo_send.at[side, piece],
            halo_recv.at[side, piece],
            ("xy", 1 - side),
        )

    def send_halo(sweep, piece):
        for side in range(2):

            @pl.when(beside[1 - side])
            def _():
                halo_copy(sweep, side, piece).start()

    def early_copy(side, p, c):
        return remote(
            halo_out.at[1, 1 - side, p, c],
            FA.at[:, p, c, :],
            early_send,
            early_recv,
            ("xy", side),
        )

    def early_moved(side):
        return remote(
            halo_out.at[1, 1 - side],
            halo_out.at[1, 1 - side],
            early_send,
            early_recv,
            ("xy", side),
        )

    def row_copy(side, p, c):
        return remote(
            U.at[:, p, c, 0 if side else rows - 1, :],
            halo_in.at[0, side, p, c],
            row_send.at[side],
            row_recv.at[side],
            ("xy", 1 - side),
        )

    row_copies = lambda side: [row_copy(side, p, c) for p in range(2) for c in range(3)]
    rows_moved = lambda side: remote(
        halo_in.at[0, side],
        halo_in.at[0, side],
        row_send.at[side],
        row_recv.at[side],
        ("xy", 1 - side),
    )

    def pack(first, last, z, values):
        for i in range(6):
            at = (i // 3, i % 3, pl.ds(z, 1), slice(None))
            first[at] = values[i][:1, :]
            last[at] = values[i][rows - 1 :, :]

    for side in range(2):

        for sweep in range(SWEEPS):

            @pl.when(jnp.logical_not(beside[side]))
            def _():
                halo_in[sweep, side] = jnp.zeros(halo_in.shape[2:], jnp.float32)

        @pl.when((iz if side == 0 else ngz - 1 - iz) < 2)
        def _():
            for part in range(3, 9):
                info_in[side, part] = jnp.zeros(info_in.shape[2:], jnp.float32)
            lam_in[side] = jnp.zeros(lam_in.shape[1:], jnp.float32)
            for sweep in range(SWEEPS):
                ch_in[sweep, side] = jnp.zeros(ch_in.shape[2:], jnp.float32)

    loads[PIECES].wait()
    loads[PIECES + 1].wait()

    def diagonal(z, carry):
        ids = C[z]
        sigma = jnp.zeros(plane, jnp.float32)
        for kind in range(kinds):
            sigma = jnp.where(ids == kind, conductance[kind], sigma)
        SG[z] = sigma
        DR[z] = 2.0 + 4.0 * coupling + penalty * B[z].astype(jnp.float32)
        return carry

    loop(0, depth, diagonal, 0, 4)

    def diag(z):
        real = jnp.broadcast_to(DR[z][None], (3,) + plane)
        sigma = SG[z]
        return real, jnp.stack([sigma * strengths[j] for j in range(3)])

    none = (jnp.zeros((3,) + plane, jnp.float32),) * 2

    def pivots(k, carry):
        p, q = carry
        z, back = k, depth - 1 - k
        d, f = diag(z), diag(back)
        p = inv((d[0] - p[0], d[1] - p[1]))
        q = inv((f[0] - q[0], f[1] - q[1]))
        put(PH, p, z)
        put(PHI, q, back)
        return p, q

    loop(0, depth, pivots, (none, none), 2)
    ones = (jnp.ones((3,) + plane, jnp.float32), none[0])

    def columns(k, carry):
        down, up = carry
        z, back = k, depth - 1 - k
        down = mul(get(PHI, z), down)
        up = mul(get(PH, back), up)
        put(PHI, down, z)
        put(PSI, up, back)
        return down, up

    loop(0, depth, columns, (ones, ones), 2)
    for piece in range(PIECES):
        loads[piece].wait()

    @pl.when(not_far)
    def _():
        pl.semaphore_wait(barrier, count)

    @pl.when(helper)
    def _():
        pl.semaphore_signal(
            near_ready,
            inc=1,
            device_id={"xy": jnp.where(helps[0], ix - 1, ix + 1)},
            device_id_type=pl.DeviceIdType.MESH,
        )

    @pl.when(is_far)
    def _():
        pl.semaphore_wait(near_ready, 1)

    for side in range(2):

        @pl.when(beside[1 - side])
        def _():
            for copy in row_copies(side):
                copy.start()

    LEFT, RIGHT = 0, 1
    tip = (lambda: get(PHI, 0), lambda: get(PSI, depth - 1))
    across = lambda: get(PSI, 0)

    place = (iz, ngz - 1 - iz)
    even = [lax.rem(k, 2) == 0 for k in place]
    odd = [lax.rem(k, 2) == 1 for k in place]
    onward = [ngz - 1 - k for k in place]

    def to(side, steps):
        return {"gz": iz + steps if side == LEFT else iz - steps}

    def chain_copy(src, dst, send, recv, side, steps):
        return pltpu.make_async_remote_copy(
            src_ref=src,
            dst_ref=dst,
            send_sem=send,
            recv_sem=recv,
            device_id=to(side, steps),
            device_id_type=pl.DeviceIdType.MESH,
        )

    whole = slice(None)
    way = (lambda side: 0) if ngz == 4 else (lambda side: side)

    def tip_copy(side, j):
        return chain_copy(
            info_out.at[side, j],
            info_in.at[side, j],
            tip_send.at[way(side)],
            tip_recv.at[way(side), j],
            side,
            1,
        )

    def info_copy(side):
        return chain_copy(
            info_out.at[side, 3:9],
            info_in.at[side, 3:9],
            info_send.at[way(side)],
            info_recv.at[way(side)],
            side,
            1,
        )

    def lam_copy(side, steps, j):
        return chain_copy(
            lam_out.at[side, j],
            lam_in.at[side, j],
            lam_send.at[way(side), steps - 1],
            lam_recv.at[way(side), j],
            side,
            steps,
        )

    def own_copy(sweep, side, j):
        return chain_copy(
            own_out.at[sweep, side, j],
            own_in.at[sweep, side, j],
            own_send.at[sweep, way(side)],
            own_recv.at[sweep, way(side), j],
            side,
            1,
        )

    def x_copy(sweep, side, steps, j):
        return chain_copy(
            ch_out.at[sweep, side, j],
            ch_in.at[sweep, side, j],
            ch_send.at[sweep, way(side), steps - 1],
            ch_recv.at[sweep, way(side), j],
            side,
            steps,
        )


    both = jnp.logical_and

    def send_info(side):
        sends = both(even[side], onward[side] >= 1)
        parts = (tip[1 - side](), tip[side](), across())
        for part in range(3):
            for j in range(3):
                for p in range(2):
                    info_out[side, part * 3 + j, p] = parts[part][p][j]
            if part == 0:

                @pl.when(sends)
                def _():
                    for j in range(3):
                        tip_copy(side, j).start()

        @pl.when(both(sends, place[side] > 0))
        def _():
            info_copy(side).start()

    def pass_lam(side):
        @pl.when(both(odd[side], place[side] >= 2))
        def _():
            info_copy(side).wait_recv()

        for j in range(3):

            @pl.when(odd[side])
            def _():
                tip_copy(side, j).wait_recv()

            @pl.when(place[side] >= 2)
            def _():
                lam_copy(side, 1, j).wait_recv()

            tips = [(info_in[side, 3 * k + j, 0], info_in[side, 3 * k + j, 1]) for k in range(3)]
            given = (lam_in[side, j, 0], lam_in[side, j, 1])

            @pl.when(odd[side])
            def _():
                skip = mul(tips[2], inv(one_minus(mul(tips[1], given))))
                lam = add(tips[0], mul(tips[2], mul(skip, given)))
                for p in range(2):
                    coef[8 + side, p, j] = skip[p]
                    coef[10 + side, p, j] = lam[p]

            @pl.when(even[side])
            def _():
                for p in range(2):
                    coef[10 + side, p, j] = given[p]

            of = lambda pair: (pair[0][j], pair[1][j])
            lam = (coef[10 + side, 0, j], coef[10 + side, 1, j])
            kappa = mul(of(across()), inv(one_minus(mul(of(tip[side]()), lam))))
            over = mul(kappa, lam)
            value = add(of(tip[1 - side]()), mul(of(across()), over))
            for p in range(2):
                coef[side, p, j] = kappa[p]
                coef[2 + side, p, j] = over[p]
                lam_out[side, j, p] = value[p]

            @pl.when(both(odd[side], onward[side] >= 1))
            def _():
                lam_copy(side, 1, j).start()

        @pl.when(both(odd[side], onward[side] >= 2))
        def _():
            for j in range(3):
                lam_copy(side, 2, j).start()

    def own_base(side, j):
        return add(
            (ends[1 - side, 0, j], ends[1 - side, 1, j]),
            mul(
                (coef[2 + side, 0, j], coef[2 + side, 1, j]),
                (ends[side, 0, j], ends[side, 1, j]),
            ),
        )

    def own_sum(sweep, side):
        for j in range(3):
            base = own_base(side, j)
            for p in range(2):
                own_out[sweep, side, j, p] = base[p]

            @pl.when(both(even[side], onward[side] >= 1))
            def _():
                own_copy(sweep, side, j).start()

    def pass_chain(sweep, side):
        for j in range(3):
            base = own_base(side, j)

            @pl.when(odd[side])
            def _():
                own_copy(sweep, side, j).wait_recv()

            @pl.when(place[side] >= 2)
            def _():
                x_copy(sweep, side, 1, j).wait_recv()

            given = (ch_in[sweep, side, j, 0], ch_in[sweep, side, j, 1])

            @pl.when(odd[side])
            def _():
                own = (own_in[sweep, side, j, 0], own_in[sweep, side, j, 1])
                x = add(own, mul((coef[8 + side, 0, j], coef[8 + side, 1, j]), given))
                for p in range(2):
                    value_in[side, j, p] = x[p]

            @pl.when(even[side])
            def _():
                for p in range(2):
                    value_in[side, j, p] = given[p]

            x = (value_in[side, j, 0], value_in[side, j, 1])
            result = add(base, mul((coef[side, 0, j], coef[side, 1, j]), x))
            for p in range(2):
                ch_out[sweep, side, j, p] = result[p]

            @pl.when(both(odd[side], onward[side] >= 2))
            def _():
                x_copy(sweep, side, 2, j).start()

        @pl.when(both(odd[side], onward[side] >= 1))
        def _():
            for j in range(3):
                x_copy(sweep, side, 1, j).start()

    left_first = iz * 2 < ngz - 1

    def near_side(run):
        @pl.when(left_first)
        def _():
            run(LEFT)

        @pl.when(jnp.logical_not(left_first))
        def _():
            run(RIGHT)

    def far_side(run):
        @pl.when(left_first)
        def _():
            run(RIGHT)

        @pl.when(jnp.logical_not(left_first))
        def _():
            run(LEFT)

    def far_source(side, i):
        edge = pl.ds(rows - 1 if side else 0, 1)
        return (C.at[:, edge, :], B.at[:, edge, :])[i] if i < 2 else U.at[:, :, i - 2, edge, :]

    def far_target(i, first):
        at = pl.ds(first if i < 2 else first + i - 2, 1)
        return (CX.at[0, :, at, :], BX.at[0, :, at, :])[i] if i < 2 else XR.at[:, :, at, :]

    def far_copy(side, i):
        return pltpu.make_async_remote_copy(
            src_ref=far_source(side, i),
            dst_ref=far_target(i, 4 if i < 2 else 0),
            send_sem=far_send.at[min(i, 2)],
            recv_sem=far_recv.at[min(i, 2)],
            device_id={"xy": ix + 1 if side else ix - 1},
            device_id_type=pl.DeviceIdType.MESH,
        )

    def kept_copy(side, i):
        return pltpu.make_async_copy(
            far_source(side, i), far_target(i, 0 if i < 2 else 4), far_local.at[min(i, 2)]
        )

    def field_moved(side):
        return pltpu.make_async_remote_copy(
            src_ref=XR.at[:, :, 0:3, :],
            dst_ref=XR.at[:, :, 0:3, :],
            send_sem=far_send.at[2],
            recv_sem=far_recv.at[2],
            device_id={"xy": ix + 1 if side else ix - 1},
            device_id_type=pl.DeviceIdType.MESH,
        )

    def field_kept():
        return pltpu.make_async_copy(XR.at[:, :, 4:7, :], XR.at[:, :, 4:7, :], far_local.at[2])

    def lines_kept(i):
        ref = (CX, BX)[i].at[1, :, 0:2, :]
        return pltpu.make_async_copy(ref, ref, far_local.at[3 + i])

    def line_copy(side, i):
        first = rows - 1 if side else 0
        edge = pl.ds(first if i < 2 else (first - 1 if side else first + 1), 1)
        at = pl.ds(0 if i < 2 else 4, 1)
        return pltpu.make_async_copy(
            (C, B)[i % 2].at[:, edge, :], (CX, BX)[i % 2].at[1, :, at, :], far_local.at[3 + i % 2]
        )

    def far_begin():
        pl.semaphore_wait(barrier, 1)
        for side in range(2):

            @pl.when(far[side])
            def _():
                for i in range(5):
                    far_copy(side, i).start()
                for i in range(5):
                    kept_copy(side, i).start()
                for i in range(4):
                    line_copy(side, i).start()

    def near_lam(side):
        pl.when(place[side] < 2)(functools.partial(pass_lam, side))

    def far_lam(side):
        pl.when(place[side] == 2)(functools.partial(pass_lam, side))

    def last_lam(side):
        pl.when(place[side] >= 3)(functools.partial(pass_lam, side))

    near_side(send_info)
    far_side(send_info)

    angle_matrix = rotation(angles, (rows, 128))
    for c in range(3):
        for j in range(3):
            QM[c, j] = angle_matrix[c][j]

    def matrix():
        return [
            [jnp.concatenate([QM[c, j]] * (width // 128), axis=1) for j in range(3)]
            for c in range(3)
        ]

    def pack_columns(z, carry):
        for src, dst in ((PHI, EPHI), (PSI, EPSI)):
            pack(dst.at[0], dst.at[1], z, [src[z, i // 3, i % 3] for i in range(6)])
        return carry

    loop(0, depth, pack_columns, 0, 4)

    row = lax.broadcasted_iota(jnp.int32, plane, 0)
    lane = lax.broadcasted_iota(jnp.int32, plane, 1)
    zero = jnp.zeros(plane, jnp.float32)

    def turn(q, driven):
        return [
            jnp.stack(
                [
                    q[0][j] * driven[p][0] + q[1][j] * driven[p][1] + q[2][j] * driven[p][2]
                    for j in range(3)
                ]
            )
            for p in range(2)
        ]

    def inner(z, carry):
        first, last = carry
        q = matrix()
        driven = []
        for p in range(2):
            of = []
            for c in range(3):
                u = U[z, p, c]
                around = jnp.where(lane == 0, zero, pltpu.roll(u, 1, 1))
                around += jnp.where(lane == width - 1, zero, pltpu.roll(u, width - 1, 1))
                around += jnp.where(row == 0, zero, pltpu.roll(u, 1, 0))
                around += jnp.where(row == rows - 1, zero, pltpu.roll(u, rows - 1, 0))
                of.append(S[z, p, c] + coupling * around)
            driven.append(of)
        turned = turn(q, driven)
        put(T, turned, z)
        return add(first, mul(get(PHI, z), turned)), add(last, mul(get(PSI, z), turned))

    tiles = [pl.ds(z, rows) for z in range(0, depth, rows)]

    def outer(sweep, side, tile, carry):
        first, last = carry
        q = matrix()
        turned = turn(
            q,
            [[coupling * halo_in[sweep, side, p, c, tile] for c in range(3)] for p in range(2)],
        )
        for p in range(2):
            EH[side, p, :, tile] = turned[p]
        phi = [EPHI[side, p, :, tile] for p in range(2)]
        psi = [EPSI[side, p, :, tile] for p in range(2)]
        return add(first, mul(phi, turned)), add(last, mul(psi, turned))

    third = lax.rem(row, 4)
    part = lambda k: third == k
    used = third < 3

    def mi_copy(k, steps, parts):
        slot = steps + 3 if steps < 0 else steps + 2
        return pltpu.make_async_remote_copy(
            src_ref=mi_out.at[k, parts],
            dst_ref=mi_in.at[k, 5 - slot, parts],
            send_sem=mi_send.at[slot],
            recv_sem=mi_recv.at[0 if k == whole else k, 5 - slot],
            device_id={"gz": iz + steps},
            device_id_type=pl.DeviceIdType.MESH,
        )

    all_steps = (-3, -2, -1, 1, 2, 3)
    at_end = lambda k: jnp.logical_or(k == 0, k == ngz - 1)

    def for_all(of, act):
        for steps in all_steps:
            there = (iz + steps >= 0) & (iz + steps < ngz)
            edge_ = at_end(iz + steps * of)

            @pl.when(jnp.logical_and(there, edge_))
            def _():
                act(steps, True)

            @pl.when(jnp.logical_and(there, jnp.logical_not(edge_)))
            def _():
                act(steps, False)

    def to_all(k, first):
        def act(steps, ends_only):
            if not ends_only:
                parts = pl.ds(first, 4 if first else 6)
            else:
                parts = pl.ds(first + (2 if steps > 0 else 0), 2)
            mi_copy(k, steps, parts).start()

        for_all(0, act)

    def moved(ends_only):
        return pl.ds(0, 4 if ends_only else 10)

    def from_all(k):
        for_all(1, lambda steps, e: mi_copy(k, -steps, moved(e)).wait_recv())

    def shifts(of):
        planes = []
        for d in (-2, -1, 0, 1, 2):
            plane_ = zero
            for j in range(3):
                if 0 <= j + d <= 2:
                    plane_ = jnp.where(part(j), of(j, j + d), plane_)
            planes.append((d, plane_))
        return planes

    def mix(planes, x):
        total = None
        for d, plane_ in planes:
            term = plane_ * (x if d == 0 else pltpu.roll(x, (rows - d) % rows, 0))
            total = term if total is None else total + term
        return total

    def far_clear():
        none_ = jnp.zeros((2,) + plane, jnp.float32)
        for slot, steps in enumerate(all_steps):
            there = (iz + steps >= 0) & (iz + steps < ngz)

            @pl.when(jnp.logical_not(there))
            def _():
                for k in range(2):
                    for part_ in range(5):
                        mi_in[k, slot, 2 * part_ : 2 * part_ + 2] = none_

            @pl.when(jnp.logical_and(there, at_end(iz + steps)))
            def _():
                for k in range(2):
                    for part_ in (0, 2, 3) if steps < 0 else (1, 2, 4):
                        mi_in[k, slot, 2 * part_ : 2 * part_ + 2] = none_

    def far_setup():
        q = matrix()
        for i, (_, plane_) in enumerate(shifts(lambda j, k: q[k][j])):
            FC[i] = plane_
        for i, (_, plane_) in enumerate(shifts(lambda j, k: q[j][k])):
            FC[5 + i] = plane_
        strength = jnp.full(plane, strengths[0], jnp.float32)
        for j in (1, 2):
            strength = jnp.where(part(j), strengths[j], strength)
        FC[10] = strength

    own = row < 4

    def far_first(k):
        for side in range(2):

            @pl.when(far[side])
            def _():
                if k == 0:
                    for i in range(2):
                        kept_copy(side, i).wait()
                        far_copy(side, i).wait_recv()
                else:
                    for i in range(2):
                        lines_kept(i).wait()

        def far_diagonal(z, carry):
            ids_tile, bound = CX[k, z], BX[k, z]
            ids = jnp.where(
                own,
                jnp.broadcast_to(ids_tile[0:1, :], plane),
                jnp.broadcast_to(ids_tile[4:5, :], plane),
            )
            edge = jnp.where(
                own, jnp.broadcast_to(bound[0:1, :], plane), jnp.broadcast_to(bound[4:5, :], plane)
            )
            sigma = jnp.zeros(plane, jnp.float32)
            for kind in range(kinds):
                sigma = jnp.where(ids == kind, conductance[kind], sigma)
            FT[k, z, 0] = 2.0 + 4.0 * coupling + penalty * edge.astype(jnp.float32)
            FT[k, z, 1] = sigma * FC[10]
            return carry

        loop(0, depth, far_diagonal, 0, 4)

        def far_pivots(z, carry):
            p, q = carry
            d, f = get(FT, k, z), get(FT, k, depth - 1 - z)
            p = inv((d[0] - p[0], d[1] - p[1]))
            q = inv((f[0] - q[0], f[1] - q[1]))
            put(FP, p, k, z)
            put(FPHI, q, k, depth - 1 - z)
            return p, q

        loop(0, depth, far_pivots, ((zero, zero), (zero, zero)), 2)
        one = jnp.ones(plane, jnp.float32)

        def far_columns(z, carry):
            down, up = carry
            back = depth - 1 - z
            down = mul(get(FPHI, k, z), down)
            up = mul(get(FP, k, back), up)
            put(FPHI, down, k, z)
            put(FPSI, up, k, back)
            return down, up

        loop(0, depth, far_columns, ((one, zero), (one, zero)), 2)
        ends_ = (get(FPHI, k, 0), get(FPSI, k, depth - 1), get(FPSI, k, 0))
        for i, value in enumerate(ends_):
            mi_out[k, 2 * i] = value[0]
            mi_out[k, 2 * i + 1] = value[1]

    def send_columns(k):
        to_all(k, 0)

    def far_solve(k, rhs):
        turned_by = [(d, FC[i]) for i, d in enumerate((-2, -1, 0, 1, 2))]

        def far_sums(z, carry):
            first, last = carry
            t = tuple(
                mix(turned_by, jnp.where(used, coupling * rhs(z, p), zero)) for p in range(2)
            )
            put(FT, t, k, z)
            return add(first, mul(get(FPHI, k, z), t)), add(last, mul(get(FPSI, k, z), t))

        first, last = loop(0, depth, far_sums, ((zero, zero), (zero, zero)), 4)
        for i, value in enumerate((first, last)):
            mi_out[k, 6 + 2 * i] = value[0]
            mi_out[k, 7 + 2 * i] = value[1]
        to_all(k, 6)

        def far_forward(z, m):
            m = mul(get(FP, k, z), add(get(FT, k, z), m))
            put(FT, m, k, z)
            return m

        def far_backward(i, w):
            z = depth - 1 - i
            w = add(get(FT, k, z), mul(get(FP, k, z), w))
            put(FT, w, k, z)
            return w

        loop(0, depth, far_forward, (zero, zero), 4)
        loop(0, depth, far_backward, (zero, zero), 4)

    def far_second():
        for side in range(2):

            @pl.when(far[side])
            def _():
                field_moved(side).wait_recv()

        far_solve(0, lambda z, p: XR[z, p])

    def far_meet(k, take):
        from_all(k)
        block = lambda slot: [(mi_in[k, slot, 2 * i], mi_in[k, slot, 2 * i + 1]) for i in range(5)]
        x = lam = y = mu = (zero, zero)
        for slot in range(3):
            top, bottom, cross, first, last = block(slot)
            det = inv(one_minus(mul(top, lam)))
            x, lam = (
                add(last, mul(cross, mul(det, add(x, mul(lam, first))))),
                add(bottom, mul(mul(cross, cross), mul(det, lam))),
            )
        for slot in (5, 4, 3):
            top, bottom, cross, first, last = block(slot)
            det = inv(one_minus(mul(bottom, mu)))
            y, mu = (
                add(first, mul(cross, mul(det, add(y, mul(mu, last))))),
                add(top, mul(mul(cross, cross), mul(det, mu))),
            )
        top, bottom, cross, first, last = [(mi_out[k, 2 * i], mi_out[k, 2 * i + 1]) for i in range(5)]
        g, h = add(x, mul(lam, first)), add(y, mul(mu, last))
        alpha, beta = one_minus(mul(lam, top)), one_minus(mul(mu, bottom))
        lc, mc = mul(lam, cross), mul(mu, cross)
        both_ = mul(lc, mc)
        all_ = mul(alpha, beta)
        det = inv((all_[0] - both_[0], all_[1] - both_[1]))
        put(far_ends, mul(det, add(mul(g, beta), mul(lc, h))), 0)
        put(far_ends, mul(det, add(mul(h, alpha), mul(mc, g))), 1)
        back_by = [(d, FC[5 + i]) for i, d in enumerate((-2, -1, 0, 1, 2))]

        def far_join(z, carry):
            before, after = get(far_ends, 0), get(far_ends, 1)
            w = add(
                add(get(FT, k, z), mul(get(FPHI, k, z), before)), mul(get(FPSI, k, z), after)
            )
            for p in range(2):
                take(z, p, mix(back_by, w[p]))
            return carry

        loop(0, depth, far_join, 0, 4)

    def far_third():
        def keep(z, p, u):
            FT[0, z, p] = u

        far_meet(0, keep)
        for side in range(2):

            @pl.when(far[side])
            def _():
                early_moved(side).wait_recv()

        def rhs(z, p):
            u = FT[0, z, p]
            beside_ = jnp.where(lane == 0, zero, pltpu.roll(u, 1, 1))
            beside_ += jnp.where(lane == width - 1, zero, pltpu.roll(u, width - 1, 1))
            early = jnp.where(row < 3, FA[z, p], zero)
            return pltpu.roll(u, 4, 0) + jnp.where(own, beside_ + early, zero)

        far_solve(1, rhs)

    def far_last():
        here = row == jnp.where(far[1], rows - 1, 0)
        next_ = row == jnp.where(far[1], rows - 2, 1)

        def give(z, p, u):
            for c in range(3):
                OUT[z, p, c] += jnp.where(
                    here,
                    jnp.broadcast_to(u[c : c + 1, :], plane),
                    jnp.where(next_, jnp.broadcast_to(u[4 + c : 5 + c, :], plane), zero),
                )

        far_meet(1, give)

    loads[PIECES + 2].wait()
    for sweep in range(SWEEPS):
        sums = loop(0, depth, inner, (none, none), 4)
        if sweep == 0:
            near_side(near_lam)
        else:
            pl.when(is_far)(far_second)
        halves = [(none, none), (none, none)]
        for piece in range(PIECES):
            for side in range(2):

                if sweep == 0 and piece == 0:

                    @pl.when(beside[side])
                    def _():
                        rows_moved(side).wait_recv()

                if sweep:

                    @pl.when(beside[side])
                    def _():
                        halo_copy(sweep, side, piece).wait_recv()

                for tile in tiles[piece * len(tiles) // PIECES : (piece + 1) * len(tiles) // PIECES]:
                    halves[side] = outer(sweep, side, tile, halves[side])
        for side in range(2):
            here = row == (0 if side == 0 else rows - 1)
            sums = tuple(
                add(
                    sums[end],
                    tuple(
                        jnp.where(here[None], jnp.sum(part, axis=1, keepdims=True), 0.0)
                        for part in halves[side][end]
                    ),
                )
                for end in range(2)
            )
        put(ends, sums[0], 0)
        put(ends, sums[1], 1)

        near_side(functools.partial(own_sum, sweep))
        if sweep == 0:

            @pl.when(is_far)
            def _():
                far_begin()
                near_side(functools.partial(pass_chain, sweep))

            far_side(far_lam)
        far_side(functools.partial(own_sum, sweep))
        if sweep:
            near_side(functools.partial(pass_chain, sweep))
        else:

            @pl.when(not_far)
            def _():
                near_side(functools.partial(pass_chain, sweep))

        def forward(z, m):
            given = []
            for p in range(2):
                edges = []
                for j in range(3):
                    above = jnp.broadcast_to(EH[0, p, j, pl.ds(z, 1), :], plane)
                    below = jnp.broadcast_to(EH[1, p, j, pl.ds(z, 1), :], plane)
                    edges.append(
                        jnp.where(row == 0, above, zero) + jnp.where(row == rows - 1, below, zero)
                    )
                given.append(T[z, p] + jnp.stack(edges))
            m = mul(get(PH, z), add(given, m))
            put(T, m, z)
            return m

        def backward(k, w):
            z = depth - 1 - k
            w = add(get(T, z), mul(get(PH, z), w))
            put(T, w, z)
            if sweep < SWEEPS - 1:
                pack(ET.at[0], ET.at[1], z, [w[i // 3][i % 3] for i in range(6)])
            return w

        loop(0, depth, forward, none, 4)
        loop(0, depth, backward, none, 4)
        if sweep:

            @pl.when(is_far)
            def _():
                send_columns(1)
                far_third()

        else:

            @pl.when(is_far)
            def _():
                far_clear()
                far_setup()
                far_first(1)

        if sweep == 0:
            far_side(last_lam)
            for side in range(2):
                lam = get(coef, 10 + side)
                away = tuple(
                    jnp.stack([lam_out[1 - side, j, p] for j in range(3)]) for p in range(2)
                )
                det = inv(one_minus(mul(lam, away)))
                put(coef, det, 6 + side)
                put(coef, mul(det, lam), 4 + side)
        far_side(functools.partial(pass_chain, sweep))

        for side in range(2):
            for j in range(3):
                arrived = (value_in[side, j, 0], value_in[side, j, 1])
                other = (ch_out[sweep, 1 - side, j, 0], ch_out[sweep, 1 - side, j, 1])
                value = add(
                    mul((coef[6 + side, 0, j], coef[6 + side, 1, j]), arrived),
                    mul((coef[4 + side, 0, j], coef[4 + side, 1, j]), other),
                )
                near[side, 0, j] = value[0]
                near[side, 1, j] = value[1]

        final = sweep == SWEEPS - 1

        def join_edge(side, tile):
            q = matrix()
            r = 0 if side == 0 else rows - 1
            w = [ET[side, p, :, tile] for p in range(2)]
            for end, column in ((0, EPHI), (1, EPSI)):
                entry = [
                    jnp.broadcast_to(near[end, p, :, r : r + 1, :], (3,) + plane)
                    for p in range(2)
                ]
                w = add(w, mul([column[side, p, :, tile] for p in range(2)], entry))
            for p in range(2):
                for c in range(3):
                    halo_out[sweep + 1, 1 - side, p, c, tile] = (
                        q[c][0] * w[p][0] + q[c][1] * w[p][1] + q[c][2] * w[p][2]
                    )

        if not final:
            for piece in range(PIECES):
                for tile in tiles[piece * len(tiles) // PIECES : (piece + 1) * len(tiles) // PIECES]:
                    for side in range(2):
                        join_edge(side, tile)
                send_halo(sweep + 1, piece)
            for side in range(2):

                @pl.when(far[side])
                def _():
                    for p in range(2):
                        for c in range(3):
                            early_copy(side, p, c).start()


        def join(z, carry):
            q = matrix()
            before, after = get(near, 0), get(near, 1)
            w = add(add(get(T, z), mul(get(PHI, z), before)), mul(get(PSI, z), after))
            values = []
            for p in range(2):
                for c in range(3):
                    values.append(q[c][0] * w[p][0] + q[c][1] * w[p][1] + q[c][2] * w[p][2])
            target = OUT if final else U
            for i in range(6):
                target[z, i // 3, i % 3] = values[i]
            return carry

        if not final:
            for side in range(2):

                @pl.when(far[side])
                def _():
                    for i in range(2):
                        far_copy(side, i).wait_send()
                    field_moved(side).wait_send()
                    field_kept().wait()

                @pl.when(beside[1 - side])
                def _():
                    rows_moved(side).wait_send()

        loop(0, depth, join, 0, 4)

        if not final:


            @pl.when(is_far)
            def _():
                far_first(0)
                send_columns(0)

        else:
            pl.when(is_far)(far_last)

    @pl.when(is_far)
    def _():
        for_all(0, lambda steps, e: mi_copy(whole, steps, moved(e)).wait_send())

    for side in range(2):

        @pl.when(beside[1 - side])
        def _():
            for sweep in range(1, SWEEPS):
                for piece in range(PIECES):
                    halo_copy(sweep, side, piece).wait_send()

        @pl.when(far[side])
        def _():
            early_moved(side).wait_send()

        sends = both(even[side], onward[side] >= 1)

        @pl.when(sends)
        def _():
            chain_copy(
                info_out.at[side, 0:3],
                info_in.at[side, 0:3],
                tip_send.at[way(side)],
                info_recv.at[way(side)],
                side,
                1,
            ).wait_send()
            for sweep in range(SWEEPS):
                own_copy(sweep, side, whole).wait_send()

        @pl.when(both(sends, place[side] > 0))
        def _():
            info_copy(side).wait_send()

        for steps in (2, 1):

            @pl.when(both(odd[side], onward[side] >= steps))
            def _():
                lam_copy(side, steps, whole).wait_send()
                for sweep in range(SWEEPS):
                    x_copy(sweep, side, steps, whole).wait_send()


def local(ngz, nxy, field, source, classes, boundary, conductance, angles, strengths):
    depth, _, _, rows, width = field.shape
    f32 = jnp.float32
    block = pltpu.VMEM(field.shape, f32)
    flat = (depth, rows, width)
    line = (2, 3, rows, width)
    pair = (2, rows, width)
    edge = (2, 2, 3, depth, width)
    narrow = pltpu.VMEM((depth, 2, rows, width), f32)
    lines = pltpu.VMEM((2, depth, 2, rows, width), f32)
    dma = pltpu.SemaphoreType.DMA
    ways = 1 if ngz == 4 else 2
    hbm = pl.BlockSpec(memory_space=pl.ANY)
    smem = pl.BlockSpec(memory_space=pltpu.SMEM)
    return pl.pallas_call(
        functools.partial(relax, ngz, nxy),
        out_shape=pltpu.VMEM(field.shape, f32),
        in_specs=[hbm] * 4 + [smem] * 3,
        out_specs=pl.BlockSpec(memory_space=pltpu.VMEM),
        scratch_shapes=[
            block,
            block,
            pltpu.VMEM(flat, jnp.int32),
            pltpu.VMEM(flat, jnp.int32),
            pltpu.VMEM(flat, f32),
            pltpu.VMEM(flat, f32),
            block,
            block,
            block,
            block,
            pltpu.VMEM((3, 3, rows, 128), f32),
            pltpu.VMEM(edge, f32),
            pltpu.VMEM(edge, f32),
            pltpu.VMEM(edge, f32),
            pltpu.VMEM(edge, f32),
            pltpu.VMEM((2,) + line, f32),
            pltpu.VMEM((14,) + line, f32),
            pltpu.VMEM((2,) + line, f32),
            pltpu.VMEM((SWEEPS,) + edge, f32),
            pltpu.VMEM((SWEEPS,) + edge, f32),
            pltpu.VMEM((2, 3) + pair, f32),
            pltpu.VMEM((2, 9) + pair, f32),
            pltpu.VMEM((2, 9) + pair, f32),
            pltpu.VMEM((2, 3) + pair, f32),
            pltpu.VMEM((2, 3) + pair, f32),
            pltpu.VMEM((SWEEPS, 2, 3) + pair, f32),
            pltpu.VMEM((SWEEPS, 2, 3) + pair, f32),
            pltpu.VMEM((SWEEPS, 2, 3) + pair, f32),
            pltpu.VMEM((SWEEPS, 2, 3) + pair, f32),
            narrow,
            narrow,
            pltpu.VMEM((2,) + flat, jnp.int32),
            pltpu.VMEM((2,) + flat, jnp.int32),
            lines,
            lines,
            lines,
            lines,
            pltpu.VMEM((11, rows, width), f32),
            pltpu.VMEM((2,) + pair, f32),
            pltpu.VMEM((2, 6, 10, rows, width), f32),
            pltpu.VMEM((2, 10, rows, width), f32),
            dma((PIECES + 3,)),
            dma((2, PIECES)),
            dma((2, PIECES)),
            dma((ways,)),
            dma((ways, 3)),
            dma((ways,)),
            dma((ways,)),
            dma((ways, 2)),
            dma((ways, 3)),
            dma((SWEEPS, ways)),
            dma((SWEEPS, ways, 3)),
            dma((SWEEPS, ways, 2)),
            dma((SWEEPS, ways, 3)),
            dma((5,)),
            dma((3,)),
            dma((3,)),
            pltpu.SemaphoreType.REGULAR,
            dma((2,)),
            dma((2,)),
            dma(()),
            dma(()),
            dma((6,)),
            dma((2, 6)),
        ],
        compiler_params=pltpu.CompilerParams(collective_id=0, has_side_effects=True, vmem_limit_bytes=VMEM_LIMIT),
    )(field, source, classes, boundary, conductance, angles, strengths)


def solution(mesh):
    in_specs = (
        P("gz", None, None, "xy", None),
        P("gz", None, None, "xy", None),
        P("gz", "xy", None),
        P("gz", "xy", None),
        P(),
        P(),
        P(),
    )
    out_specs = P("gz", None, None, "xy", None)
    body = functools.partial(local, mesh.shape["gz"], mesh.shape["xy"])
    return jax.shard_map(body, mesh=mesh, in_specs=in_specs, out_specs=out_specs, check_vma=False)
```

```python
import functools

import jax
import jax.numpy as jnp
from jax import lax
from jax.experimental import pallas as pl
from jax.experimental.pallas import tpu as pltpu
from jax.sharding import PartitionSpec as P

SWEEPS = 2
PIECES = 2
VMEM_LIMIT = 62 * 2**20

coupling = 0.1
penalty = 4.0


def mul(a, b):
    return (a[0] * b[0] - a[1] * b[1], a[0] * b[1] + a[1] * b[0])


def add(a, b):
    return (a[0] + b[0], a[1] + b[1])


def inv(a):
    weight = 1.0 / (a[0] * a[0] + a[1] * a[1])
    return (a[0] * weight, -a[1] * weight)


def one_minus(a):
    return (1.0 - a[0], -a[1])


def get(ref, *at):
    return (ref[at + (0,)], ref[at + (1,)])


def put(ref, value, *at):
    ref[at + (0,)] = value[0]
    ref[at + (1,)] = value[1]


def loop(low, high, body, carry, by):
    by = by if (high - low) % by == 0 else 1

    def several(k, carry):
        for i in range(by):
            carry = body(low + k * by + i, carry)
        return carry

    return lax.fori_loop(0, (high - low) // by, several, carry)


def rotation(angles, shape):
    cos = [jnp.cos(jnp.full(shape, angles[i], jnp.float32)) for i in range(3)]
    sin = [jnp.sin(jnp.full(shape, angles[i], jnp.float32)) for i in range(3)]
    (ca, cb, cc), (sa, sb, sc) = cos, sin
    left = [[ca * cb, -sa, ca * sb], [sa * cb, ca, sa * sb], [-sb, jnp.zeros_like(cb), cb]]
    return [[row[0] * cc + row[1] * sc, row[1] * cc - row[0] * sc, row[2]] for row in left]


def relax(
    ngz,
    nxy,
    field,
    source,
    classes,
    boundary,
    conductance,
    angles,
    strengths,
    OUT,
    U,
    S,
    C,
    B,
    SG,
    DR,
    PH,
    PHI,
    PSI,
    T,
    QM,
    EPHI,
    EPSI,
    EH,
    ET,
    ends,
    coef,
    near,
    halo_out,
    halo_in,
    value_in,
    info_in,
    info_out,
    lam_in,
    lam_out,
    own_in,
    own_out,
    ch_in,
    ch_out,
    XR,
    FA,
    CX,
    BX,
    FP,
    FPHI,
    FPSI,
    FT,
    FC,
    far_ends,
    mi_in,
    mi_out,
    in_sems,
    halo_send,
    halo_recv,
    tip_send,
    tip_recv,
    info_send,
    info_recv,
    lam_send,
    lam_recv,
    own_send,
    own_recv,
    ch_send,
    ch_recv,
    far_send,
    far_recv,
    near_ready,
    row_send,
    row_recv,
    early_send,
    early_recv,
    mi_send,
    mi_recv,
):
    ix, iz = lax.axis_index("xy"), lax.axis_index("gz")
    depth, _, _, rows, width = U.shape
    kinds = conductance.shape[0]
    plane = (rows, width)
    has = {
        ("xy", 0): ix > 0,
        ("xy", 1): ix < nxy - 1,
    }
    where_is = {
        ("xy", 0): ix - 1,
        ("xy", 1): ix + 1,
    }
    middle = nxy // 2
    far = (ix == middle, ix == middle - 1)
    is_far = jnp.logical_or(far[0], far[1])
    not_far = jnp.logical_not(is_far)
    helps = (ix == middle + 1, ix == middle - 2)
    helper = jnp.logical_or(helps[0], helps[1])
    pair = jnp.where(far[0], ix + 1, ix - 1)
    beside = [jnp.logical_and(has["xy", side], jnp.logical_not(far[side])) for side in range(2)]
    for steps in (1, 2):
        has["gz", -steps] = iz >= steps
        has["gz", steps] = iz < ngz - steps
        where_is["gz", -steps] = iz - steps
        where_is["gz", steps] = iz + steps
    signals = {}
    for key, there in has.items():
        signals[key] = jnp.logical_and(there, not_far)
        if key[0] == "xy":
            signals[key] = jnp.logical_and(signals[key], jnp.logical_not(helps[key[1]]))
    count = sum(there.astype(jnp.int32) for there in signals.values())
    count += ngz * helper.astype(jnp.int32)
    zs = depth // PIECES
    spans = [pl.ds(piece * zs, zs) for piece in range(PIECES)]
    moves = [(field.at[span], U.at[span]) for span in spans]
    moves += [(classes, C), (boundary, B), (source, S)]
    loads = [
        pltpu.make_async_copy(src, dst, in_sems.at[i]) for i, (src, dst) in enumerate(moves)
    ]
    for load in loads[PIECES : PIECES + 2] + loads[:PIECES] + loads[PIECES + 2 :]:
        load.start()

    barrier = pltpu.get_barrier_semaphore()
    for key, there in signals.items():

        @pl.when(there)
        def _():
            pl.semaphore_signal(
                barrier,
                inc=1,
                device_id={key[0]: where_is[key]},
                device_id_type=pl.DeviceIdType.MESH,
            )


    @pl.when(is_far)
    def _():
        for g in range(ngz):
            pl.semaphore_signal(
                barrier,
                inc=1,
                device_id={"xy": pair, "gz": g},
                device_id_type=pl.DeviceIdType.MESH,
            )
        pl.semaphore_signal(
            barrier,
            inc=1,
            device_id={"xy": jnp.where(far[0], ix - 1, ix + 1)},
            device_id_type=pl.DeviceIdType.MESH,
        )

    def remote(src, dst, send, recv, key):
        return pltpu.make_async_remote_copy(
            src_ref=src,
            dst_ref=dst,
            send_sem=send,
            recv_sem=recv,
            device_id={key[0]: where_is[key]},
            device_id_type=pl.DeviceIdType.MESH,
        )

    def halo_copy(sweep, side, piece):
        span = pl.ds(piece * zs, zs)
        return remote(
            halo_out.at[sweep, side, :, :, span],
            halo_in.at[sweep, side, :, :, span],
            halo_send.at[side],
            halo_recv.at[side, piece],
            ("xy", 1 - side),
        )

    def send_halo(sweep, piece):
        for side in range(2):

            @pl.when(beside[1 - side])
            def _():
                halo_copy(sweep, side, piece).start()

    def early_copy(side, p, c):
        return remote(
            halo_out.at[1, 1 - side, p, c],
            FA.at[:, p, c, :],
            early_send,
            early_recv,
            ("xy", side),
        )

    def early_moved(side):
        return remote(
            halo_out.at[1, 1 - side],
            halo_out.at[1, 1 - side],
            early_send,
            early_recv,
            ("xy", side),
        )

    def row_copy(side, p, c):
        return remote(
            U.at[:, p, c, 0 if side else rows - 1, :],
            halo_in.at[0, side, p, c],
            row_send.at[side],
            row_recv.at[side],
            ("xy", 1 - side),
        )

    row_copies = lambda side: [row_copy(side, p, c) for p in range(2) for c in range(3)]
    rows_moved = lambda side: remote(
        halo_in.at[0, side],
        halo_in.at[0, side],
        row_send.at[side],
        row_recv.at[side],
        ("xy", 1 - side),
    )

    def pack(first, last, z, values):
        for i in range(6):
            at = (i // 3, i % 3, pl.ds(z, 1), slice(None))
            first[at] = values[i][:1, :]
            last[at] = values[i][rows - 1 :, :]

    for side in range(2):

        for sweep in range(SWEEPS):

            @pl.when(jnp.logical_not(beside[side]))
            def _():
                halo_in[sweep, side] = jnp.zeros(halo_in.shape[2:], jnp.float32)

        @pl.when((iz if side == 0 else ngz - 1 - iz) < 2)
        def _():
            for part in range(3, 9):
                info_in[side, part] = jnp.zeros(info_in.shape[2:], jnp.float32)
            lam_in[side] = jnp.zeros(lam_in.shape[1:], jnp.float32)
            for sweep in range(SWEEPS):
                ch_in[sweep, side] = jnp.zeros(ch_in.shape[2:], jnp.float32)

    loads[PIECES].wait()
    loads[PIECES + 1].wait()

    def diagonal(z, carry):
        ids = C[z]
        sigma = jnp.zeros(plane, jnp.float32)
        for kind in range(kinds):
            sigma = jnp.where(ids == kind, conductance[kind], sigma)
        SG[z] = sigma
        DR[z] = 2.0 + 4.0 * coupling + penalty * B[z].astype(jnp.float32)
        return carry

    loop(0, depth, diagonal, 0, 4)

    def diag(z):
        real = jnp.broadcast_to(DR[z][None], (3,) + plane)
        sigma = SG[z]
        return real, jnp.stack([sigma * strengths[j] for j in range(3)])

    none = (jnp.zeros((3,) + plane, jnp.float32),) * 2

    def pivots(k, carry):
        p, q = carry
        z, back = k, depth - 1 - k
        d, f = diag(z), diag(back)
        p = inv((d[0] - p[0], d[1] - p[1]))
        q = inv((f[0] - q[0], f[1] - q[1]))
        put(PH, p, z)
        put(PHI, q, back)
        return p, q

    loop(0, depth, pivots, (none, none), 2)
    ones = (jnp.ones((3,) + plane, jnp.float32), none[0])

    def columns(k, carry):
        down, up = carry
        z, back = k, depth - 1 - k
        down = mul(get(PHI, z), down)
        up = mul(get(PH, back), up)
        put(PHI, down, z)
        put(PSI, up, back)
        return down, up

    loop(0, depth, columns, (ones, ones), 2)
    for piece in range(PIECES):
        loads[piece].wait()

    @pl.when(not_far)
    def _():
        pl.semaphore_wait(barrier, count)

    @pl.when(helper)
    def _():
        pl.semaphore_signal(
            near_ready,
            inc=1,
            device_id={"xy": jnp.where(helps[0], ix - 1, ix + 1)},
            device_id_type=pl.DeviceIdType.MESH,
        )

    @pl.when(is_far)
    def _():
        pl.semaphore_wait(near_ready, 1)

    for side in range(2):

        @pl.when(beside[1 - side])
        def _():
            for copy in row_copies(side):
                copy.start()

    LEFT, RIGHT = 0, 1
    tip = (lambda: get(PHI, 0), lambda: get(PSI, depth - 1))
    across = lambda: get(PSI, 0)

    place = (iz, ngz - 1 - iz)
    even = [lax.rem(k, 2) == 0 for k in place]
    odd = [lax.rem(k, 2) == 1 for k in place]
    onward = [ngz - 1 - k for k in place]

    def to(side, steps):
        return {"gz": iz + steps if side == LEFT else iz - steps}

    def chain_copy(src, dst, send, recv, side, steps):
        return pltpu.make_async_remote_copy(
            src_ref=src,
            dst_ref=dst,
            send_sem=send,
            recv_sem=recv,
            device_id=to(side, steps),
            device_id_type=pl.DeviceIdType.MESH,
        )

    whole = slice(None)
    way = (lambda side: 0) if ngz == 4 else (lambda side: side)

    def tip_copy(side, j):
        return chain_copy(
            info_out.at[side, j],
            info_in.at[side, j],
            tip_send.at[way(side)],
            tip_recv.at[way(side), j],
            side,
            1,
        )

    def info_copy(side):
        return chain_copy(
            info_out.at[side, 3:9],
            info_in.at[side, 3:9],
            info_send.at[way(side)],
            info_recv.at[way(side)],
            side,
            1,
        )

    def lam_copy(side, steps, j):
        return chain_copy(
            lam_out.at[side, j],
            lam_in.at[side, j],
            lam_send.at[way(side), steps - 1],
            lam_recv.at[way(side), j],
            side,
            steps,
        )

    def own_copy(sweep, side, j):
        return chain_copy(
            own_out.at[sweep, side, j],
            own_in.at[sweep, side, j],
            own_send.at[sweep, way(side)],
            own_recv.at[sweep, way(side), j],
            side,
            1,
        )

    def x_copy(sweep, side, steps, j):
        return chain_copy(
            ch_out.at[sweep, side, j],
            ch_in.at[sweep, side, j],
            ch_send.at[sweep, way(side), steps - 1],
            ch_recv.at[sweep, way(side), j],
            side,
            steps,
        )


    both = jnp.logical_and

    def send_info(side):
        sends = both(even[side], onward[side] >= 1)
        parts = (tip[1 - side](), tip[side](), across())
        for part in range(3):
            for j in range(3):
                for p in range(2):
                    info_out[side, part * 3 + j, p] = parts[part][p][j]
            if part == 0:

                @pl.when(sends)
                def _():
                    for j in range(3):
                        tip_copy(side, j).start()

        @pl.when(both(sends, place[side] > 0))
        def _():
            info_copy(side).start()

    def pass_lam(side):
        @pl.when(both(odd[side], place[side] >= 2))
        def _():
            info_copy(side).wait_recv()

        for j in range(3):

            @pl.when(odd[side])
            def _():
                tip_copy(side, j).wait_recv()

            @pl.when(place[side] >= 2)
            def _():
                lam_copy(side, 1, j).wait_recv()

            tips = [(info_in[side, 3 * k + j, 0], info_in[side, 3 * k + j, 1]) for k in range(3)]
            given = (lam_in[side, j, 0], lam_in[side, j, 1])

            @pl.when(odd[side])
            def _():
                skip = mul(tips[2], inv(one_minus(mul(tips[1], given))))
                lam = add(tips[0], mul(tips[2], mul(skip, given)))
                for p in range(2):
                    coef[8 + side, p, j] = skip[p]
                    coef[10 + side, p, j] = lam[p]

            @pl.when(even[side])
            def _():
                for p in range(2):
                    coef[10 + side, p, j] = given[p]

            of = lambda pair: (pair[0][j], pair[1][j])
            lam = (coef[10 + side, 0, j], coef[10 + side, 1, j])
            kappa = mul(of(across()), inv(one_minus(mul(of(tip[side]()), lam))))
            over = mul(kappa, lam)
            value = add(of(tip[1 - side]()), mul(of(across()), over))
            for p in range(2):
                coef[side, p, j] = kappa[p]
                coef[2 + side, p, j] = over[p]
                lam_out[side, j, p] = value[p]

            @pl.when(both(odd[side], onward[side] >= 1))
            def _():
                lam_copy(side, 1, j).start()

        @pl.when(both(odd[side], onward[side] >= 2))
        def _():
            for j in range(3):
                lam_copy(side, 2, j).start()

    def own_base(side, j):
        return add(
            (ends[1 - side, 0, j], ends[1 - side, 1, j]),
            mul(
                (coef[2 + side, 0, j], coef[2 + side, 1, j]),
                (ends[side, 0, j], ends[side, 1, j]),
            ),
        )

    def own_sum(sweep, side):
        for j in range(3):
            base = own_base(side, j)
            for p in range(2):
                own_out[sweep, side, j, p] = base[p]

            @pl.when(both(even[side], onward[side] >= 1))
            def _():
                own_copy(sweep, side, j).start()

    def pass_chain(sweep, side):
        for j in range(3):
            base = own_base(side, j)

            @pl.when(odd[side])
            def _():
                own_copy(sweep, side, j).wait_recv()

            @pl.when(place[side] >= 2)
            def _():
                x_copy(sweep, side, 1, j).wait_recv()

            given = (ch_in[sweep, side, j, 0], ch_in[sweep, side, j, 1])

            @pl.when(odd[side])
            def _():
                own = (own_in[sweep, side, j, 0], own_in[sweep, side, j, 1])
                x = add(own, mul((coef[8 + side, 0, j], coef[8 + side, 1, j]), given))
                for p in range(2):
                    value_in[side, j, p] = x[p]

            @pl.when(even[side])
            def _():
                for p in range(2):
                    value_in[side, j, p] = given[p]

            x = (value_in[side, j, 0], value_in[side, j, 1])
            result = add(base, mul((coef[side, 0, j], coef[side, 1, j]), x))
            for p in range(2):
                ch_out[sweep, side, j, p] = result[p]

            @pl.when(both(odd[side], onward[side] >= 2))
            def _():
                x_copy(sweep, side, 2, j).start()

        @pl.when(both(odd[side], onward[side] >= 1))
        def _():
            for j in range(3):
                x_copy(sweep, side, 1, j).start()

    left_first = iz * 2 < ngz - 1

    def near_side(run):
        @pl.when(left_first)
        def _():
            run(LEFT)

        @pl.when(jnp.logical_not(left_first))
        def _():
            run(RIGHT)

    def far_side(run):
        @pl.when(left_first)
        def _():
            run(RIGHT)

        @pl.when(jnp.logical_not(left_first))
        def _():
            run(LEFT)

    def far_source(side, i):
        edge = pl.ds(rows - 1 if side else 0, 1)
        return (C.at[:, edge, :], B.at[:, edge, :])[i] if i < 2 else U.at[:, :, i - 2, edge, :]

    def far_target(i, first):
        at = pl.ds(first if i < 2 else first + i - 2, 1)
        return (CX.at[0, :, at, :], BX.at[0, :, at, :])[i] if i < 2 else XR.at[:, :, at, :]

    def far_copy(side, i):
        return pltpu.make_async_remote_copy(
            src_ref=far_source(side, i),
            dst_ref=far_target(i, 4 if i < 2 else 0),
            send_sem=far_send.at[min(i, 2)],
            recv_sem=far_recv.at[min(i, 2)],
            device_id={"xy": ix + 1 if side else ix - 1},
            device_id_type=pl.DeviceIdType.MESH,
        )

    def kept_copy(side, i):
        return pltpu.make_async_copy(
            far_source(side, i), far_target(i, 0 if i < 2 else 4), in_sems.at[min(i, 2)]
        )

    def field_moved(side):
        return pltpu.make_async_remote_copy(
            src_ref=XR.at[:, :, 0:3, :],
            dst_ref=XR.at[:, :, 0:3, :],
            send_sem=far_send.at[2],
            recv_sem=far_recv.at[2],
            device_id={"xy": ix + 1 if side else ix - 1},
            device_id_type=pl.DeviceIdType.MESH,
        )

    def field_kept():
        return pltpu.make_async_copy(XR.at[:, :, 4:7, :], XR.at[:, :, 4:7, :], in_sems.at[2])

    def lines_kept(i):
        ref = (CX, BX)[i].at[1, :, 0:2, :]
        return pltpu.make_async_copy(ref, ref, in_sems.at[3 + i])

    def line_copy(side, i):
        first = rows - 1 if side else 0
        edge = pl.ds(first if i < 2 else (first - 1 if side else first + 1), 1)
        at = pl.ds(0 if i < 2 else 4, 1)
        return pltpu.make_async_copy(
            (C, B)[i % 2].at[:, edge, :], (CX, BX)[i % 2].at[1, :, at, :], in_sems.at[3 + i % 2]
        )

    def far_begin():
        pl.semaphore_wait(barrier, 1)
        for side in range(2):

            @pl.when(far[side])
            def _():
                for i in range(5):
                    far_copy(side, i).start()
                for i in range(5):
                    kept_copy(side, i).start()
                for i in range(4):
                    line_copy(side, i).start()

    def near_lam(side):
        pl.when(place[side] < 2)(functools.partial(pass_lam, side))

    def far_lam(side):
        pl.when(place[side] == 2)(functools.partial(pass_lam, side))

    def last_lam(side):
        pl.when(place[side] >= 3)(functools.partial(pass_lam, side))

    near_side(send_info)
    far_side(send_info)

    angle_matrix = rotation(angles, (rows, 128))
    for c in range(3):
        for j in range(3):
            QM[c, j] = angle_matrix[c][j]

    def matrix():
        return [
            [jnp.concatenate([QM[c, j]] * (width // 128), axis=1) for j in range(3)]
            for c in range(3)
        ]

    def pack_columns(z, carry):
        for src, dst in ((PHI, EPHI), (PSI, EPSI)):
            pack(dst.at[0], dst.at[1], z, [src[z, i // 3, i % 3] for i in range(6)])
        return carry

    loop(0, depth, pack_columns, 0, 4)

    row = lax.broadcasted_iota(jnp.int32, plane, 0)
    lane = lax.broadcasted_iota(jnp.int32, plane, 1)
    zero = jnp.zeros(plane, jnp.float32)

    def turn(q, driven):
        return [
            jnp.stack(
                [
                    q[0][j] * driven[p][0] + q[1][j] * driven[p][1] + q[2][j] * driven[p][2]
                    for j in range(3)
                ]
            )
            for p in range(2)
        ]

    def inner(z, carry):
        first, last = carry
        q = matrix()
        driven = []
        for p in range(2):
            of = []
            for c in range(3):
                u = U[z, p, c]
                around = jnp.where(lane == 0, zero, pltpu.roll(u, 1, 1))
                around += jnp.where(lane == width - 1, zero, pltpu.roll(u, width - 1, 1))
                around += jnp.where(row == 0, zero, pltpu.roll(u, 1, 0))
                around += jnp.where(row == rows - 1, zero, pltpu.roll(u, rows - 1, 0))
                of.append(S[z, p, c] + coupling * around)
            driven.append(of)
        turned = turn(q, driven)
        put(T, turned, z)
        return add(first, mul(get(PHI, z), turned)), add(last, mul(get(PSI, z), turned))

    tiles = [pl.ds(z, rows) for z in range(0, depth, rows)]

    def outer(sweep, side, tile, carry):
        first, last = carry
        q = matrix()
        turned = turn(
            q,
            [[coupling * halo_in[sweep, side, p, c, tile] for c in range(3)] for p in range(2)],
        )
        for p in range(2):
            EH[side, p, :, tile] = turned[p]
        phi = [EPHI[side, p, :, tile] for p in range(2)]
        psi = [EPSI[side, p, :, tile] for p in range(2)]
        return add(first, mul(phi, turned)), add(last, mul(psi, turned))

    third = lax.rem(row, 4)
    part = lambda k: third == k
    used = third < 3

    def mi_copy(k, steps, parts):
        slot = steps + 3 if steps < 0 else steps + 2
        return pltpu.make_async_remote_copy(
            src_ref=mi_out.at[k, parts],
            dst_ref=mi_in.at[k, 5 - slot, parts],
            send_sem=mi_send.at[slot],
            recv_sem=mi_recv.at[0 if k == whole else k, 5 - slot],
            device_id={"gz": iz + steps},
            device_id_type=pl.DeviceIdType.MESH,
        )

    all_steps = (-3, -2, -1, 1, 2, 3)
    at_end = lambda k: jnp.logical_or(k == 0, k == ngz - 1)

    def for_all(of, act):
        for steps in all_steps:
            there = (iz + steps >= 0) & (iz + steps < ngz)
            edge_ = at_end(iz + steps * of)

            @pl.when(jnp.logical_and(there, edge_))
            def _():
                act(steps, True)

            @pl.when(jnp.logical_and(there, jnp.logical_not(edge_)))
            def _():
                act(steps, False)

    def to_all(k, first):
        def act(steps, ends_only):
            if not ends_only:
                parts = pl.ds(first, 4 if first else 6)
            else:
                parts = pl.ds(first + (2 if steps > 0 else 0), 2)
            mi_copy(k, steps, parts).start()

        for_all(0, act)

    def moved(ends_only):
        return pl.ds(0, 4 if ends_only else 10)

    def from_all(k):
        for_all(1, lambda steps, e: mi_copy(k, -steps, moved(e)).wait_recv())

    def shifts(of):
        planes = []
        for d in (-2, -1, 0, 1, 2):
            plane_ = zero
            for j in range(3):
                if 0 <= j + d <= 2:
                    plane_ = jnp.where(part(j), of(j, j + d), plane_)
            planes.append((d, plane_))
        return planes

    def mix(planes, x):
        total = None
        for d, plane_ in planes:
            term = plane_ * (x if d == 0 else pltpu.roll(x, (rows - d) % rows, 0))
            total = term if total is None else total + term
        return total

    def far_clear():
        none_ = jnp.zeros((2,) + plane, jnp.float32)
        for slot, steps in enumerate(all_steps):
            there = (iz + steps >= 0) & (iz + steps < ngz)

            @pl.when(jnp.logical_not(there))
            def _():
                for k in range(2):
                    for part_ in range(5):
                        mi_in[k, slot, 2 * part_ : 2 * part_ + 2] = none_

            @pl.when(jnp.logical_and(there, at_end(iz + steps)))
            def _():
                for k in range(2):
                    for part_ in (0, 2, 3) if steps < 0 else (1, 2, 4):
                        mi_in[k, slot, 2 * part_ : 2 * part_ + 2] = none_

    def far_setup():
        q = matrix()
        for i, (_, plane_) in enumerate(shifts(lambda j, k: q[k][j])):
            FC[i] = plane_
        for i, (_, plane_) in enumerate(shifts(lambda j, k: q[j][k])):
            FC[5 + i] = plane_
        strength = jnp.full(plane, strengths[0], jnp.float32)
        for j in (1, 2):
            strength = jnp.where(part(j), strengths[j], strength)
        FC[10] = strength

    own = row < 4

    def far_first(k):
        for side in range(2):

            @pl.when(far[side])
            def _():
                if k == 0:
                    for i in range(2):
                        kept_copy(side, i).wait()
                        far_copy(side, i).wait_recv()
                else:
                    for i in range(2):
                        lines_kept(i).wait()

        def far_diagonal(z, carry):
            ids_tile, bound = CX[k, z], BX[k, z]
            ids = jnp.where(
                own,
                jnp.broadcast_to(ids_tile[0:1, :], plane),
                jnp.broadcast_to(ids_tile[4:5, :], plane),
            )
            edge = jnp.where(
                own, jnp.broadcast_to(bound[0:1, :], plane), jnp.broadcast_to(bound[4:5, :], plane)
            )
            sigma = jnp.zeros(plane, jnp.float32)
            for kind in range(kinds):
                sigma = jnp.where(ids == kind, conductance[kind], sigma)
            FT[k, z, 0] = 2.0 + 4.0 * coupling + penalty * edge.astype(jnp.float32)
            FT[k, z, 1] = sigma * FC[10]
            return carry

        loop(0, depth, far_diagonal, 0, 4)

        def far_pivots(z, carry):
            p, q = carry
            d, f = get(FT, k, z), get(FT, k, depth - 1 - z)
            p = inv((d[0] - p[0], d[1] - p[1]))
            q = inv((f[0] - q[0], f[1] - q[1]))
            put(FP, p, k, z)
            put(FPHI, q, k, depth - 1 - z)
            return p, q

        loop(0, depth, far_pivots, ((zero, zero), (zero, zero)), 2)
        one = jnp.ones(plane, jnp.float32)

        def far_columns(z, carry):
            down, up = carry
            back = depth - 1 - z
            down = mul(get(FPHI, k, z), down)
            up = mul(get(FP, k, back), up)
            put(FPHI, down, k, z)
            put(FPSI, up, k, back)
            return down, up

        loop(0, depth, far_columns, ((one, zero), (one, zero)), 2)
        ends_ = (get(FPHI, k, 0), get(FPSI, k, depth - 1), get(FPSI, k, 0))
        for i, value in enumerate(ends_):
            mi_out[k, 2 * i] = value[0]
            mi_out[k, 2 * i + 1] = value[1]

    def send_columns(k):
        to_all(k, 0)

    def far_solve(k, rhs):
        turned_by = [(d, FC[i]) for i, d in enumerate((-2, -1, 0, 1, 2))]

        def far_sums(z, carry):
            first, last = carry
            t = tuple(
                mix(turned_by, jnp.where(used, coupling * rhs(z, p), zero)) for p in range(2)
            )
            put(FT, t, k, z)
            return add(first, mul(get(FPHI, k, z), t)), add(last, mul(get(FPSI, k, z), t))

        first, last = loop(0, depth, far_sums, ((zero, zero), (zero, zero)), 4)
        for i, value in enumerate((first, last)):
            mi_out[k, 6 + 2 * i] = value[0]
            mi_out[k, 7 + 2 * i] = value[1]
        to_all(k, 6)

        def far_forward(z, m):
            m = mul(get(FP, k, z), add(get(FT, k, z), m))
            put(FT, m, k, z)
            return m

        def far_backward(i, w):
            z = depth - 1 - i
            w = add(get(FT, k, z), mul(get(FP, k, z), w))
            put(FT, w, k, z)
            return w

        loop(0, depth, far_forward, (zero, zero), 4)
        loop(0, depth, far_backward, (zero, zero), 4)

    def far_second():
        for side in range(2):

            @pl.when(far[side])
            def _():
                field_moved(side).wait_recv()

        far_solve(0, lambda z, p: XR[z, p])

    def far_meet(k, take):
        from_all(k)
        block = lambda slot: [(mi_in[k, slot, 2 * i], mi_in[k, slot, 2 * i + 1]) for i in range(5)]
        x = lam = y = mu = (zero, zero)
        for slot in range(3):
            top, bottom, cross, first, last = block(slot)
            det = inv(one_minus(mul(top, lam)))
            x, lam = (
                add(last, mul(cross, mul(det, add(x, mul(lam, first))))),
                add(bottom, mul(mul(cross, cross), mul(det, lam))),
            )
        for slot in (5, 4, 3):
            top, bottom, cross, first, last = block(slot)
            det = inv(one_minus(mul(bottom, mu)))
            y, mu = (
                add(first, mul(cross, mul(det, add(y, mul(mu, last))))),
                add(top, mul(mul(cross, cross), mul(det, mu))),
            )
        top, bottom, cross, first, last = [(mi_out[k, 2 * i], mi_out[k, 2 * i + 1]) for i in range(5)]
        g, h = add(x, mul(lam, first)), add(y, mul(mu, last))
        alpha, beta = one_minus(mul(lam, top)), one_minus(mul(mu, bottom))
        lc, mc = mul(lam, cross), mul(mu, cross)
        both_ = mul(lc, mc)
        all_ = mul(alpha, beta)
        det = inv((all_[0] - both_[0], all_[1] - both_[1]))
        put(far_ends, mul(det, add(mul(g, beta), mul(lc, h))), 0)
        put(far_ends, mul(det, add(mul(h, alpha), mul(mc, g))), 1)
        back_by = [(d, FC[5 + i]) for i, d in enumerate((-2, -1, 0, 1, 2))]

        def far_join(z, carry):
            before, after = get(far_ends, 0), get(far_ends, 1)
            w = add(
                add(get(FT, k, z), mul(get(FPHI, k, z), before)), mul(get(FPSI, k, z), after)
            )
            for p in range(2):
                take(z, p, mix(back_by, w[p]))
            return carry

        loop(0, depth, far_join, 0, 4)

    def far_third():
        def keep(z, p, u):
            FT[0, z, p] = u

        far_meet(0, keep)
        for side in range(2):

            @pl.when(far[side])
            def _():
                early_moved(side).wait_recv()

        def rhs(z, p):
            u = FT[0, z, p]
            beside_ = jnp.where(lane == 0, zero, pltpu.roll(u, 1, 1))
            beside_ += jnp.where(lane == width - 1, zero, pltpu.roll(u, width - 1, 1))
            early = jnp.where(row < 3, FA[z, p], zero)
            return pltpu.roll(u, 4, 0) + jnp.where(own, beside_ + early, zero)

        far_solve(1, rhs)

    def far_last():
        here = row == jnp.where(far[1], rows - 1, 0)
        next_ = row == jnp.where(far[1], rows - 2, 1)

        def give(z, p, u):
            for c in range(3):
                OUT[z, p, c] += jnp.where(
                    here,
                    jnp.broadcast_to(u[c : c + 1, :], plane),
                    jnp.where(next_, jnp.broadcast_to(u[4 + c : 5 + c, :], plane), zero),
                )

        far_meet(1, give)

    loads[PIECES + 2].wait()
    for sweep in range(SWEEPS):
        sums = loop(0, depth, inner, (none, none), 4)
        if sweep == 0:
            near_side(near_lam)
        halves = [(none, none), (none, none)]
        for piece in range(PIECES):
            for side in range(2):

                if sweep == 0 and piece == 0:

                    @pl.when(beside[side])
                    def _():
                        rows_moved(side).wait_recv()

                if sweep:

                    @pl.when(beside[side])
                    def _():
                        halo_copy(sweep, side, piece).wait_recv()

                for tile in tiles[piece * len(tiles) // PIECES : (piece + 1) * len(tiles) // PIECES]:
                    halves[side] = outer(sweep, side, tile, halves[side])
        for side in range(2):
            here = row == (0 if side == 0 else rows - 1)
            sums = tuple(
                add(
                    sums[end],
                    tuple(
                        jnp.where(here[None], jnp.sum(part, axis=1, keepdims=True), 0.0)
                        for part in halves[side][end]
                    ),
                )
                for end in range(2)
            )
        put(ends, sums[0], 0)
        put(ends, sums[1], 1)

        near_side(functools.partial(own_sum, sweep))
        if sweep == 0:
            pl.when(is_far)(far_begin)
            far_side(far_lam)
        far_side(functools.partial(own_sum, sweep))
        if sweep:

            @pl.when(is_far)
            def _():
                far_second()

        near_side(functools.partial(pass_chain, sweep))

        def forward(z, m):
            given = []
            for p in range(2):
                edges = []
                for j in range(3):
                    above = jnp.broadcast_to(EH[0, p, j, pl.ds(z, 1), :], plane)
                    below = jnp.broadcast_to(EH[1, p, j, pl.ds(z, 1), :], plane)
                    edges.append(
                        jnp.where(row == 0, above, zero) + jnp.where(row == rows - 1, below, zero)
                    )
                given.append(T[z, p] + jnp.stack(edges))
            m = mul(get(PH, z), add(given, m))
            put(T, m, z)
            return m

        def backward(k, w):
            z = depth - 1 - k
            w = add(get(T, z), mul(get(PH, z), w))
            put(T, w, z)
            if sweep < SWEEPS - 1:
                pack(ET.at[0], ET.at[1], z, [w[i // 3][i % 3] for i in range(6)])
            return w

        loop(0, depth, forward, none, 4)
        loop(0, depth, backward, none, 4)
        if sweep:

            @pl.when(is_far)
            def _():
                send_columns(1)
                far_third()

        else:

            @pl.when(is_far)
            def _():
                far_clear()
                far_setup()
                far_first(1)

        if sweep == 0:
            far_side(last_lam)
            for side in range(2):
                lam = get(coef, 10 + side)
                away = tuple(
                    jnp.stack([lam_out[1 - side, j, p] for j in range(3)]) for p in range(2)
                )
                det = inv(one_minus(mul(lam, away)))
                put(coef, det, 6 + side)
                put(coef, mul(det, lam), 4 + side)
        far_side(functools.partial(pass_chain, sweep))

        for side in range(2):
            for j in range(3):
                arrived = (value_in[side, j, 0], value_in[side, j, 1])
                other = (ch_out[sweep, 1 - side, j, 0], ch_out[sweep, 1 - side, j, 1])
                value = add(
                    mul((coef[6 + side, 0, j], coef[6 + side, 1, j]), arrived),
                    mul((coef[4 + side, 0, j], coef[4 + side, 1, j]), other),
                )
                near[side, 0, j] = value[0]
                near[side, 1, j] = value[1]

        final = sweep == SWEEPS - 1

        def join_edge(side, tile):
            q = matrix()
            r = 0 if side == 0 else rows - 1
            w = [ET[side, p, :, tile] for p in range(2)]
            for end, column in ((0, EPHI), (1, EPSI)):
                entry = [
                    jnp.broadcast_to(near[end, p, :, r : r + 1, :], (3,) + plane)
                    for p in range(2)
                ]
                w = add(w, mul([column[side, p, :, tile] for p in range(2)], entry))
            for p in range(2):
                for c in range(3):
                    halo_out[sweep + 1, 1 - side, p, c, tile] = (
                        q[c][0] * w[p][0] + q[c][1] * w[p][1] + q[c][2] * w[p][2]
                    )

        if not final:
            for piece in range(PIECES):
                for tile in tiles[piece * len(tiles) // PIECES : (piece + 1) * len(tiles) // PIECES]:
                    for side in range(2):
                        join_edge(side, tile)
                send_halo(sweep + 1, piece)
            for side in range(2):

                @pl.when(far[side])
                def _():
                    for p in range(2):
                        for c in range(3):
                            early_copy(side, p, c).start()


        def join(z, carry):
            q = matrix()
            before, after = get(near, 0), get(near, 1)
            w = add(add(get(T, z), mul(get(PHI, z), before)), mul(get(PSI, z), after))
            values = []
            for p in range(2):
                for c in range(3):
                    values.append(q[c][0] * w[p][0] + q[c][1] * w[p][1] + q[c][2] * w[p][2])
            target = OUT if final else U
            for i in range(6):
                target[z, i // 3, i % 3] = values[i]
            return carry

        if not final:
            for side in range(2):

                @pl.when(far[side])
                def _():
                    for i in range(2):
                        far_copy(side, i).wait_send()
                    field_moved(side).wait_send()
                    field_kept().wait()

                @pl.when(beside[1 - side])
                def _():
                    rows_moved(side).wait_send()

        loop(0, depth, join, 0, 4)

        if not final:


            @pl.when(is_far)
            def _():
                far_first(0)
                send_columns(0)

        else:
            pl.when(is_far)(far_last)

    @pl.when(is_far)
    def _():
        for_all(0, lambda steps, e: mi_copy(whole, steps, moved(e)).wait_send())

    for side in range(2):

        @pl.when(beside[1 - side])
        def _():
            remote(
                halo_out.at[1, side],
                halo_in.at[1, side],
                halo_send.at[side],
                halo_recv.at[side, 0],
                ("xy", 1 - side),
            ).wait_send()

        @pl.when(far[side])
        def _():
            early_moved(side).wait_send()

        sends = both(even[side], onward[side] >= 1)

        @pl.when(sends)
        def _():
            chain_copy(
                info_out.at[side, 0:3],
                info_in.at[side, 0:3],
                tip_send.at[way(side)],
                info_recv.at[way(side)],
                side,
                1,
            ).wait_send()
            for sweep in range(SWEEPS):
                own_copy(sweep, side, whole).wait_send()

        @pl.when(both(sends, place[side] > 0))
        def _():
            info_copy(side).wait_send()

        for steps in (2, 1):

            @pl.when(both(odd[side], onward[side] >= steps))
            def _():
                lam_copy(side, steps, whole).wait_send()
                for sweep in range(SWEEPS):
                    x_copy(sweep, side, steps, whole).wait_send()


def local(ngz, nxy, field, source, classes, boundary, conductance, angles, strengths):
    depth, _, _, rows, width = field.shape
    f32 = jnp.float32
    block = pltpu.VMEM(field.shape, f32)
    flat = (depth, rows, width)
    line = (2, 3, rows, width)
    pair = (2, rows, width)
    edge = (2, 2, 3, depth, width)
    narrow = pltpu.VMEM((depth, 2, rows, width), f32)
    lines = pltpu.VMEM((2, depth, 2, rows, width), f32)
    dma = pltpu.SemaphoreType.DMA
    ways = 1 if ngz == 4 else 2
    hbm = pl.BlockSpec(memory_space=pl.ANY)
    smem = pl.BlockSpec(memory_space=pltpu.SMEM)
    return pl.pallas_call(
        functools.partial(relax, ngz, nxy),
        out_shape=pltpu.VMEM(field.shape, f32),
        in_specs=[hbm] * 4 + [smem] * 3,
        out_specs=pl.BlockSpec(memory_space=pltpu.VMEM),
        scratch_shapes=[
            block,
            block,
            pltpu.VMEM(flat, jnp.int32),
            pltpu.VMEM(flat, jnp.int32),
            pltpu.VMEM(flat, f32),
            pltpu.VMEM(flat, f32),
            block,
            block,
            block,
            block,
            pltpu.VMEM((3, 3, rows, 128), f32),
            pltpu.VMEM(edge, f32),
            pltpu.VMEM(edge, f32),
            pltpu.VMEM(edge, f32),
            pltpu.VMEM(edge, f32),
            pltpu.VMEM((2,) + line, f32),
            pltpu.VMEM((14,) + line, f32),
            pltpu.VMEM((2,) + line, f32),
            pltpu.VMEM((SWEEPS,) + edge, f32),
            pltpu.VMEM((SWEEPS,) + edge, f32),
            pltpu.VMEM((2, 3) + pair, f32),
            pltpu.VMEM((2, 9) + pair, f32),
            pltpu.VMEM((2, 9) + pair, f32),
            pltpu.VMEM((2, 3) + pair, f32),
            pltpu.VMEM((2, 3) + pair, f32),
            pltpu.VMEM((SWEEPS, 2, 3) + pair, f32),
            pltpu.VMEM((SWEEPS, 2, 3) + pair, f32),
            pltpu.VMEM((SWEEPS, 2, 3) + pair, f32),
            pltpu.VMEM((SWEEPS, 2, 3) + pair, f32),
            narrow,
            narrow,
            pltpu.VMEM((2,) + flat, jnp.int32),
            pltpu.VMEM((2,) + flat, jnp.int32),
            lines,
            lines,
            lines,
            lines,
            pltpu.VMEM((11, rows, width), f32),
            pltpu.VMEM((2,) + pair, f32),
            pltpu.VMEM((2, 6, 10, rows, width), f32),
            pltpu.VMEM((2, 10, rows, width), f32),
            dma((PIECES + 3,)),
            dma((2,)),
            dma((2, PIECES)),
            dma((ways,)),
            dma((ways, 3)),
            dma((ways,)),
            dma((ways,)),
            dma((ways, 2)),
            dma((ways, 3)),
            dma((SWEEPS, ways)),
            dma((SWEEPS, ways, 3)),
            dma((SWEEPS, ways, 2)),
            dma((SWEEPS, ways, 3)),
            dma((3,)),
            dma((3,)),
            pltpu.SemaphoreType.REGULAR,
            dma((2,)),
            dma((2,)),
            dma(()),
            dma(()),
            dma((6,)),
            dma((2, 6)),
        ],
        compiler_params=pltpu.CompilerParams(collective_id=0, has_side_effects=True, vmem_limit_bytes=VMEM_LIMIT),
    )(field, source, classes, boundary, conductance, angles, strengths)


def solution(mesh):
    in_specs = (
        P("gz", None, None, "xy", None),
        P("gz", None, None, "xy", None),
        P("gz", "xy", None),
        P("gz", "xy", None),
        P(),
        P(),
        P(),
    )
    out_specs = P("gz", None, None, "xy", None)
    body = functools.partial(local, mesh.shape["gz"], mesh.shape["xy"])
    return jax.shard_map(body, mesh=mesh, in_specs=in_specs, out_specs=out_specs, check_vma=False)
```

```python
import functools

import jax
import jax.numpy as jnp
from jax import lax
from jax.experimental import pallas as pl
from jax.experimental.pallas import tpu as pltpu
from jax.sharding import PartitionSpec as P

SWEEPS = 2
PIECES = 2
VMEM_LIMIT = 62 * 2**20

coupling = 0.1
penalty = 4.0


def mul(a, b):
    return (a[0] * b[0] - a[1] * b[1], a[0] * b[1] + a[1] * b[0])


def add(a, b):
    return (a[0] + b[0], a[1] + b[1])


def inv(a):
    weight = 1.0 / (a[0] * a[0] + a[1] * a[1])
    return (a[0] * weight, -a[1] * weight)


def one_minus(a):
    return (1.0 - a[0], -a[1])


def get(ref, *at):
    return (ref[at + (0,)], ref[at + (1,)])


def put(ref, value, *at):
    ref[at + (0,)] = value[0]
    ref[at + (1,)] = value[1]


def loop(low, high, body, carry, by):
    by = by if (high - low) % by == 0 else 1

    def several(k, carry):
        for i in range(by):
            carry = body(low + k * by + i, carry)
        return carry

    return lax.fori_loop(0, (high - low) // by, several, carry)


def rotation(angles, shape):
    cos = [jnp.cos(jnp.full(shape, angles[i], jnp.float32)) for i in range(3)]
    sin = [jnp.sin(jnp.full(shape, angles[i], jnp.float32)) for i in range(3)]
    (ca, cb, cc), (sa, sb, sc) = cos, sin
    left = [[ca * cb, -sa, ca * sb], [sa * cb, ca, sa * sb], [-sb, jnp.zeros_like(cb), cb]]
    return [[row[0] * cc + row[1] * sc, row[1] * cc - row[0] * sc, row[2]] for row in left]


def relax(
    ngz,
    nxy,
    field,
    source,
    classes,
    boundary,
    conductance,
    angles,
    strengths,
    OUT,
    U,
    S,
    C,
    B,
    SG,
    DR,
    PH,
    PHI,
    PSI,
    T,
    QM,
    EPHI,
    EPSI,
    EH,
    ET,
    ends,
    coef,
    near,
    halo_out,
    halo_in,
    value_in,
    info_in,
    info_out,
    lam_in,
    lam_out,
    own_in,
    own_out,
    ch_in,
    ch_out,
    XR,
    FA,
    CX,
    BX,
    FP,
    FPHI,
    FPSI,
    FT,
    FC,
    far_ends,
    mi_in,
    mi_out,
    in_sems,
    halo_send,
    halo_recv,
    tip_send,
    tip_recv,
    info_send,
    info_recv,
    lam_send,
    lam_recv,
    own_send,
    own_recv,
    ch_send,
    ch_recv,
    far_send,
    far_recv,
    near_ready,
    row_send,
    row_recv,
    early_send,
    early_recv,
    mi_send,
    mi_recv,
):
    ix, iz = lax.axis_index("xy"), lax.axis_index("gz")
    depth, _, _, rows, width = U.shape
    kinds = conductance.shape[0]
    plane = (rows, width)
    has = {
        ("xy", 0): ix > 0,
        ("xy", 1): ix < nxy - 1,
    }
    where_is = {
        ("xy", 0): ix - 1,
        ("xy", 1): ix + 1,
    }
    middle = nxy // 2
    far = (ix == middle, ix == middle - 1)
    is_far = jnp.logical_or(far[0], far[1])
    not_far = jnp.logical_not(is_far)
    helps = (ix == middle + 1, ix == middle - 2)
    helper = jnp.logical_or(helps[0], helps[1])
    pair = jnp.where(far[0], ix + 1, ix - 1)
    beside = [jnp.logical_and(has["xy", side], jnp.logical_not(far[side])) for side in range(2)]
    for steps in (1, 2):
        has["gz", -steps] = iz >= steps
        has["gz", steps] = iz < ngz - steps
        where_is["gz", -steps] = iz - steps
        where_is["gz", steps] = iz + steps
    signals = {}
    for key, there in has.items():
        signals[key] = jnp.logical_and(there, not_far)
        if key[0] == "xy":
            signals[key] = jnp.logical_and(signals[key], jnp.logical_not(helps[key[1]]))
    count = sum(there.astype(jnp.int32) for there in signals.values())
    count += ngz * helper.astype(jnp.int32)
    zs = depth // PIECES
    spans = [pl.ds(piece * zs, zs) for piece in range(PIECES)]
    moves = [(field.at[span], U.at[span]) for span in spans]
    moves += [(classes, C), (boundary, B), (source, S)]
    loads = [
        pltpu.make_async_copy(src, dst, in_sems.at[i]) for i, (src, dst) in enumerate(moves)
    ]
    for load in loads[PIECES : PIECES + 2] + loads[:PIECES] + loads[PIECES + 2 :]:
        load.start()

    barrier = pltpu.get_barrier_semaphore()
    for key, there in signals.items():

        @pl.when(there)
        def _():
            pl.semaphore_signal(
                barrier,
                inc=1,
                device_id={key[0]: where_is[key]},
                device_id_type=pl.DeviceIdType.MESH,
            )


    @pl.when(is_far)
    def _():
        for g in range(ngz):
            pl.semaphore_signal(
                barrier,
                inc=1,
                device_id={"xy": pair, "gz": g},
                device_id_type=pl.DeviceIdType.MESH,
            )
        pl.semaphore_signal(
            barrier,
            inc=1,
            device_id={"xy": jnp.where(far[0], ix - 1, ix + 1)},
            device_id_type=pl.DeviceIdType.MESH,
        )

    def remote(src, dst, send, recv, key):
        return pltpu.make_async_remote_copy(
            src_ref=src,
            dst_ref=dst,
            send_sem=send,
            recv_sem=recv,
            device_id={key[0]: where_is[key]},
            device_id_type=pl.DeviceIdType.MESH,
        )

    def halo_copy(sweep, side, piece):
        span = pl.ds(piece * zs, zs)
        return remote(
            halo_out.at[sweep, side, :, :, span],
            halo_in.at[sweep, side, :, :, span],
            halo_send.at[side],
            halo_recv.at[side, piece],
            ("xy", 1 - side),
        )

    def send_halo(sweep, piece):
        for side in range(2):

            @pl.when(beside[1 - side])
            def _():
                halo_copy(sweep, side, piece).start()

    def early_copy(side, p, c):
        return remote(
            halo_out.at[1, 1 - side, p, c],
            FA.at[:, p, c, :],
            early_send,
            early_recv,
            ("xy", side),
        )

    def early_moved(side):
        return remote(
            halo_out.at[1, 1 - side],
            halo_out.at[1, 1 - side],
            early_send,
            early_recv,
            ("xy", side),
        )

    def row_copy(side, p, c):
        return remote(
            U.at[:, p, c, 0 if side else rows - 1, :],
            halo_in.at[0, side, p, c],
            row_send.at[side],
            row_recv.at[side],
            ("xy", 1 - side),
        )

    row_copies = lambda side: [row_copy(side, p, c) for p in range(2) for c in range(3)]
    rows_moved = lambda side: remote(
        halo_in.at[0, side],
        halo_in.at[0, side],
        row_send.at[side],
        row_recv.at[side],
        ("xy", 1 - side),
    )

    def pack(first, last, z, values):
        for i in range(6):
            at = (i // 3, i % 3, pl.ds(z, 1), slice(None))
            first[at] = values[i][:1, :]
            last[at] = values[i][rows - 1 :, :]

    for side in range(2):

        for sweep in range(SWEEPS):

            @pl.when(jnp.logical_not(beside[side]))
            def _():
                halo_in[sweep, side] = jnp.zeros(halo_in.shape[2:], jnp.float32)

        @pl.when((iz if side == 0 else ngz - 1 - iz) < 2)
        def _():
            for part in range(3, 9):
                info_in[side, part] = jnp.zeros(info_in.shape[2:], jnp.float32)
            lam_in[side] = jnp.zeros(lam_in.shape[1:], jnp.float32)
            for sweep in range(SWEEPS):
                ch_in[sweep, side] = jnp.zeros(ch_in.shape[2:], jnp.float32)

    loads[PIECES].wait()
    loads[PIECES + 1].wait()

    def diagonal(z, carry):
        ids = C[z]
        sigma = jnp.zeros(plane, jnp.float32)
        for kind in range(kinds):
            sigma = jnp.where(ids == kind, conductance[kind], sigma)
        SG[z] = sigma
        DR[z] = 2.0 + 4.0 * coupling + penalty * B[z].astype(jnp.float32)
        return carry

    loop(0, depth, diagonal, 0, 4)

    def diag(z):
        real = jnp.broadcast_to(DR[z][None], (3,) + plane)
        sigma = SG[z]
        return real, jnp.stack([sigma * strengths[j] for j in range(3)])

    none = (jnp.zeros((3,) + plane, jnp.float32),) * 2

    def pivots(k, carry):
        p, q = carry
        z, back = k, depth - 1 - k
        d, f = diag(z), diag(back)
        p = inv((d[0] - p[0], d[1] - p[1]))
        q = inv((f[0] - q[0], f[1] - q[1]))
        put(PH, p, z)
        put(PHI, q, back)
        return p, q

    loop(0, depth, pivots, (none, none), 2)
    ones = (jnp.ones((3,) + plane, jnp.float32), none[0])

    def columns(k, carry):
        down, up = carry
        z, back = k, depth - 1 - k
        down = mul(get(PHI, z), down)
        up = mul(get(PH, back), up)
        put(PHI, down, z)
        put(PSI, up, back)
        return down, up

    loop(0, depth, columns, (ones, ones), 2)
    for piece in range(PIECES):
        loads[piece].wait()

    @pl.when(not_far)
    def _():
        pl.semaphore_wait(barrier, count)

    @pl.when(helper)
    def _():
        pl.semaphore_signal(
            near_ready,
            inc=1,
            device_id={"xy": jnp.where(helps[0], ix - 1, ix + 1)},
            device_id_type=pl.DeviceIdType.MESH,
        )

    @pl.when(is_far)
    def _():
        pl.semaphore_wait(near_ready, 1)

    for side in range(2):

        @pl.when(beside[1 - side])
        def _():
            for copy in row_copies(side):
                copy.start()

    LEFT, RIGHT = 0, 1
    tip = (lambda: get(PHI, 0), lambda: get(PSI, depth - 1))
    across = lambda: get(PSI, 0)

    place = (iz, ngz - 1 - iz)
    even = [lax.rem(k, 2) == 0 for k in place]
    odd = [lax.rem(k, 2) == 1 for k in place]
    onward = [ngz - 1 - k for k in place]

    def to(side, steps):
        return {"gz": iz + steps if side == LEFT else iz - steps}

    def chain_copy(src, dst, send, recv, side, steps):
        return pltpu.make_async_remote_copy(
            src_ref=src,
            dst_ref=dst,
            send_sem=send,
            recv_sem=recv,
            device_id=to(side, steps),
            device_id_type=pl.DeviceIdType.MESH,
        )

    whole = slice(None)
    way = (lambda side: 0) if ngz == 4 else (lambda side: side)

    def tip_copy(side, j):
        return chain_copy(
            info_out.at[side, j],
            info_in.at[side, j],
            tip_send.at[way(side)],
            tip_recv.at[way(side), j],
            side,
            1,
        )

    def info_copy(side):
        return chain_copy(
            info_out.at[side, 3:9],
            info_in.at[side, 3:9],
            info_send.at[way(side)],
            info_recv.at[way(side)],
            side,
            1,
        )

    def lam_copy(side, steps, j):
        return chain_copy(
            lam_out.at[side, j],
            lam_in.at[side, j],
            lam_send.at[way(side), steps - 1],
            lam_recv.at[way(side), j],
            side,
            steps,
        )

    def own_copy(sweep, side, j):
        return chain_copy(
            own_out.at[sweep, side, j],
            own_in.at[sweep, side, j],
            own_send.at[sweep, way(side)],
            own_recv.at[sweep, way(side), j],
            side,
            1,
        )

    def x_copy(sweep, side, steps, j):
        return chain_copy(
            ch_out.at[sweep, side, j],
            ch_in.at[sweep, side, j],
            ch_send.at[sweep, way(side), steps - 1],
            ch_recv.at[sweep, way(side), j],
            side,
            steps,
        )


    both = jnp.logical_and

    def send_info(side):
        sends = both(even[side], onward[side] >= 1)
        parts = (tip[1 - side](), tip[side](), across())
        for part in range(3):
            for j in range(3):
                for p in range(2):
                    info_out[side, part * 3 + j, p] = parts[part][p][j]
            if part == 0:

                @pl.when(sends)
                def _():
                    for j in range(3):
                        tip_copy(side, j).start()

        @pl.when(both(sends, place[side] > 0))
        def _():
            info_copy(side).start()

    def pass_lam(side):
        @pl.when(both(odd[side], place[side] >= 2))
        def _():
            info_copy(side).wait_recv()

        for j in range(3):

            @pl.when(odd[side])
            def _():
                tip_copy(side, j).wait_recv()

            @pl.when(place[side] >= 2)
            def _():
                lam_copy(side, 1, j).wait_recv()

            tips = [(info_in[side, 3 * k + j, 0], info_in[side, 3 * k + j, 1]) for k in range(3)]
            given = (lam_in[side, j, 0], lam_in[side, j, 1])

            @pl.when(odd[side])
            def _():
                skip = mul(tips[2], inv(one_minus(mul(tips[1], given))))
                lam = add(tips[0], mul(tips[2], mul(skip, given)))
                for p in range(2):
                    coef[8 + side, p, j] = skip[p]
                    coef[10 + side, p, j] = lam[p]

            @pl.when(even[side])
            def _():
                for p in range(2):
                    coef[10 + side, p, j] = given[p]

            of = lambda pair: (pair[0][j], pair[1][j])
            lam = (coef[10 + side, 0, j], coef[10 + side, 1, j])
            kappa = mul(of(across()), inv(one_minus(mul(of(tip[side]()), lam))))
            over = mul(kappa, lam)
            value = add(of(tip[1 - side]()), mul(of(across()), over))
            for p in range(2):
                coef[side, p, j] = kappa[p]
                coef[2 + side, p, j] = over[p]
                lam_out[side, j, p] = value[p]

            @pl.when(both(odd[side], onward[side] >= 1))
            def _():
                lam_copy(side, 1, j).start()

        @pl.when(both(odd[side], onward[side] >= 2))
        def _():
            for j in range(3):
                lam_copy(side, 2, j).start()

    def own_base(side, j):
        return add(
            (ends[1 - side, 0, j], ends[1 - side, 1, j]),
            mul(
                (coef[2 + side, 0, j], coef[2 + side, 1, j]),
                (ends[side, 0, j], ends[side, 1, j]),
            ),
        )

    def own_sum(sweep, side):
        for j in range(3):
            base = own_base(side, j)
            for p in range(2):
                own_out[sweep, side, j, p] = base[p]

            @pl.when(both(even[side], onward[side] >= 1))
            def _():
                own_copy(sweep, side, j).start()

    def pass_chain(sweep, side):
        for j in range(3):
            base = own_base(side, j)

            @pl.when(odd[side])
            def _():
                own_copy(sweep, side, j).wait_recv()

            @pl.when(place[side] >= 2)
            def _():
                x_copy(sweep, side, 1, j).wait_recv()

            given = (ch_in[sweep, side, j, 0], ch_in[sweep, side, j, 1])

            @pl.when(odd[side])
            def _():
                own = (own_in[sweep, side, j, 0], own_in[sweep, side, j, 1])
                x = add(own, mul((coef[8 + side, 0, j], coef[8 + side, 1, j]), given))
                for p in range(2):
                    value_in[side, j, p] = x[p]

            @pl.when(even[side])
            def _():
                for p in range(2):
                    value_in[side, j, p] = given[p]

            x = (value_in[side, j, 0], value_in[side, j, 1])
            result = add(base, mul((coef[side, 0, j], coef[side, 1, j]), x))
            for p in range(2):
                ch_out[sweep, side, j, p] = result[p]

            @pl.when(both(odd[side], onward[side] >= 2))
            def _():
                x_copy(sweep, side, 2, j).start()

        @pl.when(both(odd[side], onward[side] >= 1))
        def _():
            for j in range(3):
                x_copy(sweep, side, 1, j).start()

    left_first = iz * 2 < ngz - 1

    def near_side(run):
        @pl.when(left_first)
        def _():
            run(LEFT)

        @pl.when(jnp.logical_not(left_first))
        def _():
            run(RIGHT)

    def far_side(run):
        @pl.when(left_first)
        def _():
            run(RIGHT)

        @pl.when(jnp.logical_not(left_first))
        def _():
            run(LEFT)

    def far_source(side, i):
        edge = pl.ds(rows - 1 if side else 0, 1)
        return (C.at[:, edge, :], B.at[:, edge, :])[i] if i < 2 else U.at[:, :, i - 2, edge, :]

    def far_target(i, first):
        at = pl.ds(first if i < 2 else first + i - 2, 1)
        return (CX.at[0, :, at, :], BX.at[0, :, at, :])[i] if i < 2 else XR.at[:, :, at, :]

    def far_copy(side, i):
        return pltpu.make_async_remote_copy(
            src_ref=far_source(side, i),
            dst_ref=far_target(i, 4 if i < 2 else 0),
            send_sem=far_send.at[min(i, 2)],
            recv_sem=far_recv.at[min(i, 2)],
            device_id={"xy": ix + 1 if side else ix - 1},
            device_id_type=pl.DeviceIdType.MESH,
        )

    def kept_copy(side, i):
        return pltpu.make_async_copy(
            far_source(side, i), far_target(i, 0 if i < 2 else 4), in_sems.at[min(i, 2)]
        )

    def field_moved(side):
        return pltpu.make_async_remote_copy(
            src_ref=XR.at[:, :, 0:3, :],
            dst_ref=XR.at[:, :, 0:3, :],
            send_sem=far_send.at[2],
            recv_sem=far_recv.at[2],
            device_id={"xy": ix + 1 if side else ix - 1},
            device_id_type=pl.DeviceIdType.MESH,
        )

    def field_kept():
        return pltpu.make_async_copy(XR.at[:, :, 4:7, :], XR.at[:, :, 4:7, :], in_sems.at[2])

    def lines_kept(i):
        ref = (CX, BX)[i].at[1, :, 0:2, :]
        return pltpu.make_async_copy(ref, ref, in_sems.at[3 + i])

    def line_copy(side, i):
        first = rows - 1 if side else 0
        edge = pl.ds(first if i < 2 else (first - 1 if side else first + 1), 1)
        at = pl.ds(0 if i < 2 else 4, 1)
        return pltpu.make_async_copy(
            (C, B)[i % 2].at[:, edge, :], (CX, BX)[i % 2].at[1, :, at, :], in_sems.at[3 + i % 2]
        )

    def far_begin():
        pl.semaphore_wait(barrier, 1)
        for side in range(2):

            @pl.when(far[side])
            def _():
                for i in range(5):
                    far_copy(side, i).start()
                for i in range(5):
                    kept_copy(side, i).start()
                for i in range(4):
                    line_copy(side, i).start()

    def near_lam(side):
        pl.when(place[side] < 2)(functools.partial(pass_lam, side))

    def far_lam(side):
        pl.when(place[side] == 2)(functools.partial(pass_lam, side))

    def last_lam(side):
        pl.when(place[side] >= 3)(functools.partial(pass_lam, side))

    near_side(send_info)
    far_side(send_info)

    angle_matrix = rotation(angles, (rows, 128))
    for c in range(3):
        for j in range(3):
            QM[c, j] = angle_matrix[c][j]

    def matrix():
        return [
            [jnp.concatenate([QM[c, j]] * (width // 128), axis=1) for j in range(3)]
            for c in range(3)
        ]

    def pack_columns(z, carry):
        for src, dst in ((PHI, EPHI), (PSI, EPSI)):
            pack(dst.at[0], dst.at[1], z, [src[z, i // 3, i % 3] for i in range(6)])
        return carry

    loop(0, depth, pack_columns, 0, 4)

    row = lax.broadcasted_iota(jnp.int32, plane, 0)
    lane = lax.broadcasted_iota(jnp.int32, plane, 1)
    zero = jnp.zeros(plane, jnp.float32)

    def turn(q, driven):
        return [
            jnp.stack(
                [
                    q[0][j] * driven[p][0] + q[1][j] * driven[p][1] + q[2][j] * driven[p][2]
                    for j in range(3)
                ]
            )
            for p in range(2)
        ]

    tall = lax.broadcasted_iota(jnp.int32, (rows, width // 2), 0)
    slim = lax.broadcasted_iota(jnp.int32, (rows, width // 2), 1)

    def inner(z, carry):
        first, last = carry
        q = matrix()
        half = width // 2
        driven = []
        for p in range(2):
            of = []
            for c in range(3):
                a, b = U[z, p, c, :, :half], U[z, p, c, :, half:]
                al, bl = pltpu.roll(a, 1, 1), pltpu.roll(b, 1, 1)
                ar, br = pltpu.roll(a, half - 1, 1), pltpu.roll(b, half - 1, 1)
                low, high = slim == 0, slim == half - 1
                around = []
                for v, l, r in (
                    (a, jnp.where(low, 0.0, al), jnp.where(high, br, ar)),
                    (b, jnp.where(low, al, bl), jnp.where(high, 0.0, br)),
                ):
                    up = jnp.where(tall == 0, 0.0, pltpu.roll(v, 1, 0))
                    down = jnp.where(tall == rows - 1, 0.0, pltpu.roll(v, rows - 1, 0))
                    around.append((l + r) + (up + down))
                of.append(S[z, p, c] + coupling * jnp.concatenate(around, axis=1))
            driven.append(of)
        turned = turn(q, driven)
        put(T, turned, z)
        return add(first, mul(get(PHI, z), turned)), add(last, mul(get(PSI, z), turned))

    tiles = [pl.ds(z, rows) for z in range(0, depth, rows)]

    def outer(sweep, side, tile, carry):
        first, last = carry
        q = matrix()
        turned = turn(
            q,
            [[coupling * halo_in[sweep, side, p, c, tile] for c in range(3)] for p in range(2)],
        )
        for p in range(2):
            EH[side, p, :, tile] = turned[p]
        phi = [EPHI[side, p, :, tile] for p in range(2)]
        psi = [EPSI[side, p, :, tile] for p in range(2)]
        return add(first, mul(phi, turned)), add(last, mul(psi, turned))

    third = lax.rem(row, 4)
    part = lambda k: third == k
    used = third < 3

    def mi_copy(k, steps, parts):
        slot = steps + 3 if steps < 0 else steps + 2
        return pltpu.make_async_remote_copy(
            src_ref=mi_out.at[k, parts],
            dst_ref=mi_in.at[k, 5 - slot, parts],
            send_sem=mi_send.at[slot],
            recv_sem=mi_recv.at[0 if k == whole else k, 5 - slot],
            device_id={"gz": iz + steps},
            device_id_type=pl.DeviceIdType.MESH,
        )

    all_steps = (-3, -2, -1, 1, 2, 3)
    at_end = lambda k: jnp.logical_or(k == 0, k == ngz - 1)

    def for_all(of, act):
        for steps in all_steps:
            there = (iz + steps >= 0) & (iz + steps < ngz)
            edge_ = at_end(iz + steps * of)

            @pl.when(jnp.logical_and(there, edge_))
            def _():
                act(steps, True)

            @pl.when(jnp.logical_and(there, jnp.logical_not(edge_)))
            def _():
                act(steps, False)

    def to_all(k, first):
        def act(steps, ends_only):
            if not ends_only:
                parts = pl.ds(first, 4 if first else 6)
            else:
                parts = pl.ds(first + (2 if steps > 0 else 0), 2)
            mi_copy(k, steps, parts).start()

        for_all(0, act)

    def moved(ends_only):
        return pl.ds(0, 4 if ends_only else 10)

    def from_all(k):
        for_all(1, lambda steps, e: mi_copy(k, -steps, moved(e)).wait_recv())

    def shifts(of):
        planes = []
        for d in (-2, -1, 0, 1, 2):
            plane_ = zero
            for j in range(3):
                if 0 <= j + d <= 2:
                    plane_ = jnp.where(part(j), of(j, j + d), plane_)
            planes.append((d, plane_))
        return planes

    def mix(planes, x):
        total = None
        for d, plane_ in planes:
            term = plane_ * (x if d == 0 else pltpu.roll(x, (rows - d) % rows, 0))
            total = term if total is None else total + term
        return total

    def far_clear():
        none_ = jnp.zeros((2,) + plane, jnp.float32)
        for slot, steps in enumerate(all_steps):
            there = (iz + steps >= 0) & (iz + steps < ngz)

            @pl.when(jnp.logical_not(there))
            def _():
                for k in range(2):
                    for part_ in range(5):
                        mi_in[k, slot, 2 * part_ : 2 * part_ + 2] = none_

            @pl.when(jnp.logical_and(there, at_end(iz + steps)))
            def _():
                for k in range(2):
                    for part_ in (0, 2, 3) if steps < 0 else (1, 2, 4):
                        mi_in[k, slot, 2 * part_ : 2 * part_ + 2] = none_

    def far_setup():
        q = matrix()
        for i, (_, plane_) in enumerate(shifts(lambda j, k: q[k][j])):
            FC[i] = plane_
        for i, (_, plane_) in enumerate(shifts(lambda j, k: q[j][k])):
            FC[5 + i] = plane_
        strength = jnp.full(plane, strengths[0], jnp.float32)
        for j in (1, 2):
            strength = jnp.where(part(j), strengths[j], strength)
        FC[10] = strength

    own = row < 4

    def far_first(k):
        for side in range(2):

            @pl.when(far[side])
            def _():
                if k == 0:
                    for i in range(2):
                        kept_copy(side, i).wait()
                        far_copy(side, i).wait_recv()
                else:
                    for i in range(2):
                        lines_kept(i).wait()

        def far_diagonal(z, carry):
            ids_tile, bound = CX[k, z], BX[k, z]
            ids = jnp.where(
                own,
                jnp.broadcast_to(ids_tile[0:1, :], plane),
                jnp.broadcast_to(ids_tile[4:5, :], plane),
            )
            edge = jnp.where(
                own, jnp.broadcast_to(bound[0:1, :], plane), jnp.broadcast_to(bound[4:5, :], plane)
            )
            sigma = jnp.zeros(plane, jnp.float32)
            for kind in range(kinds):
                sigma = jnp.where(ids == kind, conductance[kind], sigma)
            FT[k, z, 0] = 2.0 + 4.0 * coupling + penalty * edge.astype(jnp.float32)
            FT[k, z, 1] = sigma * FC[10]
            return carry

        loop(0, depth, far_diagonal, 0, 4)

        def far_pivots(z, carry):
            p, q = carry
            d, f = get(FT, k, z), get(FT, k, depth - 1 - z)
            p = inv((d[0] - p[0], d[1] - p[1]))
            q = inv((f[0] - q[0], f[1] - q[1]))
            put(FP, p, k, z)
            put(FPHI, q, k, depth - 1 - z)
            return p, q

        loop(0, depth, far_pivots, ((zero, zero), (zero, zero)), 2)
        one = jnp.ones(plane, jnp.float32)

        def far_columns(z, carry):
            down, up = carry
            back = depth - 1 - z
            down = mul(get(FPHI, k, z), down)
            up = mul(get(FP, k, back), up)
            put(FPHI, down, k, z)
            put(FPSI, up, k, back)
            return down, up

        loop(0, depth, far_columns, ((one, zero), (one, zero)), 2)
        ends_ = (get(FPHI, k, 0), get(FPSI, k, depth - 1), get(FPSI, k, 0))
        for i, value in enumerate(ends_):
            mi_out[k, 2 * i] = value[0]
            mi_out[k, 2 * i + 1] = value[1]

    def send_columns(k):
        to_all(k, 0)

    def far_solve(k, rhs):
        turned_by = [(d, FC[i]) for i, d in enumerate((-2, -1, 0, 1, 2))]

        def far_sums(z, carry):
            first, last = carry
            t = tuple(
                mix(turned_by, jnp.where(used, coupling * rhs(z, p), zero)) for p in range(2)
            )
            put(FT, t, k, z)
            return add(first, mul(get(FPHI, k, z), t)), add(last, mul(get(FPSI, k, z), t))

        first, last = loop(0, depth, far_sums, ((zero, zero), (zero, zero)), 4)
        for i, value in enumerate((first, last)):
            mi_out[k, 6 + 2 * i] = value[0]
            mi_out[k, 7 + 2 * i] = value[1]
        to_all(k, 6)

        def far_forward(z, m):
            m = mul(get(FP, k, z), add(get(FT, k, z), m))
            put(FT, m, k, z)
            return m

        def far_backward(i, w):
            z = depth - 1 - i
            w = add(get(FT, k, z), mul(get(FP, k, z), w))
            put(FT, w, k, z)
            return w

        loop(0, depth, far_forward, (zero, zero), 4)
        loop(0, depth, far_backward, (zero, zero), 4)

    def far_second():
        for side in range(2):

            @pl.when(far[side])
            def _():
                field_moved(side).wait_recv()

        far_solve(0, lambda z, p: XR[z, p])

    def far_meet(k, take):
        from_all(k)
        block = lambda slot: [(mi_in[k, slot, 2 * i], mi_in[k, slot, 2 * i + 1]) for i in range(5)]
        x = lam = y = mu = (zero, zero)
        for slot in range(3):
            top, bottom, cross, first, last = block(slot)
            det = inv(one_minus(mul(top, lam)))
            x, lam = (
                add(last, mul(cross, mul(det, add(x, mul(lam, first))))),
                add(bottom, mul(mul(cross, cross), mul(det, lam))),
            )
        for slot in (5, 4, 3):
            top, bottom, cross, first, last = block(slot)
            det = inv(one_minus(mul(bottom, mu)))
            y, mu = (
                add(first, mul(cross, mul(det, add(y, mul(mu, last))))),
                add(top, mul(mul(cross, cross), mul(det, mu))),
            )
        top, bottom, cross, first, last = [(mi_out[k, 2 * i], mi_out[k, 2 * i + 1]) for i in range(5)]
        g, h = add(x, mul(lam, first)), add(y, mul(mu, last))
        alpha, beta = one_minus(mul(lam, top)), one_minus(mul(mu, bottom))
        lc, mc = mul(lam, cross), mul(mu, cross)
        both_ = mul(lc, mc)
        all_ = mul(alpha, beta)
        det = inv((all_[0] - both_[0], all_[1] - both_[1]))
        put(far_ends, mul(det, add(mul(g, beta), mul(lc, h))), 0)
        put(far_ends, mul(det, add(mul(h, alpha), mul(mc, g))), 1)
        back_by = [(d, FC[5 + i]) for i, d in enumerate((-2, -1, 0, 1, 2))]

        def far_join(z, carry):
            before, after = get(far_ends, 0), get(far_ends, 1)
            w = add(
                add(get(FT, k, z), mul(get(FPHI, k, z), before)), mul(get(FPSI, k, z), after)
            )
            for p in range(2):
                take(z, p, mix(back_by, w[p]))
            return carry

        loop(0, depth, far_join, 0, 4)

    def far_third():
        def keep(z, p, u):
            FT[0, z, p] = u

        far_meet(0, keep)
        for side in range(2):

            @pl.when(far[side])
            def _():
                early_moved(side).wait_recv()

        def rhs(z, p):
            u = FT[0, z, p]
            beside_ = jnp.where(lane == 0, zero, pltpu.roll(u, 1, 1))
            beside_ += jnp.where(lane == width - 1, zero, pltpu.roll(u, width - 1, 1))
            early = jnp.where(row < 3, FA[z, p], zero)
            return pltpu.roll(u, 4, 0) + jnp.where(own, beside_ + early, zero)

        far_solve(1, rhs)

    def far_last():
        here = row == jnp.where(far[1], rows - 1, 0)
        next_ = row == jnp.where(far[1], rows - 2, 1)

        def give(z, p, u):
            for c in range(3):
                OUT[z, p, c] += jnp.where(
                    here,
                    jnp.broadcast_to(u[c : c + 1, :], plane),
                    jnp.where(next_, jnp.broadcast_to(u[4 + c : 5 + c, :], plane), zero),
                )

        far_meet(1, give)

    loads[PIECES + 2].wait()
    for sweep in range(SWEEPS):
        sums = loop(0, depth, inner, (none, none), 4)
        if sweep == 0:
            near_side(near_lam)
        halves = [(none, none), (none, none)]
        for piece in range(PIECES):
            for side in range(2):

                if sweep == 0 and piece == 0:

                    @pl.when(beside[side])
                    def _():
                        rows_moved(side).wait_recv()

                if sweep:

                    @pl.when(beside[side])
                    def _():
                        halo_copy(sweep, side, piece).wait_recv()

                for tile in tiles[piece * len(tiles) // PIECES : (piece + 1) * len(tiles) // PIECES]:
                    halves[side] = outer(sweep, side, tile, halves[side])
        for side in range(2):
            here = row == (0 if side == 0 else rows - 1)
            sums = tuple(
                add(
                    sums[end],
                    tuple(
                        jnp.where(here[None], jnp.sum(part, axis=1, keepdims=True), 0.0)
                        for part in halves[side][end]
                    ),
                )
                for end in range(2)
            )
        put(ends, sums[0], 0)
        put(ends, sums[1], 1)

        near_side(functools.partial(own_sum, sweep))
        if sweep == 0:
            pl.when(is_far)(far_begin)
            far_side(far_lam)
        far_side(functools.partial(own_sum, sweep))
        if sweep:

            @pl.when(is_far)
            def _():
                far_second()

        near_side(functools.partial(pass_chain, sweep))

        def forward(z, m):
            given = []
            for p in range(2):
                edges = []
                for j in range(3):
                    above = jnp.broadcast_to(EH[0, p, j, pl.ds(z, 1), :], plane)
                    below = jnp.broadcast_to(EH[1, p, j, pl.ds(z, 1), :], plane)
                    edges.append(
                        jnp.where(row == 0, above, zero) + jnp.where(row == rows - 1, below, zero)
                    )
                given.append(T[z, p] + jnp.stack(edges))
            m = mul(get(PH, z), add(given, m))
            put(T, m, z)
            return m

        def backward(k, w):
            z = depth - 1 - k
            w = add(get(T, z), mul(get(PH, z), w))
            put(T, w, z)
            if sweep < SWEEPS - 1:
                pack(ET.at[0], ET.at[1], z, [w[i // 3][i % 3] for i in range(6)])
            return w

        loop(0, depth, forward, none, 4)
        loop(0, depth, backward, none, 4)
        if sweep:

            @pl.when(is_far)
            def _():
                send_columns(1)
                far_third()

        else:

            @pl.when(is_far)
            def _():
                far_clear()
                far_setup()
                far_first(1)

        if sweep == 0:
            far_side(last_lam)
            for side in range(2):
                lam = get(coef, 10 + side)
                away = tuple(
                    jnp.stack([lam_out[1 - side, j, p] for j in range(3)]) for p in range(2)
                )
                det = inv(one_minus(mul(lam, away)))
                put(coef, det, 6 + side)
                put(coef, mul(det, lam), 4 + side)
        far_side(functools.partial(pass_chain, sweep))

        for side in range(2):
            for j in range(3):
                arrived = (value_in[side, j, 0], value_in[side, j, 1])
                other = (ch_out[sweep, 1 - side, j, 0], ch_out[sweep, 1 - side, j, 1])
                value = add(
                    mul((coef[6 + side, 0, j], coef[6 + side, 1, j]), arrived),
                    mul((coef[4 + side, 0, j], coef[4 + side, 1, j]), other),
                )
                near[side, 0, j] = value[0]
                near[side, 1, j] = value[1]

        final = sweep == SWEEPS - 1

        def join_edge(side, tile):
            q = matrix()
            r = 0 if side == 0 else rows - 1
            w = [ET[side, p, :, tile] for p in range(2)]
            for end, column in ((0, EPHI), (1, EPSI)):
                entry = [
                    jnp.broadcast_to(near[end, p, :, r : r + 1, :], (3,) + plane)
                    for p in range(2)
                ]
                w = add(w, mul([column[side, p, :, tile] for p in range(2)], entry))
            for p in range(2):
                for c in range(3):
                    halo_out[sweep + 1, 1 - side, p, c, tile] = (
                        q[c][0] * w[p][0] + q[c][1] * w[p][1] + q[c][2] * w[p][2]
                    )

        if not final:
            for piece in range(PIECES):
                for tile in tiles[piece * len(tiles) // PIECES : (piece + 1) * len(tiles) // PIECES]:
                    for side in range(2):
                        join_edge(side, tile)
                send_halo(sweep + 1, piece)
            for side in range(2):

                @pl.when(far[side])
                def _():
                    for p in range(2):
                        for c in range(3):
                            early_copy(side, p, c).start()


        def join(z, carry):
            q = matrix()
            before, after = get(near, 0), get(near, 1)
            w = add(add(get(T, z), mul(get(PHI, z), before)), mul(get(PSI, z), after))
            values = []
            for p in range(2):
                for c in range(3):
                    values.append(q[c][0] * w[p][0] + q[c][1] * w[p][1] + q[c][2] * w[p][2])
            target = OUT if final else U
            for i in range(6):
                target[z, i // 3, i % 3] = values[i]
            return carry

        if not final:
            for side in range(2):

                @pl.when(far[side])
                def _():
                    for i in range(2):
                        far_copy(side, i).wait_send()
                    field_moved(side).wait_send()
                    field_kept().wait()

                @pl.when(beside[1 - side])
                def _():
                    rows_moved(side).wait_send()

        loop(0, depth, join, 0, 4)

        if not final:


            @pl.when(is_far)
            def _():
                far_first(0)
                send_columns(0)

        else:
            pl.when(is_far)(far_last)

    @pl.when(is_far)
    def _():
        for_all(0, lambda steps, e: mi_copy(whole, steps, moved(e)).wait_send())

    for side in range(2):

        @pl.when(beside[1 - side])
        def _():
            remote(
                halo_out.at[1, side],
                halo_in.at[1, side],
                halo_send.at[side],
                halo_recv.at[side, 0],
                ("xy", 1 - side),
            ).wait_send()

        @pl.when(far[side])
        def _():
            early_moved(side).wait_send()

        sends = both(even[side], onward[side] >= 1)

        @pl.when(sends)
        def _():
            chain_copy(
                info_out.at[side, 0:3],
                info_in.at[side, 0:3],
                tip_send.at[way(side)],
                info_recv.at[way(side)],
                side,
                1,
            ).wait_send()
            for sweep in range(SWEEPS):
                own_copy(sweep, side, whole).wait_send()

        @pl.when(both(sends, place[side] > 0))
        def _():
            info_copy(side).wait_send()

        for steps in (2, 1):

            @pl.when(both(odd[side], onward[side] >= steps))
            def _():
                lam_copy(side, steps, whole).wait_send()
                for sweep in range(SWEEPS):
                    x_copy(sweep, side, steps, whole).wait_send()


def local(ngz, nxy, field, source, classes, boundary, conductance, angles, strengths):
    depth, _, _, rows, width = field.shape
    f32 = jnp.float32
    block = pltpu.VMEM(field.shape, f32)
    flat = (depth, rows, width)
    line = (2, 3, rows, width)
    pair = (2, rows, width)
    edge = (2, 2, 3, depth, width)
    narrow = pltpu.VMEM((depth, 2, rows, width), f32)
    lines = pltpu.VMEM((2, depth, 2, rows, width), f32)
    dma = pltpu.SemaphoreType.DMA
    ways = 1 if ngz == 4 else 2
    hbm = pl.BlockSpec(memory_space=pl.ANY)
    smem = pl.BlockSpec(memory_space=pltpu.SMEM)
    return pl.pallas_call(
        functools.partial(relax, ngz, nxy),
        out_shape=pltpu.VMEM(field.shape, f32),
        in_specs=[hbm] * 4 + [smem] * 3,
        out_specs=pl.BlockSpec(memory_space=pltpu.VMEM),
        scratch_shapes=[
            block,
            block,
            pltpu.VMEM(flat, jnp.int32),
            pltpu.VMEM(flat, jnp.int32),
            pltpu.VMEM(flat, f32),
            pltpu.VMEM(flat, f32),
            block,
            block,
            block,
            block,
            pltpu.VMEM((3, 3, rows, 128), f32),
            pltpu.VMEM(edge, f32),
            pltpu.VMEM(edge, f32),
            pltpu.VMEM(edge, f32),
            pltpu.VMEM(edge, f32),
            pltpu.VMEM((2,) + line, f32),
            pltpu.VMEM((14,) + line, f32),
            pltpu.VMEM((2,) + line, f32),
            pltpu.VMEM((SWEEPS,) + edge, f32),
            pltpu.VMEM((SWEEPS,) + edge, f32),
            pltpu.VMEM((2, 3) + pair, f32),
            pltpu.VMEM((2, 9) + pair, f32),
            pltpu.VMEM((2, 9) + pair, f32),
            pltpu.VMEM((2, 3) + pair, f32),
            pltpu.VMEM((2, 3) + pair, f32),
            pltpu.VMEM((SWEEPS, 2, 3) + pair, f32),
            pltpu.VMEM((SWEEPS, 2, 3) + pair, f32),
            pltpu.VMEM((SWEEPS, 2, 3) + pair, f32),
            pltpu.VMEM((SWEEPS, 2, 3) + pair, f32),
            narrow,
            narrow,
            pltpu.VMEM((2,) + flat, jnp.int32),
            pltpu.VMEM((2,) + flat, jnp.int32),
            lines,
            lines,
            lines,
            lines,
            pltpu.VMEM((11, rows, width), f32),
            pltpu.VMEM((2,) + pair, f32),
            pltpu.VMEM((2, 6, 10, rows, width), f32),
            pltpu.VMEM((2, 10, rows, width), f32),
            dma((PIECES + 3,)),
            dma((2,)),
            dma((2, PIECES)),
            dma((ways,)),
            dma((ways, 3)),
            dma((ways,)),
            dma((ways,)),
            dma((ways, 2)),
            dma((ways, 3)),
            dma((SWEEPS, ways)),
            dma((SWEEPS, ways, 3)),
            dma((SWEEPS, ways, 2)),
            dma((SWEEPS, ways, 3)),
            dma((3,)),
            dma((3,)),
            pltpu.SemaphoreType.REGULAR,
            dma((2,)),
            dma((2,)),
            dma(()),
            dma(()),
            dma((6,)),
            dma((2, 6)),
        ],
        compiler_params=pltpu.CompilerParams(collective_id=0, has_side_effects=True, vmem_limit_bytes=VMEM_LIMIT),
    )(field, source, classes, boundary, conductance, angles, strengths)


def solution(mesh):
    in_specs = (
        P("gz", None, None, "xy", None),
        P("gz", None, None, "xy", None),
        P("gz", "xy", None),
        P("gz", "xy", None),
        P(),
        P(),
        P(),
    )
    out_specs = P("gz", None, None, "xy", None)
    body = functools.partial(local, mesh.shape["gz"], mesh.shape["xy"])
    return jax.shard_map(body, mesh=mesh, in_specs=in_specs, out_specs=out_specs, check_vma=False)
```
